16 devices in a mesh: shard: 2 (over z), worker: 8 (over y, x, core).
Axes of the slice: x: 2, y: 2, z: 2, core: 2. Of those that a mesh axis runs over, the one named last changes fastest.
Arguments:
- w1_local: float32 [16, 4, 256, 1024], P(('shard', 'worker'))
- w2_local: float32 [16, 4, 1024, 256], P(('shard', 'worker'))
- w1_global: float32 [4, 256, 1024], replicated
- w2_global: float32 [4, 1024, 256], replicated
- mom1: float32 [4, 256, 1024], replicated
- mom2: float32 [4, 1024, 256], replicated
- x_batches: bfloat16 [16, 4, 128, 256], P(('shard', 'worker'))
- y_targets: bfloat16 [16, 4, 128, 256], P(('shard', 'worker'))
Outputs:
- output 1: float32 [16, 4, 256, 1024], P(('shard', 'worker'))
- output 2: float32 [16, 4, 1024, 256], P(('shard', 'worker'))
- output 3: float32 [4, 256, 1024], replicated
- output 4: float32 [4, 1024, 256], replicated
- output 5: float32 [4, 256, 1024], replicated
- output 6: float32 [4, 1024, 256], replicated
All inputs are finite; a program needn't handle non-finite values.
Results may differ from the reference program's by a relative error of at most 0.00194075.
Values are sent between devices in bfloat16 or wider.
A program may use at most 1 GiB of HBM per device.

```python
import jax
import jax.numpy as jnp
from jax import lax

D = 256
FF = 1024
LAYERS = 4
BATCH = 128
STEPS = 4
WORKERS = 16
FRAGS = 2
TAU = 1

INNER_LR = 2.0 * D / (FF * LAYERS)
OUTER_LR = 0.7
OUTER_MOM = 0.9
MERGE_MIX = 0.5


def setup_inputs(seed: int = 0) -> dict:
    keys = jax.random.split(jax.random.key(seed), 10)
    in_scale = D ** -0.5
    out_scale = (FF * LAYERS) ** -0.5
    shape_one = (LAYERS, D, FF)
    shape_two = (LAYERS, FF, D)
    w1_global = in_scale * jax.random.normal(keys[0], shape_one, jnp.float32)
    w2_global = out_scale * jax.random.normal(keys[1], shape_two, jnp.float32)
    w1_base = w1_global + 0.1 * in_scale * jax.random.normal(keys[2], shape_one, jnp.float32)
    w2_base = w2_global + 0.1 * out_scale * jax.random.normal(keys[3], shape_two, jnp.float32)
    w1_local = w1_base[None] + 0.2 * in_scale * jax.random.normal(keys[4], (WORKERS,) + shape_one, jnp.float32)
    w2_local = w2_base[None] + 0.2 * out_scale * jax.random.normal(keys[5], (WORKERS,) + shape_two, jnp.float32)
    mom1 = 0.1 * in_scale * jax.random.normal(keys[6], shape_one, jnp.float32)
    mom2 = 0.1 * out_scale * jax.random.normal(keys[7], shape_two, jnp.float32)
    batch_shape = (WORKERS, STEPS, BATCH, D)
    x_batches = jax.random.normal(keys[8], batch_shape, jnp.float32).astype(jnp.bfloat16)
    y_targets = jax.random.normal(keys[9], batch_shape, jnp.float32).astype(jnp.bfloat16)
    return {'w1_local': w1_local, 'w2_local': w2_local, 'w1_global': w1_global, 'w2_global': w2_global, 'mom1': mom1, 'mom2': mom2, 'x_batches': x_batches, 'y_targets': y_targets}


def gelu_fn(pre_act):
    return jax.nn.gelu(pre_act, approximate=True)


def inner_step(w1_stack, w2_stack, x_tok, y_tok):
    def fwd_layer(hidden, weights):
        w1_layer, w2_layer = weights
        h_bf = hidden.astype(jnp.bfloat16)
        pre_act = jnp.dot(h_bf, w1_layer.astype(jnp.bfloat16), preferred_element_type=jnp.float32)
        u_bf = gelu_fn(pre_act).astype(jnp.bfloat16)
        out_hidden = hidden + jnp.dot(u_bf, w2_layer.astype(jnp.bfloat16), preferred_element_type=jnp.float32)
        return out_hidden, (h_bf, pre_act)
    h_last, (h_saved, act_saved) = lax.scan(fwd_layer, x_tok.astype(jnp.float32), (w1_stack, w2_stack))
    d_hidden = (2.0 / (BATCH * D)) * (h_last - y_tok.astype(jnp.float32))
    def bwd_layer(d_h, saved):
        h_bf, pre_act, w1_layer, w2_layer = saved
        u_val, gelu_back = jax.vjp(gelu_fn, pre_act)
        dh_bf = d_h.astype(jnp.bfloat16)
        grad_w2 = jnp.dot(u_val.astype(jnp.bfloat16).T, dh_bf, preferred_element_type=jnp.float32)
        d_u = jnp.dot(dh_bf, w2_layer.astype(jnp.bfloat16).T, preferred_element_type=jnp.float32)
        d_act = gelu_back(d_u)[0].astype(jnp.bfloat16)
        grad_w1 = jnp.dot(h_bf.T, d_act, preferred_element_type=jnp.float32)
        d_next = d_h + jnp.dot(d_act, w1_layer.astype(jnp.bfloat16).T, preferred_element_type=jnp.float32)
        return d_next, (grad_w1, grad_w2)
    _, (grads_one, grads_two) = lax.scan(bwd_layer, d_hidden, (h_saved, act_saved, w1_stack, w2_stack), reverse=True)
    return w1_stack - INNER_LR * grads_one, w2_stack - INNER_LR * grads_two


def run_steps(w1_all, w2_all, x_batches, y_targets, first_step, end_step):
    def one_worker(worker_args):
        w1_own, w2_own, x_own, y_own = worker_args
        def body(step_idx, carry):
            return inner_step(carry[0], carry[1], x_own[step_idx], y_own[step_idx])
        return lax.fori_loop(first_step, end_step, body, (w1_own, w2_own))
    return lax.map(one_worker, (w1_all, w2_all, x_batches, y_targets))


def outer_update(local_frag, global_frag, mom_frag):
    frag_delta = global_frag[None] - local_frag
    mean_delta = jnp.mean(frag_delta.astype(jnp.bfloat16).astype(jnp.float32), axis=0)
    new_mom = OUTER_MOM * mom_frag + mean_delta
    new_global = global_frag - OUTER_LR * (OUTER_MOM * new_mom + mean_delta)
    return new_global, new_mom


def reference(w1_local, w2_local, w1_global, w2_global, mom1, mom2, x_batches, y_targets):
    frag_layers = LAYERS // FRAGS
    frag_steps = STEPS // FRAGS
    steps_done = 0
    for frag_idx in range(FRAGS):
        first_layer = frag_idx * frag_layers
        end_layer = first_layer + frag_layers
        sync_step = (frag_idx + 1) * frag_steps - 1 - TAU
        w1_local, w2_local = run_steps(w1_local, w2_local, x_batches, y_targets, steps_done, sync_step + 1)
        glob_one, new_mom1 = outer_update(w1_local[:, first_layer:end_layer], w1_global[first_layer:end_layer], mom1[first_layer:end_layer])
        glob_two, new_mom2 = outer_update(w2_local[:, first_layer:end_layer], w2_global[first_layer:end_layer], mom2[first_layer:end_layer])
        w1_global = w1_global.at[first_layer:end_layer].set(glob_one)
        w2_global = w2_global.at[first_layer:end_layer].set(glob_two)
        mom1 = mom1.at[first_layer:end_layer].set(new_mom1)
        mom2 = mom2.at[first_layer:end_layer].set(new_mom2)
        w1_local, w2_local = run_steps(w1_local, w2_local, x_batches, y_targets, sync_step + 1, sync_step + TAU + 1)
        w1_local = w1_local.at[:, first_layer:end_layer].set(MERGE_MIX * w1_local[:, first_layer:end_layer] + (1.0 - MERGE_MIX) * glob_one[None])
        w2_local = w2_local.at[:, first_layer:end_layer].set(MERGE_MIX * w2_local[:, first_layer:end_layer] + (1.0 - MERGE_MIX) * glob_two[None])
        steps_done = sync_step + TAU + 1
    return w1_local, w2_local, w1_global, w2_global, mom1, mom2
```

```python
import jax
import jax.numpy as jnp
from jax import lax
from jax.experimental import pallas as pl
from jax.experimental.pallas import tpu as pltpu
from jax.sharding import PartitionSpec as P

OUTER_LR = 0.7
OUTER_MOM = 0.9
MERGE_MIX = 0.5

L = 4
H = 4
D = 256
FF = 1024
B = 128
NB = FF // D
INNER_LR = 2.0 * D / (FF * L)
N_ALL = 16
F32 = jnp.float32
BF16 = jnp.bfloat16
MESH = pl.DeviceIdType.MESH
ANY = pl.BlockSpec(memory_space=pl.ANY)
VMEM = pl.BlockSpec(memory_space=pltpu.VMEM)

PIECES = ((1, 2), (1, 1), (0, 2), (0, 1))
COLOR_UNITS = ((3, 3, 2), (3, 2, 3), (2, 3, 3), (3, 3, 2))
GROUPS = []
for piece_idx in range(4):
    first_unit = 0
    for color in range(3):
        GROUPS.append((piece_idx, color, first_unit, COLOR_UNITS[piece_idx][color]))
        first_unit += COLOR_UNITS[piece_idx][color]
RS1, RS2, AG0, AG1, AG2, DDA, DDB = range(7)


def dot(a, b, ca, cb):
    return lax.dot_general(a, b, (((ca,), (cb,)), ((), ())), preferred_element_type=F32)


def gelu_pair(a):
    k0 = 0.7978845608028654
    a2 = a * a
    t = jnp.tanh(k0 * (a + 0.044715 * (a2 * a)))
    half = 0.5 * (1.0 + t)
    u = a * half
    du = half + (0.5 * a) * (1.0 - t * t) * (k0 * (1.0 + (3 * 0.044715) * a2))
    return u, du


def main_body(w1_in, w2_in, g1_in, g2_in, m1_in, m2_in, x_in, y_in,
              w1, w2, g1, g2, m1, m2,
              xb, yb, w1b, w2b, hb, ub, du, hid, dhid,
              delta, raw, s1, r1, s2, r2, full,
              ld_sem, s0_send, s0_recv, st_send, st_recv):
    zc = lax.axis_index('shard')
    wk = lax.axis_index('worker')
    core = lax.rem(wk, 2)
    xc = lax.rem(wk // 2, 2)
    yc = wk // 4
    coord = (xc, yc, zc)

    def chip_peer(dim, same_core=True):
        w = wk
        s = zc
        if dim == 0:
            w = wk + 2 - 4 * xc
        elif dim == 1:
            w = wk + 4 - 8 * yc
        elif dim == 2:
            s = 1 - zc
        if not same_core:
            w = w + 1 - 2 * core
        return (s, w)

    partner = chip_peer(3, False)

    bar = pltpu.get_barrier_semaphore()
    pl.semaphore_signal(bar, inc=1, device_id=partner, device_id_type=MESH)
    for dim in range(3):
        for same in (True, False):
            pl.semaphore_signal(bar, inc=1, device_id=chip_peer(dim, same), device_id_type=MESH)

    def loads():
        cps = [pltpu.make_async_copy(x_in.at[0], xb, ld_sem.at[24]),
               pltpu.make_async_copy(y_in.at[0], yb, ld_sem.at[25])]
        for lay in range(L):
            cps.append(pltpu.make_async_copy(w1_in.at[0, lay], w1.at[0, lay], ld_sem.at[lay]))
            cps.append(pltpu.make_async_copy(w2_in.at[0, lay], w2.at[0, lay], ld_sem.at[4 + lay]))
        gcps = []
        for lay in range(L):
            gcps.append(pltpu.make_async_copy(g1_in.at[lay], g1.at[lay], ld_sem.at[8 + lay]))
            gcps.append(pltpu.make_async_copy(g2_in.at[lay], g2.at[lay], ld_sem.at[12 + lay]))
            gcps.append(pltpu.make_async_copy(m1_in.at[lay], m1.at[lay], ld_sem.at[16 + lay]))
            gcps.append(pltpu.make_async_copy(m2_in.at[lay], m2.at[lay], ld_sem.at[20 + lay]))
        return cps, gcps

    cps, gcps = loads()
    for cp in cps + gcps:
        cp.start()
    cps[0].wait()
    cps[1].wait()
    for lay in range(L):
        cps[2 + 2 * lay].wait()
        cps[3 + 2 * lay].wait()

        def cast1(i, _, lay=lay):
            rows = pl.ds(pl.multiple_of(i * 32, 32), 32)
            w1b[lay, rows, :] = w1[0, lay, rows, :].astype(BF16)
            return 0

        def cast2(i, _, lay=lay):
            rows = pl.ds(pl.multiple_of(i * 128, 128), 128)
            w2b[lay, rows, :] = w2[0, lay, rows, :].astype(BF16)
            return 0

        lax.fori_loop(0, D // 32, cast1, 0)
        lax.fori_loop(0, FF // 128, cast2, 0)
    for cp in gcps:
        cp.wait()
    pl.semaphore_wait(bar, 7)

    def dims_of(color_idx):
        return color_idx % 3, (color_idx + 1) % 3, (color_idx + 2) % 3

    def rs0_copies(gi):
        p, c, u0, nu = GROUPS[gi]
        d0 = dims_of(c)[0]
        k0 = coord[d0]
        us = pl.ds(u0, nu)
        other = 1 - core

        def rows(tc, blk):
            return pl.ds(pl.multiple_of(tc * 64 + blk * 32, 32), 32)

        out = []
        for idx, (tc, blk, dev) in enumerate(((other, k0, partner),
                                               (core, 1 - k0, chip_peer(d0, True)),
                                               (other, 1 - k0, chip_peer(d0, False)))):
            out.append(pltpu.make_async_remote_copy(
                src_ref=delta.at[p, us, rows(tc, blk)], dst_ref=raw.at[idx, p, us],
                send_sem=s0_send.at[gi, idx], recv_sem=s0_recv.at[gi, idx],
                device_id=dev, device_id_type=MESH))
        return out

    def stage_copy(stage, gi):
        p, c, u0, nu = GROUPS[gi]
        d0, d1, d2 = dims_of(c)
        k0, k1, k2 = coord[d0], coord[d1], coord[d2]
        us = pl.ds(u0, nu)
        if stage == RS1:
            src, dst, dev = s1.at[p, us, pl.ds(pl.multiple_of((1 - k1) * 16, 16), 16)], r1.at[p, us], chip_peer(d1)
        elif stage == RS2:
            src, dst, dev = s2.at[p, us, pl.ds(pl.multiple_of((1 - k2) * 8, 8), 8)], r2.at[p, us], chip_peer(d2)
        else:
            base = core * 64
            if stage == AG0:
                off, n, dev = base + k0 * 32 + k1 * 16 + k2 * 8, 8, chip_peer(d2)
            elif stage == AG1:
                off, n, dev = base + k0 * 32 + k1 * 16, 16, chip_peer(d1)
            elif stage == AG2:
                off, n, dev = base + k0 * 32, 32, chip_peer(d0)
            elif stage == DDA:
                off, n, dev = base + k0 * 32, 32, partner
            else:
                off, n, dev = base + (1 - k0) * 32, 32, partner
            src = full.at[p, us, pl.ds(pl.multiple_of(off, 8), n)]
            dst = src
        return pltpu.make_async_remote_copy(
            src_ref=src, dst_ref=dst, send_sem=st_send.at[stage, gi], recv_sem=st_recv.at[stage, gi],
            device_id=dev, device_id_type=MESH)

    def unit_slice(mat, u):
        if mat == 2:
            return pl.ds(u * 128, 128), pl.ds(0, 256)
        return pl.ds((u % 2) * 128, 128), pl.ds((u // 2) * 256, 256)

    def make_delta(p, lay):
        mat = PIECES[p][1]
        wr, gr = (w1, g1) if mat == 1 else (w2, g2)
        for u in range(8):
            rows, cols = unit_slice(mat, u)
            delta[p, u] = (gr[lay, rows, cols] - wr[0, lay, rows, cols]).astype(BF16)
        for gi in range(3 * p, 3 * p + 3):
            for cp in rs0_copies(gi):
                cp.start()

    def forward(k):
        hid[...] = xb[k].astype(F32)

        def layer(lay, _):
            h_bf = hid[...].astype(BF16)
            hb[lay] = h_bf
            acc = hid[...]
            for j in range(NB):
                cols = slice(j * D, (j + 1) * D)
                a = dot(h_bf, w1b[lay, :, cols], 1, 0)
                u, dg = gelu_pair(a)
                u_bf = u.astype(BF16)
                ub[lay, :, cols] = u_bf
                du[lay, :, cols] = dg
                acc = acc + dot(u_bf, w2b[lay, cols, :], 1, 0)
            hid[...] = acc
            return 0

        lax.fori_loop(0, L, layer, 0)

    def backward(k):
        frag = k // 2
        dhid[...] = (2.0 / (B * D)) * (hid[...] - yb[k].astype(F32))

        def layer(li, _):
            lay = (L - 1) - li
            e = dhid[...].astype(BF16)
            h_bf = hb[lay]
            acc = dhid[...]
            for j in range(NB):
                cols = slice(j * D, (j + 1) * D)
                d_u = dot(e, w2b[lay, cols, :], 1, 1)
                c = (du[lay, :, cols] * d_u).astype(BF16)
                g_w2 = dot(ub[lay, :, cols], e, 0, 0)
                new2 = w2[0, lay, cols, :] - INNER_LR * g_w2
                w2[0, lay, cols, :] = new2
                w2b[lay, cols, :] = new2.astype(BF16)
                acc = acc + dot(c, w1b[lay, :, cols], 1, 1)
                g_w1 = dot(h_bf, c, 0, 0)
                new1 = w1[0, lay, :, cols] - INNER_LR * g_w1
                w1[0, lay, :, cols] = new1
                w1b[lay, :, cols] = new1.astype(BF16)
            dhid[...] = acc
            even = lax.rem(k, 2) == 0
            for p in (0, 2):
                @pl.when(even & (lay == 2 * frag + PIECES[p][0]))
                def _(p=p):
                    make_delta(p, lay)
                    make_delta(p + 1, lay)
            return 0

        lax.fori_loop(0, L, layer, 0)

    def sync(frag):
        for gi, (p, c, u0, nu) in enumerate(GROUPS):
            d0, d1, d2 = dims_of(c)
            k0 = coord[d0]
            rows = pl.ds(pl.multiple_of(core * 64 + k0 * 32, 32), 32)
            for cp in rs0_copies(gi):
                cp.wait_recv()
            for u in range(u0, u0 + nu):
                s1[p, u] = ((delta[p, u, rows, :].astype(F32) + raw[0, p, u].astype(F32))
                            + (raw[1, p, u].astype(F32) + raw[2, p, u].astype(F32)))
            stage_copy(RS1, gi).start()
        for gi, (p, c, u0, nu) in enumerate(GROUPS):
            d0, d1, d2 = dims_of(c)
            k1 = coord[d1]
            rows = pl.ds(pl.multiple_of(k1 * 16, 16), 16)
            stage_copy(RS1, gi).wait_recv()
            for u in range(u0, u0 + nu):
                s2[p, u] = s1[p, u, rows, :] + r1[p, u]
            stage_copy(RS2, gi).start()
        for gi, (p, c, u0, nu) in enumerate(GROUPS):
            d0, d1, d2 = dims_of(c)
            k0, k1, k2 = coord[d0], coord[d1], coord[d2]
            rows = pl.ds(pl.multiple_of(k2 * 8, 8), 8)
            out_rows = pl.ds(pl.multiple_of(core * 64 + k0 * 32 + k1 * 16 + k2 * 8, 8), 8)
            stage_copy(RS2, gi).wait_recv()
            for u in range(u0, u0 + nu):
                full[p, u, out_rows, :] = s2[p, u, rows, :] + r2[p, u]
            stage_copy(AG0, gi).start()
        for gi in range(12):
            stage_copy(AG0, gi).wait_recv()
            stage_copy(AG1, gi).start()
        for gi in range(12):
            stage_copy(AG1, gi).wait_recv()
            stage_copy(AG2, gi).start()
            stage_copy(DDA, gi).start()
        for gi in range(12):
            stage_copy(AG2, gi).wait_recv()
            stage_copy(DDB, gi).start()
        for p, (part, mat) in enumerate(PIECES):
            for gi in range(3 * p, 3 * p + 3):
                stage_copy(DDA, gi).wait_recv()
                stage_copy(DDB, gi).wait_recv()
            lay = 2 * frag + part
            wr, wbr, gr, mr = (w1, w1b, g1, m1) if mat == 1 else (w2, w2b, g2, m2)
            for u in range(8):
                rows, cols = unit_slice(mat, u)
                mean = full[p, u] * (1.0 / N_ALL)
                mom = OUTER_MOM * mr[lay, rows, cols] + mean
                glob = gr[lay, rows, cols] - OUTER_LR * (OUTER_MOM * mom + mean)
                mr[lay, rows, cols] = mom
                gr[lay, rows, cols] = glob
                merged = MERGE_MIX * wr[0, lay, rows, cols] + (1.0 - MERGE_MIX) * glob
                wr[0, lay, rows, cols] = merged
                wbr[lay, rows, cols] = merged.astype(BF16)
        for gi in range(12):
            for cp in rs0_copies(gi):
                cp.wait_send()
            for stage in range(7):
                stage_copy(stage, gi).wait_send()

    def step(k, _):
        forward(k)
        backward(k)

        @pl.when(lax.rem(k, 2) == 1)
        def _():
            sync(k // 2)
        return 0

    lax.fori_loop(0, H, step, 0)


def write_body(*refs):
    srcs, dsts, sem = refs[:6], refs[6:12], refs[12]
    cps = []
    for i in range(6):
        for lay in range(L):
            src = srcs[i].at[0, lay] if i < 2 else srcs[i].at[lay]
            dst = dsts[i].at[0, lay] if i < 2 else dsts[i].at[lay]
            cps.append(pltpu.make_async_copy(src, dst, sem.at[i, lay]))
    for cp in cps:
        cp.start()
    for cp in cps:
        cp.wait()


def solution(mesh):
    def device_fn(w1_loc, w2_loc, w1_glb, w2_glb, mom1, mom2, x_loc, y_loc):
        arrays = (w1_loc, w2_loc, w1_glb, w2_glb, mom1, mom2)
        shapes = [jax.ShapeDtypeStruct(a.shape, F32) for a in arrays]
        dma = pltpu.SemaphoreType.DMA
        work = pl.pallas_call(
            main_body,
            out_shape=shapes,
            in_specs=[ANY] * 8,
            out_specs=[VMEM] * 6,
            scratch_shapes=[
                pltpu.VMEM((H, B, D), BF16), pltpu.VMEM((H, B, D), BF16),
                pltpu.VMEM((L, D, FF), BF16), pltpu.VMEM((L, FF, D), BF16),
                pltpu.VMEM((L, B, D), BF16), pltpu.VMEM((L, B, FF), BF16), pltpu.VMEM((L, B, FF), F32),
                pltpu.VMEM((B, D), F32), pltpu.VMEM((B, D), F32),
                pltpu.VMEM((4, 8, 128, 256), BF16), pltpu.VMEM((3, 4, 8, 32, 256), BF16),
                pltpu.VMEM((4, 8, 32, 256), F32), pltpu.VMEM((4, 8, 16, 256), F32),
                pltpu.VMEM((4, 8, 16, 256), F32), pltpu.VMEM((4, 8, 8, 256), F32),
                pltpu.VMEM((4, 8, 128, 256), F32),
                dma((26,)), dma((12, 3)), dma((12, 3)), dma((7, 12)), dma((7, 12)),
            ],
            compiler_params=pltpu.CompilerParams(
                collective_id=0, has_side_effects=True, vmem_limit_bytes=28 * 2**20),
            name='diloco_round',
        )(*arrays, x_loc, y_loc)
        outs = pl.pallas_call(
            write_body,
            out_shape=shapes,
            in_specs=[VMEM] * 6,
            out_specs=[ANY] * 6,
            scratch_shapes=[dma((6, L))],
            compiler_params=pltpu.CompilerParams(vmem_limit_bytes=2 * 2**20),
            name='write_out',
        )(*work)
        return tuple(outs)

    local_spec = P(('shard', 'worker'))
    whole_spec = P()
    return jax.shard_map(device_fn, mesh=mesh, in_specs=(local_spec, local_spec, whole_spec, whole_spec, whole_spec, whole_spec, local_spec, local_spec), out_specs=(local_spec, local_spec, whole_spec, whole_spec, whole_spec, whole_spec), check_vma=False)
```

```python
import jax
import jax.numpy as jnp
from jax import lax
from jax.experimental import pallas as pl
from jax.experimental.pallas import tpu as pltpu
from jax.sharding import PartitionSpec as P

OUTER_LR = 0.7
OUTER_MOM = 0.9
MERGE_MIX = 0.5

L = 4
H = 4
D = 256
FF = 1024
B = 128
NB = FF // D
INNER_LR = 2.0 * D / (FF * L)
N_ALL = 16
F32 = jnp.float32
BF16 = jnp.bfloat16
MESH = pl.DeviceIdType.MESH
HBM = pl.BlockSpec(memory_space=pltpu.HBM)
VMEM = pl.BlockSpec(memory_space=pltpu.VMEM)

PIECES = ((1, 2), (1, 1), (0, 2), (0, 1))
COLOR_UNITS = ((3, 3, 2), (3, 2, 3), (2, 3, 3), (3, 3, 2))
GROUPS = []
for piece_idx in range(4):
    first_unit = 0
    for color in range(3):
        GROUPS.append((piece_idx, color, first_unit, COLOR_UNITS[piece_idx][color]))
        first_unit += COLOR_UNITS[piece_idx][color]
RS1, X2, AG1, AG2, DDA, DDB = range(6)


def dot(a, b, ca, cb):
    return lax.dot_general(a, b, (((ca,), (cb,)), ((), ())), preferred_element_type=F32)


def gelu_pair(a):
    k0 = 0.7978845608028654
    k1 = k0 * 0.044715
    a2 = a * a
    t = jnp.tanh(a * (k0 + k1 * a2))
    h = 0.5 + 0.5 * t
    u = a * h
    du = h + (u * (1.0 - h)) * (2.0 * k0 + (6.0 * k1) * a2)
    return u, du


def main_body(w1_in, w2_in, g1_in, g2_in, m1_in, m2_in, x_in, y_in,
              w1, w2, g1, g2, m1, m2,
              xb, yb, w1b, w2b, hb, ub, du, hid, dhid,
              delta, raw, s1, r1, s2, r2, full,
              ld_sem, s0_send, s0_recv, st_send, st_recv):
    zc = lax.axis_index('shard')
    wk = lax.axis_index('worker')
    core = lax.rem(wk, 2)
    xc = lax.rem(wk // 2, 2)
    yc = wk // 4
    coord = (xc, yc, zc)

    def chip_peer(dim, same_core=True):
        w = wk
        s = zc
        if dim == 0:
            w = wk + 2 - 4 * xc
        elif dim == 1:
            w = wk + 4 - 8 * yc
        elif dim == 2:
            s = 1 - zc
        if not same_core:
            w = w + 1 - 2 * core
        return (s, w)

    partner = chip_peer(3, False)

    bar = pltpu.get_barrier_semaphore()
    pl.semaphore_signal(bar, inc=1, device_id=partner, device_id_type=MESH)
    for dim in range(3):
        for same in (True, False):
            pl.semaphore_signal(bar, inc=1, device_id=chip_peer(dim, same), device_id_type=MESH)

    def w_load(lay):
        return (pltpu.make_async_copy(w1_in.at[0, lay], w1.at[0, lay], ld_sem.at[lay]),
                pltpu.make_async_copy(w2_in.at[0, lay], w2.at[0, lay], ld_sem.at[L + lay]))

    def g_load(mat, lay):
        if mat == 1:
            return pltpu.make_async_copy(g1_in.at[lay], g1.at[lay], ld_sem.at[2 * L + lay])
        return pltpu.make_async_copy(g2_in.at[lay], g2.at[lay], ld_sem.at[3 * L + lay])

    def m_load(mat, lay):
        if mat == 1:
            return pltpu.make_async_copy(m1_in.at[lay], m1.at[lay], ld_sem.at[4 * L + lay])
        return pltpu.make_async_copy(m2_in.at[lay], m2.at[lay], ld_sem.at[5 * L + lay])

    x_load = pltpu.make_async_copy(x_in.at[0], xb, ld_sem.at[6 * L])
    y_load = pltpu.make_async_copy(y_in.at[0], yb, ld_sem.at[6 * L + 1])
    x_load.start()
    for cp in w_load(0):
        cp.start()
    y_load.start()
    for lay in range(1, L):
        for cp in w_load(lay):
            cp.start()
    for lay in range(L):
        for mat in (1, 2):
            g_load(mat, lay).start()
    for lay in range(L):
        for mat in (1, 2):
            m_load(mat, lay).start()
    x_load.wait()
    y_load.wait()

    def dims_of(color_idx):
        return color_idx % 3, (color_idx + 1) % 3, (color_idx + 2) % 3

    def rs0_copies(gi):
        p, c, u0, nu = GROUPS[gi]
        d0 = dims_of(c)[0]
        k0 = coord[d0]
        us = pl.ds(u0, nu)
        other = 1 - core

        def rows(tc, blk):
            return pl.ds(pl.multiple_of(tc * 64 + blk * 32, 32), 32)

        out = []
        for idx, (tc, blk, dev) in enumerate(((other, k0, partner),
                                               (core, 1 - k0, chip_peer(d0, True)),
                                               (other, 1 - k0, chip_peer(d0, False)))):
            out.append(pltpu.make_async_remote_copy(
                src_ref=delta.at[p, us, rows(tc, blk)], dst_ref=raw.at[idx, p, us],
                send_sem=s0_send.at[gi, idx], recv_sem=s0_recv.at[gi, idx],
                device_id=dev, device_id_type=MESH))
        return out

    def stage_copy(stage, gi):
        p, c, u0, nu = GROUPS[gi]
        d0, d1, d2 = dims_of(c)
        k0, k1, k2 = coord[d0], coord[d1], coord[d2]
        us = pl.ds(u0, nu)
        if stage == RS1:
            src, dst, dev = s1.at[p, us, pl.ds(pl.multiple_of((1 - k1) * 16, 16), 16)], r1.at[p, us], chip_peer(d1)
        elif stage == X2:
            src, dst, dev = s2.at[p, us], r2.at[p, us], chip_peer(d2)
        else:
            base = core * 64
            if stage == AG1:
                off, n, dev = base + k0 * 32 + k1 * 16, 16, chip_peer(d1)
            elif stage == AG2:
                off, n, dev = base + k0 * 32, 32, chip_peer(d0)
            elif stage == DDA:
                off, n, dev = base + k0 * 32, 32, partner
            else:
                off, n, dev = base + (1 - k0) * 32, 32, partner
            src = full.at[p, us, pl.ds(pl.multiple_of(off, 16), n)]
            dst = src
        return pltpu.make_async_remote_copy(
            src_ref=src, dst_ref=dst, send_sem=st_send.at[stage, gi], recv_sem=st_recv.at[stage, gi],
            device_id=dev, device_id_type=MESH)

    def unit_slice(mat, u):
        if mat == 2:
            return pl.ds(u * 128, 128), pl.ds(0, 256)
        return pl.ds((u % 2) * 128, 128), pl.ds((u // 2) * 256, 256)

    def make_delta(p, lay):
        mat = PIECES[p][1]
        wr, gr = (w1, g1) if mat == 1 else (w2, g2)
        g_load(mat, lay).wait()
        for u in range(8):
            rows, cols = unit_slice(mat, u)
            delta[p, u] = (gr[lay, rows, cols] - wr[0, lay, rows, cols]).astype(BF16)
        for gi in range(3 * p, 3 * p + 3):
            for cp in rs0_copies(gi):
                cp.start()

    def forward(k):
        hid[...] = xb[k].astype(F32)

        def layer(lay, _):
            @pl.when(k == 0)
            def _():
                for cp in w_load(lay):
                    cp.wait()

                def cast(i, _):
                    rows = pl.ds(pl.multiple_of(i * 64, 64), 64)
                    w1b[lay, rows, :] = w1[0, lay, rows, :].astype(BF16)
                    rows = pl.ds(pl.multiple_of(i * 256, 256), 256)
                    w2b[lay, rows, :] = w2[0, lay, rows, :].astype(BF16)
                    return 0

                lax.fori_loop(0, 4, cast, 0)

            h_bf = hid[...].astype(BF16)
            hb[lay] = h_bf
            acc = hid[...]
            for j in range(NB):
                cols = slice(j * D, (j + 1) * D)
                a = dot(h_bf, w1b[lay, :, cols], 1, 0)
                u, dg = gelu_pair(a)
                u_bf = u.astype(BF16)
                ub[lay, :, cols] = u_bf
                du[lay, :, cols] = dg
                acc = acc + dot(u_bf, w2b[lay, cols, :], 1, 0)
            hid[...] = acc
            return 0

        lax.fori_loop(0, L, layer, 0)

    def backward(k):
        frag = k // 2
        dhid[...] = (2.0 / (B * D)) * (hid[...] - yb[k].astype(F32))

        def layer(li, _):
            lay = (L - 1) - li
            e = dhid[...].astype(BF16)
            h_bf = hb[lay]
            acc = dhid[...]
            for j in range(NB):
                cols = slice(j * D, (j + 1) * D)
                d_u = dot(e, w2b[lay, cols, :], 1, 1)
                c = (du[lay, :, cols] * d_u).astype(BF16)
                g_w2 = dot(ub[lay, :, cols], e, 0, 0)
                new2 = w2[0, lay, cols, :] - INNER_LR * g_w2
                w2[0, lay, cols, :] = new2
                w2b[lay, cols, :] = new2.astype(BF16)
                acc = acc + dot(c, w1b[lay, :, cols], 1, 1)
                g_w1 = dot(h_bf, c, 0, 0)
                new1 = w1[0, lay, :, cols] - INNER_LR * g_w1
                w1[0, lay, :, cols] = new1
                w1b[lay, :, cols] = new1.astype(BF16)
            dhid[...] = acc
            even = lax.rem(k, 2) == 0
            for p in (0, 2):
                @pl.when(even & (lay == 2 * frag + PIECES[p][0]))
                def _(p=p):
                    make_delta(p, lay)
                    make_delta(p + 1, lay)
            return 0

        lax.fori_loop(0, L, layer, 0)

    def sync(frag):
        for gi, (p, c, u0, nu) in enumerate(GROUPS):
            d0, d1, d2 = dims_of(c)
            k0 = coord[d0]
            rows = pl.ds(pl.multiple_of(core * 64 + k0 * 32, 32), 32)
            for cp in rs0_copies(gi):
                cp.wait_recv()
            for u in range(u0, u0 + nu):
                s1[p, u] = ((delta[p, u, rows, :].astype(F32) + raw[0, p, u].astype(F32))
                            + (raw[1, p, u].astype(F32) + raw[2, p, u].astype(F32)))
            stage_copy(RS1, gi).start()
        for gi, (p, c, u0, nu) in enumerate(GROUPS):
            d0, d1, d2 = dims_of(c)
            k1 = coord[d1]
            rows = pl.ds(pl.multiple_of(k1 * 16, 16), 16)
            stage_copy(RS1, gi).wait_recv()
            for u in range(u0, u0 + nu):
                s2[p, u] = s1[p, u, rows, :] + r1[p, u]
            stage_copy(X2, gi).start()
        for gi, (p, c, u0, nu) in enumerate(GROUPS):
            d0, d1, d2 = dims_of(c)
            rows = pl.ds(pl.multiple_of(core * 64 + coord[d0] * 32 + coord[d1] * 16, 16), 16)
            stage_copy(X2, gi).wait_recv()
            for u in range(u0, u0 + nu):
                full[p, u, rows, :] = s2[p, u] + r2[p, u]
            stage_copy(AG1, gi).start()
        for gi in range(12):
            stage_copy(AG1, gi).wait_recv()
            stage_copy(AG2, gi).start()
            stage_copy(DDA, gi).start()
        for gi in range(12):
            stage_copy(AG2, gi).wait_recv()
            stage_copy(DDB, gi).start()
        for p, (part, mat) in enumerate(PIECES):
            for gi in range(3 * p, 3 * p + 3):
                stage_copy(DDA, gi).wait_recv()
                stage_copy(DDB, gi).wait_recv()
            lay = 2 * frag + part
            wr, wbr, gr, mr = (w1, w1b, g1, m1) if mat == 1 else (w2, w2b, g2, m2)
            m_load(mat, lay).wait()
            for u in range(8):
                rows, cols = unit_slice(mat, u)
                mean = full[p, u] * (1.0 / N_ALL)
                mom = OUTER_MOM * mr[lay, rows, cols] + mean
                glob = gr[lay, rows, cols] - OUTER_LR * (OUTER_MOM * mom + mean)
                mr[lay, rows, cols] = mom
                gr[lay, rows, cols] = glob
                merged = MERGE_MIX * wr[0, lay, rows, cols] + (1.0 - MERGE_MIX) * glob
                wr[0, lay, rows, cols] = merged
                wbr[lay, rows, cols] = merged.astype(BF16)
        for gi in range(12):
            for cp in rs0_copies(gi):
                cp.wait_send()
            for stage in range(6):
                stage_copy(stage, gi).wait_send()

    def step(k, _):
        forward(k)

        @pl.when(k == 0)
        def _():
            pl.semaphore_wait(bar, 7)

        backward(k)

        @pl.when(lax.rem(k, 2) == 1)
        def _():
            sync(k // 2)
        return 0

    lax.fori_loop(0, H, step, 0)


def write_body(*refs):
    srcs, dsts, sem = refs[:6], refs[6:12], refs[12]
    cps = []
    for i in range(6):
        for lay in range(L):
            src = srcs[i].at[0, lay] if i < 2 else srcs[i].at[lay]
            dst = dsts[i].at[0, lay] if i < 2 else dsts[i].at[lay]
            cps.append(pltpu.make_async_copy(src, dst, sem.at[i, lay]))
    for cp in cps:
        cp.start()
    for cp in cps:
        cp.wait()


def solution(mesh):
    def device_fn(w1_loc, w2_loc, w1_glb, w2_glb, mom1, mom2, x_loc, y_loc):
        arrays = (w1_loc, w2_loc, w1_glb, w2_glb, mom1, mom2)
        shapes = [jax.ShapeDtypeStruct(a.shape, F32) for a in arrays]
        dma = pltpu.SemaphoreType.DMA
        work = pl.pallas_call(
            main_body,
            out_shape=shapes,
            in_specs=[HBM] * 8,
            out_specs=[VMEM] * 6,
            scratch_shapes=[
                pltpu.VMEM((H, B, D), BF16), pltpu.VMEM((H, B, D), BF16),
                pltpu.VMEM((L, D, FF), BF16), pltpu.VMEM((L, FF, D), BF16),
                pltpu.VMEM((L, B, D), BF16), pltpu.VMEM((L, B, FF), BF16), pltpu.VMEM((L, B, FF), F32),
                pltpu.VMEM((B, D), F32), pltpu.VMEM((B, D), F32),
                pltpu.VMEM((4, 8, 128, 256), BF16), pltpu.VMEM((3, 4, 8, 32, 256), BF16),
                pltpu.VMEM((4, 8, 32, 256), F32), pltpu.VMEM((4, 8, 16, 256), F32),
                pltpu.VMEM((4, 8, 16, 256), F32), pltpu.VMEM((4, 8, 16, 256), F32),
                pltpu.VMEM((4, 8, 128, 256), F32),
                dma((26,)), dma((12, 3)), dma((12, 3)), dma((6, 12)), dma((6, 12)),
            ],
            compiler_params=pltpu.CompilerParams(
                collective_id=0, has_side_effects=True, vmem_limit_bytes=28 * 2**20),
            name='diloco_round',
        )(*[pltpu.with_memory_space_constraint(a, pltpu.HBM) for a in (*arrays, x_loc, y_loc)])
        outs = pl.pallas_call(
            write_body,
            out_shape=shapes,
            in_specs=[VMEM] * 6,
            out_specs=[HBM] * 6,
            scratch_shapes=[dma((6, L))],
            compiler_params=pltpu.CompilerParams(vmem_limit_bytes=2 * 2**20),
            name='write_out',
        )(*work)
        return tuple(outs)

    local_spec = P(('shard', 'worker'))
    whole_spec = P()
    return jax.shard_map(device_fn, mesh=mesh, in_specs=(local_spec, local_spec, whole_spec, whole_spec, whole_spec, whole_spec, local_spec, local_spec), out_specs=(local_spec, local_spec, whole_spec, whole_spec, whole_spec, whole_spec), check_vma=False)
```

```python
import jax
import jax.numpy as jnp
from jax import lax
from jax.experimental import pallas as pl
from jax.experimental.pallas import tpu as pltpu
from jax.sharding import PartitionSpec as P

OUTER_LR = 0.7
OUTER_MOM = 0.9
MERGE_MIX = 0.5

L = 4
H = 4
D = 256
FF = 1024
B = 128
NB = FF // D
INNER_LR = 2.0 * D / (FF * L)
N_ALL = 16
F32 = jnp.float32
BF16 = jnp.bfloat16
MESH = pl.DeviceIdType.MESH
HBM = pl.BlockSpec(memory_space=pltpu.HBM)
VMEM = pl.BlockSpec(memory_space=pltpu.VMEM)

PIECES = ((1, 2), (1, 1), (0, 2), (0, 1))
COLOR_UNITS = ((3, 3, 2), (3, 2, 3), (2, 3, 3), (3, 3, 2))
GROUPS = []
for piece_idx in range(4):
    first_unit = 0
    for color in range(3):
        GROUPS.append((piece_idx, color, first_unit, COLOR_UNITS[piece_idx][color]))
        first_unit += COLOR_UNITS[piece_idx][color]
GATHER_ORDER = (0, 2, 3, 1)
RS1, X2, AG1, AG2, DDA, DDB = range(6)


def dot(a, b, ca, cb):
    return lax.dot_general(a, b, (((ca,), (cb,)), ((), ())), preferred_element_type=F32)


def gelu_pair(a):
    k0 = 0.7978845608028654
    k1 = k0 * 0.044715
    a2 = a * a
    t = jnp.tanh(a * (k0 + k1 * a2))
    h = 0.5 + 0.5 * t
    u = a * h
    du = h + (u * (1.0 - h)) * (2.0 * k0 + (6.0 * k1) * a2)
    return u, du


def main_body(w1_in, w2_in, g1_in, g2_in, m1_in, m2_in, x_in, y_in,
              w1, w2, g1, g2, m1, m2,
              xb, yb, w1b, w2b, hb, ub, du, hid, dhid, eb, cb,
              delta, raw, s1, r1, s2, r2, full,
              ld_sem, s0_send, s0_recv, st_send, st_recv):
    zc = lax.axis_index('shard')
    wk = lax.axis_index('worker')
    core = lax.rem(wk, 2)
    xc = lax.rem(wk // 2, 2)
    yc = wk // 4
    coord = (xc, yc, zc)

    def chip_peer(dim, same_core=True):
        w = wk
        s = zc
        if dim == 0:
            w = wk + 2 - 4 * xc
        elif dim == 1:
            w = wk + 4 - 8 * yc
        elif dim == 2:
            s = 1 - zc
        if not same_core:
            w = w + 1 - 2 * core
        return (s, w)

    partner = chip_peer(3, False)

    bar = pltpu.get_barrier_semaphore()
    pl.semaphore_signal(bar, inc=1, device_id=partner, device_id_type=MESH)
    for dim in range(3):
        for same in (True, False):
            pl.semaphore_signal(bar, inc=1, device_id=chip_peer(dim, same), device_id_type=MESH)

    def w_load(lay):
        return (pltpu.make_async_copy(w1_in.at[0, lay], w1.at[0, lay], ld_sem.at[lay]),
                pltpu.make_async_copy(w2_in.at[0, lay], w2.at[0, lay], ld_sem.at[L + lay]))

    def g_load(mat, lay):
        if mat == 1:
            return pltpu.make_async_copy(g1_in.at[lay], g1.at[lay], ld_sem.at[2 * L + lay])
        return pltpu.make_async_copy(g2_in.at[lay], g2.at[lay], ld_sem.at[3 * L + lay])

    def m_load(mat, lay):
        if mat == 1:
            return pltpu.make_async_copy(m1_in.at[lay], m1.at[lay], ld_sem.at[4 * L + lay])
        return pltpu.make_async_copy(m2_in.at[lay], m2.at[lay], ld_sem.at[5 * L + lay])

    x_load = pltpu.make_async_copy(x_in.at[0], xb, ld_sem.at[6 * L])
    y_load = pltpu.make_async_copy(y_in.at[0], yb, ld_sem.at[6 * L + 1])
    x_load.start()
    for cp in w_load(0):
        cp.start()
    y_load.start()
    for lay in range(1, L):
        for cp in w_load(lay):
            cp.start()
    for lay in range(L):
        for mat in (1, 2):
            g_load(mat, lay).start()
    for lay in range(L):
        for mat in (1, 2):
            m_load(mat, lay).start()
    x_load.wait()
    y_load.wait()

    def dims_of(color_idx):
        return color_idx % 3, (color_idx + 1) % 3, (color_idx + 2) % 3

    def rs0_copies(gi):
        p, c, u0, nu = GROUPS[gi]
        d0 = dims_of(c)[0]
        k0 = coord[d0]
        us = pl.ds(u0, nu)
        other = 1 - core

        def rows(tc, blk):
            return pl.ds(pl.multiple_of(tc * 64 + blk * 32, 32), 32)

        out = []
        for idx, (tc, blk, dev) in enumerate(((other, k0, partner),
                                               (core, 1 - k0, chip_peer(d0, True)),
                                               (other, 1 - k0, chip_peer(d0, False)))):
            out.append(pltpu.make_async_remote_copy(
                src_ref=delta.at[p, us, rows(tc, blk)], dst_ref=raw.at[idx, p, us],
                send_sem=s0_send.at[gi, idx], recv_sem=s0_recv.at[gi, idx],
                device_id=dev, device_id_type=MESH))
        return out

    def stage_copy(stage, gi):
        p, c, u0, nu = GROUPS[gi]
        d0, d1, d2 = dims_of(c)
        k0, k1, k2 = coord[d0], coord[d1], coord[d2]
        us = pl.ds(u0, nu)
        if stage == RS1:
            src, dst, dev = s1.at[p, us, pl.ds(pl.multiple_of((1 - k1) * 16, 16), 16)], r1.at[p, us], chip_peer(d1)
        elif stage == X2:
            src, dst, dev = s2.at[p, us], r2.at[p, us], chip_peer(d2)
        else:
            base = core * 64
            if stage == AG1:
                off, n, dev = base + k0 * 32 + k1 * 16, 16, chip_peer(d1)
            elif stage == AG2:
                off, n, dev = base + k0 * 32, 32, chip_peer(d0)
            elif stage == DDA:
                off, n, dev = base + k0 * 32, 32, partner
            else:
                off, n, dev = base + (1 - k0) * 32, 32, partner
            src = full.at[p, us, pl.ds(pl.multiple_of(off, 16), n)]
            dst = src
        return pltpu.make_async_remote_copy(
            src_ref=src, dst_ref=dst, send_sem=st_send.at[stage, gi], recv_sem=st_recv.at[stage, gi],
            device_id=dev, device_id_type=MESH)

    def unit_slice(mat, u):
        if mat == 2:
            return pl.ds(u * 128, 128), pl.ds(0, 256)
        return pl.ds((u % 2) * 128, 128), pl.ds((u // 2) * 256, 256)

    def make_delta(p, lay):
        mat = PIECES[p][1]
        wr, gr = (w1, g1) if mat == 1 else (w2, g2)
        g_load(mat, lay).wait()
        for u in range(8):
            rows, cols = unit_slice(mat, u)
            delta[p, u] = (gr[lay, rows, cols] - wr[0, lay, rows, cols]).astype(BF16)
        for gi in range(3 * p, 3 * p + 3):
            for cp in rs0_copies(gi):
                cp.start()

    def cast_layer(lay):
        for cp in w_load(lay):
            cp.wait()

        def cast(i, _):
            rows = pl.ds(pl.multiple_of(i * 64, 64), 64)
            w1b[lay, rows, :] = w1[0, lay, rows, :].astype(BF16)
            rows = pl.ds(pl.multiple_of(i * 256, 256), 256)
            w2b[lay, rows, :] = w2[0, lay, rows, :].astype(BF16)
            return 0

        lax.fori_loop(0, 4, cast, 0)

    def forward(k, before_layer_1=None):
        hid[...] = xb[k].astype(F32)

        def layer(lay, _):
            if k == 0:
                cast_layer(lay)
            if before_layer_1 is not None:
                pl.when(lay == 1)(before_layer_1)
            h_bf = hid[...].astype(BF16)
            hb[lay] = h_bf
            acc = hid[...]
            for j in range(NB):
                cols = slice(j * D, (j + 1) * D)
                a = dot(h_bf, w1b[lay, :, cols], 1, 0)
                u, dg = gelu_pair(a)
                u_bf = u.astype(BF16)
                ub[lay, :, cols] = u_bf
                du[lay, :, cols] = dg
                acc = acc + dot(u_bf, w2b[lay, cols, :], 1, 0)
            hid[...] = acc
            return 0

        lax.fori_loop(0, L, layer, 0)

    def loss_grad(k):
        dhid[...] = (2.0 / (B * D)) * (hid[...] - yb[k].astype(F32))

    def update2(lay, cols, u_j, e):
        new2 = w2[0, lay, cols, :] - INNER_LR * dot(u_j, e, 0, 0)
        w2[0, lay, cols, :] = new2
        w2b[lay, cols, :] = new2.astype(BF16)

    def update1(lay, cols, h_bf, c):
        new1 = w1[0, lay, :, cols] - INNER_LR * dot(h_bf, c, 0, 0)
        w1[0, lay, :, cols] = new1
        w1b[lay, :, cols] = new1.astype(BF16)

    def back_full(lay):
        e = dhid[...].astype(BF16)
        h_bf = hb[lay]
        acc = dhid[...]
        for j in range(NB):
            cols = slice(j * D, (j + 1) * D)
            d_u = dot(e, w2b[lay, cols, :], 1, 1)
            c = (du[lay, :, cols] * d_u).astype(BF16)
            update2(lay, cols, ub[lay, :, cols], e)
            acc = acc + dot(c, w1b[lay, :, cols], 1, 1)
            update1(lay, cols, h_bf, c)
        dhid[...] = acc

    def back_chain(lay):
        e = dhid[...].astype(BF16)
        eb[lay - 2] = e
        acc = dhid[...]
        for j in range(NB):
            cols = slice(j * D, (j + 1) * D)
            d_u = dot(e, w2b[lay, cols, :], 1, 1)
            c = (du[lay, :, cols] * d_u).astype(BF16)
            cb[lay - 2, :, cols] = c
            acc = acc + dot(c, w1b[lay, :, cols], 1, 1)
        dhid[...] = acc

    def back_weights(lay):
        e = eb[lay - 2]
        h_bf = hb[lay]
        for j in range(NB):
            cols = slice(j * D, (j + 1) * D)
            update2(lay, cols, ub[lay, :, cols], e)
            update1(lay, cols, h_bf, cb[lay - 2, :, cols])

    def reduce_stage1(p):
        for gi in range(3 * p, 3 * p + 3):
            _, c, u0, nu = GROUPS[gi]
            rows = pl.ds(pl.multiple_of(core * 64 + coord[dims_of(c)[0]] * 32, 32), 32)
            for cp in rs0_copies(gi):
                cp.wait_recv()
            for u in range(u0, u0 + nu):
                s1[p, u] = ((delta[p, u, rows, :].astype(F32) + raw[0, p, u].astype(F32))
                            + (raw[1, p, u].astype(F32) + raw[2, p, u].astype(F32)))
            stage_copy(RS1, gi).start()

    def reduce_stage2(p):
        for gi in range(3 * p, 3 * p + 3):
            _, c, u0, nu = GROUPS[gi]
            rows = pl.ds(pl.multiple_of(coord[dims_of(c)[1]] * 16, 16), 16)
            stage_copy(RS1, gi).wait_recv()
            for u in range(u0, u0 + nu):
                s2[p, u] = s1[p, u, rows, :] + r1[p, u]
            stage_copy(X2, gi).start()

    def reduce_stage3(p):
        for gi in range(3 * p, 3 * p + 3):
            _, c, u0, nu = GROUPS[gi]
            d0, d1, d2 = dims_of(c)
            rows = pl.ds(pl.multiple_of(core * 64 + coord[d0] * 32 + coord[d1] * 16, 16), 16)
            stage_copy(X2, gi).wait_recv()
            for u in range(u0, u0 + nu):
                full[p, u, rows, :] = s2[p, u] + r2[p, u]
            stage_copy(AG1, gi).start()

    def gather_stage2(p):
        for gi in range(3 * p, 3 * p + 3):
            stage_copy(AG1, gi).wait_recv()
            stage_copy(AG2, gi).start()
            stage_copy(DDA, gi).start()

    def gather_stage3(p):
        for gi in range(3 * p, 3 * p + 3):
            stage_copy(AG2, gi).wait_recv()
            stage_copy(DDB, gi).start()

    def outer_update(frag, p):
        part, mat = PIECES[p]
        lay = 2 * frag + part
        wr, wbr, gr, mr = (w1, w1b, g1, m1) if mat == 1 else (w2, w2b, g2, m2)
        m_load(mat, lay).wait()
        for gi in range(3 * p, 3 * p + 3):
            stage_copy(DDA, gi).wait_recv()
            stage_copy(DDB, gi).wait_recv()
        for u in range(8):
            rows, cols = unit_slice(mat, u)
            mean = full[p, u] * (1.0 / N_ALL)
            mom = OUTER_MOM * mr[lay, rows, cols] + mean
            glob = gr[lay, rows, cols] - OUTER_LR * (OUTER_MOM * mom + mean)
            mr[lay, rows, cols] = mom
            gr[lay, rows, cols] = glob
            merged = MERGE_MIX * wr[0, lay, rows, cols] + (1.0 - MERGE_MIX) * glob
            wr[0, lay, rows, cols] = merged
            wbr[lay, rows, cols] = merged.astype(BF16)

    last_piece = GATHER_ORDER[-1]

    def finish(frag):
        outer_update(frag, last_piece)
        for gi in range(12):
            for cp in rs0_copies(gi):
                cp.wait_send()
            for stage in range(6):
                stage_copy(stage, gi).wait_send()

    def sync(frag):
        reduce_stage1(3)
        for p in range(4):
            reduce_stage2(p)
        for p in range(4):
            reduce_stage3(p)
        for p in GATHER_ORDER:
            gather_stage2(p)
        prev = None
        for p in GATHER_ORDER:
            gather_stage3(p)
            if prev is not None:
                outer_update(frag, prev)
            prev = p

    def layers(lo, body):
        def run(i, _):
            body(i, lo - i)
            return 0
        return run

    def send_layer(lay, part):
        for p in (0, 2):
            @pl.when(part == PIECES[p][0])
            def _(p=p):
                make_delta(p, lay)
                make_delta(p + 1, lay)

    forward(0)
    pl.semaphore_wait(bar, 7)
    loss_grad(0)
    lax.fori_loop(0, 2, layers(3, lambda i, lay: back_chain(lay)), 0)

    def back_send_0(i, lay):
        back_full(lay)
        send_layer(lay, lay)

    lax.fori_loop(0, 2, layers(1, back_send_0), 0)
    lax.fori_loop(0, 2, layers(3, lambda i, lay: back_weights(lay)), 0)

    def back_hook(i, lay):
        back_full(lay)

        @pl.when(i == 0)
        def _():
            reduce_stage1(0)
            reduce_stage1(1)

        @pl.when(i == 2)
        def _():
            reduce_stage1(2)

    forward(1)
    loss_grad(1)
    lax.fori_loop(0, L, layers(3, back_hook), 0)
    sync(0)

    forward(2, lambda: finish(0))
    loss_grad(2)

    def back_send_1(i, lay):
        back_full(lay)
        pl.when(i < 2)(lambda: send_layer(lay, lay - 2))

    lax.fori_loop(0, L, layers(3, back_send_1), 0)

    forward(3)
    loss_grad(3)
    lax.fori_loop(0, L, layers(3, back_hook), 0)
    sync(1)
    finish(1)


def write_body(*refs):
    srcs, dsts, sem = refs[:6], refs[6:12], refs[12]
    cps = []
    for i in range(6):
        for lay in range(L):
            src = srcs[i].at[0, lay] if i < 2 else srcs[i].at[lay]
            dst = dsts[i].at[0, lay] if i < 2 else dsts[i].at[lay]
            cps.append(pltpu.make_async_copy(src, dst, sem.at[i, lay]))
    for cp in cps:
        cp.start()
    for cp in cps:
        cp.wait()


def solution(mesh):
    def device_fn(w1_loc, w2_loc, w1_glb, w2_glb, mom1, mom2, x_loc, y_loc):
        arrays = (w1_loc, w2_loc, w1_glb, w2_glb, mom1, mom2)
        shapes = [jax.ShapeDtypeStruct(a.shape, F32) for a in arrays]
        dma = pltpu.SemaphoreType.DMA
        work = pl.pallas_call(
            main_body,
            out_shape=shapes,
            in_specs=[HBM] * 8,
            out_specs=[VMEM] * 6,
            scratch_shapes=[
                pltpu.VMEM((H, B, D), BF16), pltpu.VMEM((H, B, D), BF16),
                pltpu.VMEM((L, D, FF), BF16), pltpu.VMEM((L, FF, D), BF16),
                pltpu.VMEM((L, B, D), BF16), pltpu.VMEM((L, B, FF), BF16), pltpu.VMEM((L, B, FF), F32),
                pltpu.VMEM((B, D), F32), pltpu.VMEM((B, D), F32),
                pltpu.VMEM((2, B, D), BF16), pltpu.VMEM((2, B, FF), BF16),
                pltpu.VMEM((4, 8, 128, 256), BF16), pltpu.VMEM((3, 4, 8, 32, 256), BF16),
                pltpu.VMEM((4, 8, 32, 256), F32), pltpu.VMEM((4, 8, 16, 256), F32),
                pltpu.VMEM((4, 8, 16, 256), F32), pltpu.VMEM((4, 8, 16, 256), F32),
                pltpu.VMEM((4, 8, 128, 256), F32),
                dma((26,)), dma((12, 3)), dma((12, 3)), dma((6, 12)), dma((6, 12)),
            ],
            compiler_params=pltpu.CompilerParams(
                collective_id=0, has_side_effects=True, vmem_limit_bytes=28 * 2**20),
            name='diloco_round',
        )(*[pltpu.with_memory_space_constraint(a, pltpu.HBM) for a in (*arrays, x_loc, y_loc)])
        outs = pl.pallas_call(
            write_body,
            out_shape=shapes,
            in_specs=[VMEM] * 6,
            out_specs=[HBM] * 6,
            scratch_shapes=[dma((6, L))],
            compiler_params=pltpu.CompilerParams(vmem_limit_bytes=2 * 2**20),
            name='write_out',
        )(*work)
        return tuple(outs)

    local_spec = P(('shard', 'worker'))
    whole_spec = P()
    return jax.shard_map(device_fn, mesh=mesh, in_specs=(local_spec, local_spec, whole_spec, whole_spec, whole_spec, whole_spec, local_spec, local_spec), out_specs=(local_spec, local_spec, whole_spec, whole_spec, whole_spec, whole_spec), check_vma=False)
```

```python
import jax
import jax.numpy as jnp
from jax import lax
from jax.experimental import pallas as pl
from jax.experimental.pallas import tpu as pltpu
from jax.sharding import PartitionSpec as P

OUTER_LR = 0.7
OUTER_MOM = 0.9
MERGE_MIX = 0.5

L = 4
H = 4
D = 256
FF = 1024
B = 128
NB = FF // D
INNER_LR = 2.0 * D / (FF * L)
N_ALL = 16
F32 = jnp.float32
BF16 = jnp.bfloat16
MESH = pl.DeviceIdType.MESH
HBM = pl.BlockSpec(memory_space=pltpu.HBM)
VMEM = pl.BlockSpec(memory_space=pltpu.VMEM)

PIECES = ((1, 2), (1, 1), (0, 2), (0, 1))
COLOR_UNITS = ((3, 3, 2), (3, 2, 3), (2, 3, 3), (3, 3, 2))
GROUPS = []
for piece_idx in range(4):
    first_unit = 0
    for color in range(3):
        GROUPS.append((piece_idx, color, first_unit, COLOR_UNITS[piece_idx][color]))
        first_unit += COLOR_UNITS[piece_idx][color]
GATHER_ORDER = (0, 2, 3, 1)
LAST = GATHER_ORDER[-1]
RS1, X2, AG1, AG2, DDA, DDB = range(6)


def dot(a, b, ca, cb):
    return lax.dot_general(a, b, (((ca,), (cb,)), ((), ())), preferred_element_type=F32)


def gelu_pair(a):
    k0 = 0.7978845608028654
    k1 = k0 * 0.044715
    a2 = a * a
    t = jnp.tanh(a * (k0 + k1 * a2))
    h = 0.5 + 0.5 * t
    u = a * h
    du = h + (u * (1.0 - h)) * (2.0 * k0 + (6.0 * k1) * a2)
    return u, du


def main_body(w1_in, w2_in, g1_in, g2_in, m1_in, m2_in, x_in, y_in,
              w1, w2, g1, g2, m1, m2,
              xb, yb, w1b, w2b, hb, ub, du, hid, dhid, eb, cb,
              delta, raw, s1, r1, s2, r2, full,
              ld_sem, s0_send, s0_recv, st_send, st_recv, un_send, un_recv):
    zc = lax.axis_index('shard')
    wk = lax.axis_index('worker')
    core = lax.rem(wk, 2)
    xc = lax.rem(wk // 2, 2)
    yc = wk // 4
    coord = (xc, yc, zc)

    def chip_peer(dim, same_core=True):
        w = wk
        s = zc
        if dim == 0:
            w = wk + 2 - 4 * xc
        elif dim == 1:
            w = wk + 4 - 8 * yc
        elif dim == 2:
            s = 1 - zc
        if not same_core:
            w = w + 1 - 2 * core
        return (s, w)

    partner = chip_peer(3, False)

    bar = pltpu.get_barrier_semaphore()
    pl.semaphore_signal(bar, inc=1, device_id=partner, device_id_type=MESH)
    for dim in range(3):
        for same in (True, False):
            pl.semaphore_signal(bar, inc=1, device_id=chip_peer(dim, same), device_id_type=MESH)

    def w_load(lay):
        return (pltpu.make_async_copy(w1_in.at[0, lay], w1.at[0, lay], ld_sem.at[lay]),
                pltpu.make_async_copy(w2_in.at[0, lay], w2.at[0, lay], ld_sem.at[L + lay]))

    def g_load(mat, lay):
        if mat == 1:
            return pltpu.make_async_copy(g1_in.at[lay], g1.at[lay], ld_sem.at[2 * L + lay])
        return pltpu.make_async_copy(g2_in.at[lay], g2.at[lay], ld_sem.at[3 * L + lay])

    def m_load(mat, lay):
        if mat == 1:
            return pltpu.make_async_copy(m1_in.at[lay], m1.at[lay], ld_sem.at[4 * L + lay])
        return pltpu.make_async_copy(m2_in.at[lay], m2.at[lay], ld_sem.at[5 * L + lay])

    x_load = pltpu.make_async_copy(x_in.at[0], xb, ld_sem.at[6 * L])
    y_load = pltpu.make_async_copy(y_in.at[0], yb, ld_sem.at[6 * L + 1])
    x_load.start()
    for cp in w_load(0):
        cp.start()
    y_load.start()
    for lay in range(1, L):
        for cp in w_load(lay):
            cp.start()
    for lay in range(L):
        for mat in (1, 2):
            g_load(mat, lay).start()
    for lay in range(L):
        for mat in (1, 2):
            m_load(mat, lay).start()
    x_load.wait()

    def dims_of(color_idx):
        return color_idx % 3, (color_idx + 1) % 3, (color_idx + 2) % 3

    def rs0_copies(gi):
        p, c, u0, nu = GROUPS[gi]
        d0 = dims_of(c)[0]
        k0 = coord[d0]
        us = pl.ds(u0, nu)
        other = 1 - core

        def rows(tc, blk):
            return pl.ds(pl.multiple_of(tc * 64 + blk * 32, 32), 32)

        out = []
        for idx, (tc, blk, dev) in enumerate(((other, k0, partner),
                                               (core, 1 - k0, chip_peer(d0, True)),
                                               (other, 1 - k0, chip_peer(d0, False)))):
            out.append(pltpu.make_async_remote_copy(
                src_ref=delta.at[p, us, rows(tc, blk)], dst_ref=raw.at[idx, p, us],
                send_sem=s0_send.at[gi, idx], recv_sem=s0_recv.at[gi, idx],
                device_id=dev, device_id_type=MESH))
        return out

    def stage_copy(stage, gi):
        p, c, u0, nu = GROUPS[gi]
        d0, d1, d2 = dims_of(c)
        k0, k1, k2 = coord[d0], coord[d1], coord[d2]
        us = pl.ds(u0, nu)
        if stage == RS1:
            src, dst, dev = s1.at[p, us, pl.ds(pl.multiple_of((1 - k1) * 16, 16), 16)], r1.at[p, us], chip_peer(d1)
        elif stage == X2:
            src, dst, dev = s2.at[p, us], r2.at[p, us], chip_peer(d2)
        else:
            base = core * 64
            if stage == AG1:
                off, n, dev = base + k0 * 32 + k1 * 16, 16, chip_peer(d1)
            elif stage == AG2:
                off, n, dev = base + k0 * 32, 32, chip_peer(d0)
            elif stage == DDA:
                off, n, dev = base + k0 * 32, 32, partner
            else:
                off, n, dev = base + (1 - k0) * 32, 32, partner
            src = full.at[p, us, pl.ds(pl.multiple_of(off, 16), n)]
            dst = src
        return pltpu.make_async_remote_copy(
            src_ref=src, dst_ref=dst, send_sem=st_send.at[stage, gi], recv_sem=st_recv.at[stage, gi],
            device_id=dev, device_id_type=MESH)

    def unit_slice(mat, u):
        if mat == 2:
            return pl.ds(u * 128, 128), pl.ds(0, 256)
        return pl.ds((u % 2) * 128, 128), pl.ds((u // 2) * 256, 256)

    def layer_0(lay, _):
        load1, load2 = w_load(lay)
        h_bf = hid[...].astype(BF16)
        hb[lay] = h_bf
        load1.wait()
        for j in range(NB):
            cols = slice(j * D, (j + 1) * D)
            w_bf = w1[0, lay, :, cols].astype(BF16)
            w1b[lay, :, cols] = w_bf
            u, dg = gelu_pair(dot(h_bf, w_bf, 1, 0))
            ub[lay, :, cols] = u.astype(BF16)
            du[lay, :, cols] = dg
        load2.wait()
        acc = hid[...]
        for j in range(NB):
            cols = slice(j * D, (j + 1) * D)
            w_bf = w2[0, lay, cols, :].astype(BF16)
            w2b[lay, cols, :] = w_bf
            acc = acc + dot(ub[lay, :, cols], w_bf, 1, 0)
        hid[...] = acc
        return 0

    def forward(k, before_layer_1=None):
        hid[...] = xb[k].astype(F32)

        def layer(lay, _):
            if before_layer_1 is not None:
                pl.when(lay == 1)(before_layer_1)
            h_bf = hid[...].astype(BF16)
            hb[lay] = h_bf
            acc = hid[...]
            for j in range(NB):
                cols = slice(j * D, (j + 1) * D)
                a = dot(h_bf, w1b[lay, :, cols], 1, 0)
                u, dg = gelu_pair(a)
                u_bf = u.astype(BF16)
                ub[lay, :, cols] = u_bf
                du[lay, :, cols] = dg
                acc = acc + dot(u_bf, w2b[lay, cols, :], 1, 0)
            hid[...] = acc
            return 0

        lax.fori_loop(0, L, layer_0 if k == 0 else layer, 0)

    def loss_grad(k):
        dhid[...] = (2.0 / (B * D)) * (hid[...] - yb[k].astype(F32))

    def update2(lay, cols, u_j, e):
        new2 = w2[0, lay, cols, :] - INNER_LR * dot(u_j, e, 0, 0)
        w2[0, lay, cols, :] = new2
        w2b[lay, cols, :] = new2.astype(BF16)

    def update1(lay, cols, h_bf, c):
        new1 = w1[0, lay, :, cols] - INNER_LR * dot(h_bf, c, 0, 0)
        w1[0, lay, :, cols] = new1
        w1b[lay, :, cols] = new1.astype(BF16)

    def send_piece(i, which):
        for p in (which, 2 + which):
            @pl.when(i == p // 2)
            def _(p=p):
                for gi in range(3 * p, 3 * p + 3):
                    for cp in rs0_copies(gi):
                        cp.start()

    def back_send(i, lay):
        p = 2 * i
        e = dhid[...].astype(BF16)
        h_bf = hb[lay]
        g_load(2, lay).wait()
        for j in range(NB):
            cols = slice(j * D, (j + 1) * D)
            new2 = w2[0, lay, cols, :] - INNER_LR * dot(ub[lay, :, cols], e, 0, 0)
            w2[0, lay, cols, :] = new2
            dl = (g2[lay, cols, :] - new2).astype(BF16)
            delta[p, 2 * j] = dl[:128]
            delta[p, 2 * j + 1] = dl[128:]
        send_piece(i, 0)
        g_load(1, lay).wait()
        acc = dhid[...]
        for j in range(NB):
            cols = slice(j * D, (j + 1) * D)
            d_u = dot(e, w2b[lay, cols, :], 1, 1)
            c = (du[lay, :, cols] * d_u).astype(BF16)
            acc = acc + dot(c, w1b[lay, :, cols], 1, 1)
            new1 = w1[0, lay, :, cols] - INNER_LR * dot(h_bf, c, 0, 0)
            w1[0, lay, :, cols] = new1
            w1b[lay, :, cols] = new1.astype(BF16)
            dl = (g1[lay, :, cols] - new1).astype(BF16)
            delta[p + 1, 2 * j] = dl[:128]
            delta[p + 1, 2 * j + 1] = dl[128:]
        dhid[...] = acc
        send_piece(i, 1)
        w2b[lay] = w2[0, lay].astype(BF16)

    def back_full(lay):
        e = dhid[...].astype(BF16)
        h_bf = hb[lay]
        acc = dhid[...]
        for j in range(NB):
            cols = slice(j * D, (j + 1) * D)
            d_u = dot(e, w2b[lay, cols, :], 1, 1)
            c = (du[lay, :, cols] * d_u).astype(BF16)
            update2(lay, cols, ub[lay, :, cols], e)
            acc = acc + dot(c, w1b[lay, :, cols], 1, 1)
            update1(lay, cols, h_bf, c)
        dhid[...] = acc

    def back_chain(lay):
        e = dhid[...].astype(BF16)
        eb[lay - 2] = e
        acc = dhid[...]
        for j in range(NB):
            cols = slice(j * D, (j + 1) * D)
            d_u = dot(e, w2b[lay, cols, :], 1, 1)
            c = (du[lay, :, cols] * d_u).astype(BF16)
            cb[lay - 2, :, cols] = c
            acc = acc + dot(c, w1b[lay, :, cols], 1, 1)
        dhid[...] = acc

    def back_weights(lay):
        e = eb[lay - 2]
        h_bf = hb[lay]
        for j in range(NB):
            cols = slice(j * D, (j + 1) * D)
            update2(lay, cols, ub[lay, :, cols], e)
            update1(lay, cols, h_bf, cb[lay - 2, :, cols])

    def reduce_stage1(p):
        for gi in range(3 * p, 3 * p + 3):
            _, c, u0, nu = GROUPS[gi]
            rows = pl.ds(pl.multiple_of(core * 64 + coord[dims_of(c)[0]] * 32, 32), 32)
            for cp in rs0_copies(gi):
                cp.wait_recv()
            for u in range(u0, u0 + nu):
                s1[p, u] = ((delta[p, u, rows, :].astype(F32) + raw[0, p, u].astype(F32))
                            + (raw[1, p, u].astype(F32) + raw[2, p, u].astype(F32)))
            stage_copy(RS1, gi).start()

    def reduce_stage2(p):
        for gi in range(3 * p, 3 * p + 3):
            _, c, u0, nu = GROUPS[gi]
            rows = pl.ds(pl.multiple_of(coord[dims_of(c)[1]] * 16, 16), 16)
            stage_copy(RS1, gi).wait_recv()
            for u in range(u0, u0 + nu):
                s2[p, u] = s1[p, u, rows, :] + r1[p, u]
            stage_copy(X2, gi).start()

    def reduce_stage3(p):
        for gi in range(3 * p, 3 * p + 3):
            _, c, u0, nu = GROUPS[gi]
            d0, d1, d2 = dims_of(c)
            rows = pl.ds(pl.multiple_of(core * 64 + coord[d0] * 32 + coord[d1] * 16, 16), 16)
            stage_copy(X2, gi).wait_recv()
            for u in range(u0, u0 + nu):
                full[p, u, rows, :] = s2[p, u] + r2[p, u]
            stage_copy(AG1, gi).start()

    def unit_copy(second, u):
        p = LAST
        d0 = dims_of([c for q, c, u0, nu in GROUPS if q == p and u0 <= u < u0 + nu][0])[0]
        k0 = coord[d0]
        off = core * 64 + ((1 - k0) if second else k0) * 32
        ref = full.at[p, u, pl.ds(pl.multiple_of(off, 16), 32)]
        return pltpu.make_async_remote_copy(
            src_ref=ref, dst_ref=ref, send_sem=un_send.at[second, u], recv_sem=un_recv.at[second, u],
            device_id=partner if second else chip_peer(d0), device_id_type=MESH)

    def gather_stage2(p):
        for gi in range(3 * p, 3 * p + 3):
            stage_copy(AG1, gi).wait_recv()
            if p != LAST:
                stage_copy(AG2, gi).start()
            else:
                _, _, u0, nu = GROUPS[gi]
                for u in range(u0, u0 + nu):
                    unit_copy(0, u).start()
            stage_copy(DDA, gi).start()

    def gather_stage3(p):
        for gi in range(3 * p, 3 * p + 3):
            stage_copy(AG2, gi).wait_recv()
            stage_copy(DDB, gi).start()

    def outer_unit(frag, p, u):
        part, mat = PIECES[p]
        lay = 2 * frag + part
        wr, wbr, gr, mr = (w1, w1b, g1, m1) if mat == 1 else (w2, w2b, g2, m2)
        rows, cols = unit_slice(mat, u)
        mean = full[p, u] * (1.0 / N_ALL)
        mom = OUTER_MOM * mr[lay, rows, cols] + mean
        glob = gr[lay, rows, cols] - OUTER_LR * (OUTER_MOM * mom + mean)
        mr[lay, rows, cols] = mom
        gr[lay, rows, cols] = glob
        merged = MERGE_MIX * wr[0, lay, rows, cols] + (1.0 - MERGE_MIX) * glob
        wr[0, lay, rows, cols] = merged
        if frag == 0:
            wbr[lay, rows, cols] = merged.astype(BF16)

    def load_momentum(frag, p):
        part, mat = PIECES[p]
        m_load(mat, 2 * frag + part).wait()

    def outer_update(frag, p):
        load_momentum(frag, p)
        for gi in range(3 * p, 3 * p + 3):
            stage_copy(DDA, gi).wait_recv()
            stage_copy(DDB, gi).wait_recv()
        for u in range(8):
            outer_unit(frag, p, u)

    def finish(frag):
        load_momentum(frag, LAST)
        first = [(u0, u0 + nu) for q, c, u0, nu in GROUPS if q == LAST]
        order = [u0 + i for i in range(3) for u0, end in first if u0 + i < end]
        for gi in range(3 * LAST, 3 * LAST + 3):
            stage_copy(DDA, gi).wait_recv()
        for idx in range(8 + 3):
            if idx < 8:
                unit_copy(0, order[idx]).wait_recv()
                unit_copy(1, order[idx]).start()
            if idx >= 3:
                unit_copy(1, order[idx - 3]).wait_recv()
                outer_unit(frag, LAST, order[idx - 3])
        for gi in range(12):
            for cp in rs0_copies(gi):
                cp.wait_send()
            for stage in range(6):
                if GROUPS[gi][0] != LAST or stage not in (AG2, DDB):
                    stage_copy(stage, gi).wait_send()
        for u in range(8):
            unit_copy(0, u).wait_send()
            unit_copy(1, u).wait_send()

    def sync(frag):
        reduce_stage1(3)
        for p in range(4):
            reduce_stage2(p)
        for p in range(4):
            reduce_stage3(p)
        for p in GATHER_ORDER:
            gather_stage2(p)
        prev = None
        for p in GATHER_ORDER[:-1]:
            gather_stage3(p)
            if prev is not None:
                outer_update(frag, prev)
            prev = p
        outer_update(frag, prev)

    def layers(lo, body):
        def run(i, _):
            body(i, lo - i)
            return 0
        return run

    forward(0)
    y_load.wait()
    pl.semaphore_wait(bar, 7)
    loss_grad(0)
    lax.fori_loop(0, 2, layers(3, lambda i, lay: back_chain(lay)), 0)

    lax.fori_loop(0, 2, layers(1, back_send), 0)
    lax.fori_loop(0, 2, layers(3, lambda i, lay: back_weights(lay)), 0)

    def back_hook(i, lay):
        back_full(lay)

        @pl.when(i == 0)
        def _():
            reduce_stage1(0)
            reduce_stage1(1)

        @pl.when(i == 2)
        def _():
            reduce_stage1(2)

    forward(1)
    loss_grad(1)
    lax.fori_loop(0, L, layers(3, back_hook), 0)
    sync(0)

    forward(2, lambda: finish(0))
    loss_grad(2)

    lax.fori_loop(0, 2, layers(3, back_send), 0)
    lax.fori_loop(0, 2, layers(1, lambda i, lay: back_full(lay)), 0)

    forward(3)
    loss_grad(3)
    lax.fori_loop(0, L, layers(3, back_hook), 0)
    sync(1)
    finish(1)


def write_body(*refs):
    srcs, dsts, sem = refs[:6], refs[6:12], refs[12]
    cps = []
    for i in range(6):
        for lay in range(L):
            src = srcs[i].at[0, lay] if i < 2 else srcs[i].at[lay]
            dst = dsts[i].at[0, lay] if i < 2 else dsts[i].at[lay]
            cps.append(pltpu.make_async_copy(src, dst, sem.at[i, lay]))
    for cp in cps:
        cp.start()
    for cp in cps:
        cp.wait()


def solution(mesh):
    def device_fn(w1_loc, w2_loc, w1_glb, w2_glb, mom1, mom2, x_loc, y_loc):
        arrays = (w1_loc, w2_loc, w1_glb, w2_glb, mom1, mom2)
        shapes = [jax.ShapeDtypeStruct(a.shape, F32) for a in arrays]
        dma = pltpu.SemaphoreType.DMA
        work = pl.pallas_call(
            main_body,
            out_shape=shapes,
            in_specs=[HBM] * 8,
            out_specs=[VMEM] * 6,
            scratch_shapes=[
                pltpu.VMEM((H, B, D), BF16), pltpu.VMEM((H, B, D), BF16),
                pltpu.VMEM((L, D, FF), BF16), pltpu.VMEM((L, FF, D), BF16),
                pltpu.VMEM((L, B, D), BF16), pltpu.VMEM((L, B, FF), BF16), pltpu.VMEM((L, B, FF), F32),
                pltpu.VMEM((B, D), F32), pltpu.VMEM((B, D), F32),
                pltpu.VMEM((2, B, D), BF16), pltpu.VMEM((2, B, FF), BF16),
                pltpu.VMEM((4, 8, 128, 256), BF16), pltpu.VMEM((3, 4, 8, 32, 256), BF16),
                pltpu.VMEM((4, 8, 32, 256), F32), pltpu.VMEM((4, 8, 16, 256), F32),
                pltpu.VMEM((4, 8, 16, 256), F32), pltpu.VMEM((4, 8, 16, 256), F32),
                pltpu.VMEM((4, 8, 128, 256), F32),
                dma((26,)), dma((12, 3)), dma((12, 3)), dma((6, 12)), dma((6, 12)), dma((2, 8)), dma((2, 8)),
            ],
            compiler_params=pltpu.CompilerParams(
                collective_id=0, has_side_effects=True, vmem_limit_bytes=28 * 2**20),
            name='diloco_round',
        )(*[pltpu.with_memory_space_constraint(a, pltpu.HBM) for a in (*arrays, x_loc, y_loc)])
        outs = pl.pallas_call(
            write_body,
            out_shape=shapes,
            in_specs=[VMEM] * 6,
            out_specs=[HBM] * 6,
            scratch_shapes=[dma((6, L))],
            compiler_params=pltpu.CompilerParams(vmem_limit_bytes=2 * 2**20),
            name='write_out',
        )(*work)
        return tuple(outs)

    local_spec = P(('shard', 'worker'))
    whole_spec = P()
    return jax.shard_map(device_fn, mesh=mesh, in_specs=(local_spec, local_spec, whole_spec, whole_spec, whole_spec, whole_spec, local_spec, local_spec), out_specs=(local_spec, local_spec, whole_spec, whole_spec, whole_spec, whole_spec), check_vma=False)
```

```python
import jax
import jax.numpy as jnp
from jax import lax
from jax.experimental import pallas as pl
from jax.experimental.pallas import tpu as pltpu
from jax.sharding import PartitionSpec as P

OUTER_LR = 0.7
OUTER_MOM = 0.9
MERGE_MIX = 0.5

L = 4
H = 4
D = 256
FF = 1024
B = 128
NB = FF // D
INNER_LR = 2.0 * D / (FF * L)
N_ALL = 16
F32 = jnp.float32
BF16 = jnp.bfloat16
MESH = pl.DeviceIdType.MESH
HBM = pl.BlockSpec(memory_space=pltpu.HBM)
VMEM = pl.BlockSpec(memory_space=pltpu.VMEM)

PIECES = ((1, 2), (1, 1), (0, 2), (0, 1))
COLOR_UNITS = ((3, 3, 2), (3, 2, 3), (2, 3, 3), (3, 3, 2))
GROUPS = []
for piece_idx in range(4):
    first_unit = 0
    for color in range(3):
        GROUPS.append((piece_idx, color, first_unit, COLOR_UNITS[piece_idx][color]))
        first_unit += COLOR_UNITS[piece_idx][color]
GATHER_ORDER = (0, 2, 3, 1)
LAST = GATHER_ORDER[-1]
RS1, X2, AG1, AG2, DDA, DDB = range(6)


def dot(a, b, ca, cb):
    return lax.dot_general(a, b, (((ca,), (cb,)), ((), ())), preferred_element_type=F32)


def gelu_pair(a):
    k0 = 0.7978845608028654
    k1 = k0 * 0.044715
    a2 = a * a
    t = jnp.tanh(a * (k0 + k1 * a2))
    h = 0.5 + 0.5 * t
    u = a * h
    du = h + (u * (1.0 - h)) * (2.0 * k0 + (6.0 * k1) * a2)
    return u, du


def main_body(w1_in, w2_in, g1_in, g2_in, m1_in, m2_in, x_in, y_in,
              w1, w2, g1, g2, m1, m2,
              xb, yb, w1b, w2b, hb, ub, du, hid, dhid, eb, cb,
              delta, raw, s1, r1, s2, r2, full,
              ld_sem, s0_send, s0_recv, st_send, st_recv):
    zc = lax.axis_index('shard')
    wk = lax.axis_index('worker')
    core = lax.rem(wk, 2)
    xc = lax.rem(wk // 2, 2)
    yc = wk // 4
    coord = (xc, yc, zc)

    def chip_peer(dim, same_core=True):
        w = wk
        s = zc
        if dim == 0:
            w = wk + 2 - 4 * xc
        elif dim == 1:
            w = wk + 4 - 8 * yc
        elif dim == 2:
            s = 1 - zc
        if not same_core:
            w = w + 1 - 2 * core
        return (s, w)

    partner = chip_peer(3, False)

    bar = pltpu.get_barrier_semaphore()
    pl.semaphore_signal(bar, inc=1, device_id=partner, device_id_type=MESH)
    for dim in range(3):
        for same in (True, False):
            pl.semaphore_signal(bar, inc=1, device_id=chip_peer(dim, same), device_id_type=MESH)

    def w_load(lay):
        return (pltpu.make_async_copy(w1_in.at[0, lay], w1.at[0, lay], ld_sem.at[lay]),
                pltpu.make_async_copy(w2_in.at[0, lay], w2.at[0, lay], ld_sem.at[L + lay]))

    def g_load(mat, lay):
        if mat == 1:
            return pltpu.make_async_copy(g1_in.at[lay], g1.at[lay], ld_sem.at[2 * L + lay])
        return pltpu.make_async_copy(g2_in.at[lay], g2.at[lay], ld_sem.at[3 * L + lay])

    def m_load(mat, lay):
        if mat == 1:
            return pltpu.make_async_copy(m1_in.at[lay], m1.at[lay], ld_sem.at[4 * L + lay])
        return pltpu.make_async_copy(m2_in.at[lay], m2.at[lay], ld_sem.at[5 * L + lay])

    x_load = pltpu.make_async_copy(x_in.at[0], xb, ld_sem.at[6 * L])
    y_load = pltpu.make_async_copy(y_in.at[0], yb, ld_sem.at[6 * L + 1])
    x_load.start()
    for cp in w_load(0):
        cp.start()
    y_load.start()
    for lay in range(1, L):
        for cp in w_load(lay):
            cp.start()
    for lay in range(L):
        for mat in (1, 2):
            g_load(mat, lay).start()
    for lay in range(L):
        for mat in (1, 2):
            m_load(mat, lay).start()
    x_load.wait()

    def dims_of(color_idx):
        return color_idx % 3, (color_idx + 1) % 3, (color_idx + 2) % 3

    def rs0_copies(gi):
        p, c, u0, nu = GROUPS[gi]
        d0 = dims_of(c)[0]
        k0 = coord[d0]
        us = pl.ds(u0, nu)
        other = 1 - core

        def rows(tc, blk):
            return pl.ds(pl.multiple_of(tc * 64 + blk * 32, 32), 32)

        out = []
        for idx, (tc, blk, dev) in enumerate(((other, k0, partner),
                                               (core, 1 - k0, chip_peer(d0, True)),
                                               (other, 1 - k0, chip_peer(d0, False)))):
            out.append(pltpu.make_async_remote_copy(
                src_ref=delta.at[p, us, rows(tc, blk)], dst_ref=raw.at[idx, p, us],
                send_sem=s0_send.at[gi, idx], recv_sem=s0_recv.at[gi, idx],
                device_id=dev, device_id_type=MESH))
        return out

    def stage_copy(stage, gi):
        p, c, u0, nu = GROUPS[gi]
        d0, d1, d2 = dims_of(c)
        k0, k1, k2 = coord[d0], coord[d1], coord[d2]
        us = pl.ds(u0, nu)
        if stage == RS1:
            src, dst, dev = s1.at[p, us, pl.ds(pl.multiple_of((1 - k1) * 16, 16), 16)], r1.at[p, us], chip_peer(d1)
        elif stage == X2:
            src, dst, dev = s2.at[p, us], r2.at[p, us], chip_peer(d2)
        else:
            base = core * 64
            if stage == AG1:
                off, n, dev = base + k0 * 32 + k1 * 16, 16, chip_peer(d1)
            elif stage == AG2:
                off, n, dev = base + k0 * 32, 32, chip_peer(d0)
            elif stage == DDA:
                off, n, dev = base + k0 * 32, 32, partner
            else:
                off, n, dev = base + (1 - k0) * 32, 32, partner
            src = full.at[p, us, pl.ds(pl.multiple_of(off, 16), n)]
            dst = src
        return pltpu.make_async_remote_copy(
            src_ref=src, dst_ref=dst, send_sem=st_send.at[stage, gi], recv_sem=st_recv.at[stage, gi],
            device_id=dev, device_id_type=MESH)

    def unit_slice(mat, u):
        if mat == 2:
            return pl.ds(u * 128, 128), pl.ds(0, 256)
        return pl.ds((u % 2) * 128, 128), pl.ds((u // 2) * 256, 256)

    def layer_0(lay, _):
        load1, load2 = w_load(lay)
        h_bf = hid[...].astype(BF16)
        hb[lay] = h_bf
        load1.wait()
        for j in range(NB):
            cols = slice(j * D, (j + 1) * D)
            w_bf = w1[0, lay, :, cols].astype(BF16)
            w1b[lay, :, cols] = w_bf
            u, dg = gelu_pair(dot(h_bf, w_bf, 1, 0))
            ub[lay, :, cols] = u.astype(BF16)
            du[lay, :, cols] = dg
        load2.wait()
        acc = hid[...]
        for j in range(NB):
            cols = slice(j * D, (j + 1) * D)
            w_bf = w2[0, lay, cols, :].astype(BF16)
            w2b[lay, cols, :] = w_bf
            acc = acc + dot(ub[lay, :, cols], w_bf, 1, 0)
        hid[...] = acc
        return 0

    def forward(k, before_layer_1=None):
        hid[...] = xb[k].astype(F32)

        def layer(lay, _):
            if before_layer_1 is not None:
                pl.when(lay == 1)(before_layer_1)
            h_bf = hid[...].astype(BF16)
            hb[lay] = h_bf
            acc = hid[...]
            for j in range(NB):
                cols = slice(j * D, (j + 1) * D)
                a = dot(h_bf, w1b[lay, :, cols], 1, 0)
                u, dg = gelu_pair(a)
                u_bf = u.astype(BF16)
                ub[lay, :, cols] = u_bf
                du[lay, :, cols] = dg
                acc = acc + dot(u_bf, w2b[lay, cols, :], 1, 0)
            hid[...] = acc
            return 0

        lax.fori_loop(0, L, layer_0 if k == 0 else layer, 0)

    def loss_grad(k):
        dhid[...] = (2.0 / (B * D)) * (hid[...] - yb[k].astype(F32))

    def update2(lay, cols, u_j, e):
        new2 = w2[0, lay, cols, :] - INNER_LR * dot(u_j, e, 0, 0)
        w2[0, lay, cols, :] = new2
        w2b[lay, cols, :] = new2.astype(BF16)

    def update1(lay, cols, h_bf, c):
        new1 = w1[0, lay, :, cols] - INNER_LR * dot(h_bf, c, 0, 0)
        w1[0, lay, :, cols] = new1
        w1b[lay, :, cols] = new1.astype(BF16)

    def send_piece(i, which):
        for p in (which, 2 + which):
            @pl.when(i == p // 2)
            def _(p=p):
                for gi in range(3 * p, 3 * p + 3):
                    for cp in rs0_copies(gi):
                        cp.start()

    def back_send(i, lay):
        p = 2 * i
        e = dhid[...].astype(BF16)
        h_bf = hb[lay]
        g_load(2, lay).wait()
        for j in range(NB):
            cols = slice(j * D, (j + 1) * D)
            new2 = w2[0, lay, cols, :] - INNER_LR * dot(ub[lay, :, cols], e, 0, 0)
            w2[0, lay, cols, :] = new2
            dl = (g2[lay, cols, :] - new2).astype(BF16)
            delta[p, 2 * j] = dl[:128]
            delta[p, 2 * j + 1] = dl[128:]
        send_piece(i, 0)
        g_load(1, lay).wait()
        acc = dhid[...]
        for j in range(NB):
            cols = slice(j * D, (j + 1) * D)
            d_u = dot(e, w2b[lay, cols, :], 1, 1)
            c = (du[lay, :, cols] * d_u).astype(BF16)
            acc = acc + dot(c, w1b[lay, :, cols], 1, 1)
            new1 = w1[0, lay, :, cols] - INNER_LR * dot(h_bf, c, 0, 0)
            w1[0, lay, :, cols] = new1
            w1b[lay, :, cols] = new1.astype(BF16)
            dl = (g1[lay, :, cols] - new1).astype(BF16)
            delta[p + 1, 2 * j] = dl[:128]
            delta[p + 1, 2 * j + 1] = dl[128:]
        dhid[...] = acc
        send_piece(i, 1)
        w2b[lay] = w2[0, lay].astype(BF16)

    def back_full(lay):
        e = dhid[...].astype(BF16)
        h_bf = hb[lay]
        acc = dhid[...]
        for j in range(NB):
            cols = slice(j * D, (j + 1) * D)
            d_u = dot(e, w2b[lay, cols, :], 1, 1)
            c = (du[lay, :, cols] * d_u).astype(BF16)
            update2(lay, cols, ub[lay, :, cols], e)
            acc = acc + dot(c, w1b[lay, :, cols], 1, 1)
            update1(lay, cols, h_bf, c)
        dhid[...] = acc

    def back_chain(lay):
        e = dhid[...].astype(BF16)
        eb[lay - 2] = e
        acc = dhid[...]
        for j in range(NB):
            cols = slice(j * D, (j + 1) * D)
            d_u = dot(e, w2b[lay, cols, :], 1, 1)
            c = (du[lay, :, cols] * d_u).astype(BF16)
            cb[lay - 2, :, cols] = c
            acc = acc + dot(c, w1b[lay, :, cols], 1, 1)
        dhid[...] = acc

    def back_weights(lay):
        e = eb[lay - 2]
        h_bf = hb[lay]
        for j in range(NB):
            cols = slice(j * D, (j + 1) * D)
            update2(lay, cols, ub[lay, :, cols], e)
            update1(lay, cols, h_bf, cb[lay - 2, :, cols])

    def reduce_stage1(p):
        for gi in range(3 * p, 3 * p + 3):
            _, c, u0, nu = GROUPS[gi]
            rows = pl.ds(pl.multiple_of(core * 64 + coord[dims_of(c)[0]] * 32, 32), 32)
            for cp in rs0_copies(gi):
                cp.wait_recv()
            for u in range(u0, u0 + nu):
                s1[p, u] = ((delta[p, u, rows, :].astype(F32) + raw[0, p, u].astype(F32))
                            + (raw[1, p, u].astype(F32) + raw[2, p, u].astype(F32)))
            stage_copy(RS1, gi).start()

    def reduce_stage2(p):
        for gi in range(3 * p, 3 * p + 3):
            _, c, u0, nu = GROUPS[gi]
            rows = pl.ds(pl.multiple_of(coord[dims_of(c)[1]] * 16, 16), 16)
            stage_copy(RS1, gi).wait_recv()
            for u in range(u0, u0 + nu):
                s2[p, u] = s1[p, u, rows, :] + r1[p, u]
            stage_copy(X2, gi).start()

    def reduce_stage3(p):
        for gi in range(3 * p, 3 * p + 3):
            _, c, u0, nu = GROUPS[gi]
            d0, d1, d2 = dims_of(c)
            rows = pl.ds(pl.multiple_of(core * 64 + coord[d0] * 32 + coord[d1] * 16, 16), 16)
            stage_copy(X2, gi).wait_recv()
            for u in range(u0, u0 + nu):
                full[p, u, rows, :] = s2[p, u] + r2[p, u]
            stage_copy(AG1, gi).start()

    def gather_stage2(p):
        for gi in range(3 * p, 3 * p + 3):
            stage_copy(AG1, gi).wait_recv()
            stage_copy(AG2, gi).start()
            stage_copy(DDA, gi).start()

    def gather_stage3(p):
        for gi in range(3 * p, 3 * p + 3):
            stage_copy(AG2, gi).wait_recv()
            stage_copy(DDB, gi).start()

    def outer_unit(frag, p, u):
        part, mat = PIECES[p]
        lay = 2 * frag + part
        wr, wbr, gr, mr = (w1, w1b, g1, m1) if mat == 1 else (w2, w2b, g2, m2)
        rows, cols = unit_slice(mat, u)
        mean = full[p, u] * (1.0 / N_ALL)
        mom = OUTER_MOM * mr[lay, rows, cols] + mean
        glob = gr[lay, rows, cols] - OUTER_LR * (OUTER_MOM * mom + mean)
        mr[lay, rows, cols] = mom
        gr[lay, rows, cols] = glob
        merged = MERGE_MIX * wr[0, lay, rows, cols] + (1.0 - MERGE_MIX) * glob
        wr[0, lay, rows, cols] = merged
        if frag == 0:
            wbr[lay, rows, cols] = merged.astype(BF16)

    def load_momentum(frag, p):
        part, mat = PIECES[p]
        m_load(mat, 2 * frag + part).wait()

    def outer_update(frag, p):
        load_momentum(frag, p)
        for gi in range(3 * p, 3 * p + 3):
            stage_copy(DDA, gi).wait_recv()
            stage_copy(DDB, gi).wait_recv()
        for u in range(8):
            outer_unit(frag, p, u)

    def finish(frag):
        gather_stage3(LAST)
        outer_update(frag, LAST)
        for gi in range(12):
            for cp in rs0_copies(gi):
                cp.wait_send()
            for stage in range(6):
                stage_copy(stage, gi).wait_send()

    def sync(frag):
        reduce_stage1(3)
        for p in range(4):
            reduce_stage2(p)
        for p in range(4):
            reduce_stage3(p)
        for p in GATHER_ORDER:
            gather_stage2(p)
        prev = None
        for p in GATHER_ORDER[:-1]:
            gather_stage3(p)
            if prev is not None:
                outer_update(frag, prev)
            prev = p
        outer_update(frag, prev)

    def layers(lo, body):
        def run(i, _):
            body(i, lo - i)
            return 0
        return run

    forward(0)
    y_load.wait()
    pl.semaphore_wait(bar, 7)
    loss_grad(0)
    lax.fori_loop(0, 2, layers(3, lambda i, lay: back_chain(lay)), 0)

    lax.fori_loop(0, 2, layers(1, back_send), 0)
    lax.fori_loop(0, 2, layers(3, lambda i, lay: back_weights(lay)), 0)

    def back_hook(i, lay):
        back_full(lay)

        @pl.when(i == 0)
        def _():
            reduce_stage1(0)
            reduce_stage1(1)

        @pl.when(i == 2)
        def _():
            reduce_stage1(2)

    forward(1)
    loss_grad(1)
    lax.fori_loop(0, L, layers(3, back_hook), 0)
    sync(0)

    forward(2, lambda: finish(0))
    loss_grad(2)

    lax.fori_loop(0, 2, layers(3, back_send), 0)
    lax.fori_loop(0, 2, layers(1, lambda i, lay: back_full(lay)), 0)

    forward(3)
    loss_grad(3)
    lax.fori_loop(0, L, layers(3, back_hook), 0)
    sync(1)
    finish(1)


def write_body(*refs):
    srcs, dsts, sem = refs[:6], refs[6:12], refs[12]
    cps = []
    for i in range(6):
        for lay in range(L):
            src = srcs[i].at[0, lay] if i < 2 else srcs[i].at[lay]
            dst = dsts[i].at[0, lay] if i < 2 else dsts[i].at[lay]
            cps.append(pltpu.make_async_copy(src, dst, sem.at[i, lay]))
    for cp in cps:
        cp.start()
    for cp in cps:
        cp.wait()


def solution(mesh):
    def device_fn(w1_loc, w2_loc, w1_glb, w2_glb, mom1, mom2, x_loc, y_loc):
        arrays = (w1_loc, w2_loc, w1_glb, w2_glb, mom1, mom2)
        shapes = [jax.ShapeDtypeStruct(a.shape, F32) for a in arrays]
        dma = pltpu.SemaphoreType.DMA
        work = pl.pallas_call(
            main_body,
            out_shape=shapes,
            in_specs=[HBM] * 8,
            out_specs=[VMEM] * 6,
            scratch_shapes=[
                pltpu.VMEM((H, B, D), BF16), pltpu.VMEM((H, B, D), BF16),
                pltpu.VMEM((L, D, FF), BF16), pltpu.VMEM((L, FF, D), BF16),
                pltpu.VMEM((L, B, D), BF16), pltpu.VMEM((L, B, FF), BF16), pltpu.VMEM((L, B, FF), F32),
                pltpu.VMEM((B, D), F32), pltpu.VMEM((B, D), F32),
                pltpu.VMEM((2, B, D), BF16), pltpu.VMEM((2, B, FF), BF16),
                pltpu.VMEM((4, 8, 128, 256), BF16), pltpu.VMEM((3, 4, 8, 32, 256), BF16),
                pltpu.VMEM((4, 8, 32, 256), F32), pltpu.VMEM((4, 8, 16, 256), F32),
                pltpu.VMEM((4, 8, 16, 256), F32), pltpu.VMEM((4, 8, 16, 256), F32),
                pltpu.VMEM((4, 8, 128, 256), F32),
                dma((26,)), dma((12, 3)), dma((12, 3)), dma((6, 12)), dma((6, 12)),
            ],
            compiler_params=pltpu.CompilerParams(
                collective_id=0, has_side_effects=True, vmem_limit_bytes=28 * 2**20),
            name='diloco_round',
        )(*[pltpu.with_memory_space_constraint(a, pltpu.HBM) for a in (*arrays, x_loc, y_loc)])
        outs = pl.pallas_call(
            write_body,
            out_shape=shapes,
            in_specs=[VMEM] * 6,
            out_specs=[HBM] * 6,
            scratch_shapes=[dma((6, L))],
            compiler_params=pltpu.CompilerParams(vmem_limit_bytes=2 * 2**20),
            name='write_out',
        )(*work)
        return tuple(outs)

    local_spec = P(('shard', 'worker'))
    whole_spec = P()
    return jax.shard_map(device_fn, mesh=mesh, in_specs=(local_spec, local_spec, whole_spec, whole_spec, whole_spec, whole_spec, local_spec, local_spec), out_specs=(local_spec, local_spec, whole_spec, whole_spec, whole_spec, whole_spec), check_vma=False)
```

```python
import jax
import jax.numpy as jnp
from jax import lax
from jax.experimental import pallas as pl
from jax.experimental.pallas import tpu as pltpu
from jax.sharding import PartitionSpec as P

OUTER_LR = 0.7
OUTER_MOM = 0.9
MERGE_MIX = 0.5

L = 4
H = 4
D = 256
FF = 1024
B = 128
NB = FF // D
INNER_LR = 2.0 * D / (FF * L)
N_ALL = 16
F32 = jnp.float32
BF16 = jnp.bfloat16
MESH = pl.DeviceIdType.MESH
HBM = pl.BlockSpec(memory_space=pltpu.HBM)
VMEM = pl.BlockSpec(memory_space=pltpu.VMEM)

PIECES = ((1, 2), (1, 1), (0, 2), (0, 1))
COLOR_UNITS = ((3, 3, 2), (3, 2, 3), (2, 3, 3), (3, 3, 2))
GROUPS = []
for piece_idx in range(4):
    first_unit = 0
    for color in range(3):
        GROUPS.append((piece_idx, color, first_unit, COLOR_UNITS[piece_idx][color]))
        first_unit += COLOR_UNITS[piece_idx][color]
GATHER_ORDER = (0, 2, 3, 1)
RS1, X2, AG1, AG2, DDA, DDB = range(6)


def dot(a, b, ca, cb):
    return lax.dot_general(a, b, (((ca,), (cb,)), ((), ())), preferred_element_type=F32)


def gelu_pair(a):
    k0 = 0.7978845608028654
    k1 = k0 * 0.044715
    a2 = a * a
    t = jnp.tanh(a * (k0 + k1 * a2))
    h = 0.5 + 0.5 * t
    u = a * h
    du = h + (u * (1.0 - h)) * (2.0 * k0 + (6.0 * k1) * a2)
    return u, du


def main_body(w1_in, w2_in, g1_in, g2_in, m1_in, m2_in, x_in, y_in,
              w1, w2, g1, g2, m1, m2,
              xb, yb, w1b, w2b, hb, ub, du, hid, dhid, eb, cb,
              delta, raw, s1, r1, s2, r2, full,
              ld_sem, s0_send, s0_recv, st_send, st_recv):
    zc = lax.axis_index('shard')
    wk = lax.axis_index('worker')
    core = lax.rem(wk, 2)
    xc = lax.rem(wk // 2, 2)
    yc = wk // 4
    coord = (xc, yc, zc)

    def chip_peer(dim, same_core=True):
        w = wk
        s = zc
        if dim == 0:
            w = wk + 2 - 4 * xc
        elif dim == 1:
            w = wk + 4 - 8 * yc
        elif dim == 2:
            s = 1 - zc
        if not same_core:
            w = w + 1 - 2 * core
        return (s, w)

    partner = chip_peer(3, False)

    bar = pltpu.get_barrier_semaphore()
    pl.semaphore_signal(bar, inc=1, device_id=partner, device_id_type=MESH)
    for dim in range(3):
        for same in (True, False):
            pl.semaphore_signal(bar, inc=1, device_id=chip_peer(dim, same), device_id_type=MESH)

    def w_load(lay):
        return (pltpu.make_async_copy(w1_in.at[0, lay], w1.at[0, lay], ld_sem.at[lay]),
                pltpu.make_async_copy(w2_in.at[0, lay], w2.at[0, lay], ld_sem.at[L + lay]))

    def g_load(mat, lay):
        if mat == 1:
            return pltpu.make_async_copy(g1_in.at[lay], g1.at[lay], ld_sem.at[2 * L + lay])
        return pltpu.make_async_copy(g2_in.at[lay], g2.at[lay], ld_sem.at[3 * L + lay])

    def m_load(mat, lay):
        if mat == 1:
            return pltpu.make_async_copy(m1_in.at[lay], m1.at[lay], ld_sem.at[4 * L + lay])
        return pltpu.make_async_copy(m2_in.at[lay], m2.at[lay], ld_sem.at[5 * L + lay])

    x_load = pltpu.make_async_copy(x_in.at[0], xb, ld_sem.at[6 * L])
    y_load = pltpu.make_async_copy(y_in.at[0], yb, ld_sem.at[6 * L + 1])
    x_load.start()
    for lay in range(2):
        for cp in w_load(lay):
            cp.start()
    y_load.start()
    x_load.wait()
    y_load.wait()

    def dims_of(color_idx):
        return color_idx % 3, (color_idx + 1) % 3, (color_idx + 2) % 3

    def rs0_copies(gi):
        p, c, u0, nu = GROUPS[gi]
        d0 = dims_of(c)[0]
        k0 = coord[d0]
        us = pl.ds(u0, nu)
        other = 1 - core

        def rows(tc, blk):
            return pl.ds(pl.multiple_of(tc * 64 + blk * 32, 32), 32)

        out = []
        for idx, (tc, blk, dev) in enumerate(((other, k0, partner),
                                               (core, 1 - k0, chip_peer(d0, True)),
                                               (other, 1 - k0, chip_peer(d0, False)))):
            out.append(pltpu.make_async_remote_copy(
                src_ref=delta.at[p, us, rows(tc, blk)], dst_ref=raw.at[idx, p, us],
                send_sem=s0_send.at[gi, idx], recv_sem=s0_recv.at[gi, idx],
                device_id=dev, device_id_type=MESH))
        return out

    def stage_copy(stage, gi):
        p, c, u0, nu = GROUPS[gi]
        d0, d1, d2 = dims_of(c)
        k0, k1, k2 = coord[d0], coord[d1], coord[d2]
        us = pl.ds(u0, nu)
        if stage == RS1:
            src, dst, dev = s1.at[p, us, pl.ds(pl.multiple_of((1 - k1) * 16, 16), 16)], r1.at[p, us], chip_peer(d1)
        elif stage == X2:
            src, dst, dev = s2.at[p, us], r2.at[p, us], chip_peer(d2)
        else:
            base = core * 64
            if stage == AG1:
                off, n, dev = base + k0 * 32 + k1 * 16, 16, chip_peer(d1)
            elif stage == AG2:
                off, n, dev = base + k0 * 32, 32, chip_peer(d0)
            elif stage == DDA:
                off, n, dev = base + k0 * 32, 32, partner
            else:
                off, n, dev = base + (1 - k0) * 32, 32, partner
            src = full.at[p, us, pl.ds(pl.multiple_of(off, 16), n)]
            dst = src
        return pltpu.make_async_remote_copy(
            src_ref=src, dst_ref=dst, send_sem=st_send.at[stage, gi], recv_sem=st_recv.at[stage, gi],
            device_id=dev, device_id_type=MESH)

    def unit_slice(mat, u):
        if mat == 2:
            return pl.ds(u * 128, 128), pl.ds(0, 256)
        return pl.ds((u % 2) * 128, 128), pl.ds((u // 2) * 256, 256)

    def make_delta(p, lay):
        mat = PIECES[p][1]
        wr, gr = (w1, g1) if mat == 1 else (w2, g2)
        g_load(mat, lay).wait()
        for u in range(8):
            rows, cols = unit_slice(mat, u)
            delta[p, u] = (gr[lay, rows, cols] - wr[0, lay, rows, cols]).astype(BF16)
        for gi in range(3 * p, 3 * p + 3):
            for cp in rs0_copies(gi):
                cp.start()

    def cast_layer(lay):
        for cp in w_load(lay):
            cp.wait()

        @pl.when(lay == 0)
        def _():
            for nxt in range(2, L):
                for cp in w_load(nxt):
                    cp.start()

        @pl.when(lay == 1)
        def _():
            for nxt in (1, 0):
                g_load(2, nxt).start()
                g_load(1, nxt).start()

        def cast(i, _):
            rows = pl.ds(pl.multiple_of(i * 64, 64), 64)
            w1b[lay, rows, :] = w1[0, lay, rows, :].astype(BF16)
            rows = pl.ds(pl.multiple_of(i * 256, 256), 256)
            w2b[lay, rows, :] = w2[0, lay, rows, :].astype(BF16)
            return 0

        lax.fori_loop(0, 4, cast, 0)

    def forward(k, before_layer_1=None):
        hid[...] = xb[k].astype(F32)

        def layer(lay, _):
            if k == 0:
                cast_layer(lay)
            if before_layer_1 is not None:
                pl.when(lay == 1)(before_layer_1)
            h_bf = hid[...].astype(BF16)
            hb[lay] = h_bf
            acc = hid[...]
            for j in range(NB):
                cols = slice(j * D, (j + 1) * D)
                a = dot(h_bf, w1b[lay, :, cols], 1, 0)
                u, dg = gelu_pair(a)
                u_bf = u.astype(BF16)
                ub[lay, :, cols] = u_bf
                du[lay, :, cols] = dg
                acc = acc + dot(u_bf, w2b[lay, cols, :], 1, 0)
            hid[...] = acc
            return 0

        lax.fori_loop(0, L, layer, 0)

    def loss_grad(k):
        dhid[...] = (2.0 / (B * D)) * (hid[...] - yb[k].astype(F32))

    def update2(lay, cols, u_j, e):
        new2 = w2[0, lay, cols, :] - INNER_LR * dot(u_j, e, 0, 0)
        w2[0, lay, cols, :] = new2
        w2b[lay, cols, :] = new2.astype(BF16)

    def update1(lay, cols, h_bf, c):
        new1 = w1[0, lay, :, cols] - INNER_LR * dot(h_bf, c, 0, 0)
        w1[0, lay, :, cols] = new1
        w1b[lay, :, cols] = new1.astype(BF16)

    def back_full(lay):
        e = dhid[...].astype(BF16)
        h_bf = hb[lay]
        acc = dhid[...]
        for j in range(NB):
            cols = slice(j * D, (j + 1) * D)
            d_u = dot(e, w2b[lay, cols, :], 1, 1)
            c = (du[lay, :, cols] * d_u).astype(BF16)
            update2(lay, cols, ub[lay, :, cols], e)
            acc = acc + dot(c, w1b[lay, :, cols], 1, 1)
            update1(lay, cols, h_bf, c)
        dhid[...] = acc

    def back_chain(lay):
        e = dhid[...].astype(BF16)
        eb[lay - 2] = e
        acc = dhid[...]
        for j in range(NB):
            cols = slice(j * D, (j + 1) * D)
            d_u = dot(e, w2b[lay, cols, :], 1, 1)
            c = (du[lay, :, cols] * d_u).astype(BF16)
            cb[lay - 2, :, cols] = c
            acc = acc + dot(c, w1b[lay, :, cols], 1, 1)
        dhid[...] = acc

    def back_weights(lay):
        e = eb[lay - 2]
        h_bf = hb[lay]
        for j in range(NB):
            cols = slice(j * D, (j + 1) * D)
            update2(lay, cols, ub[lay, :, cols], e)
            update1(lay, cols, h_bf, cb[lay - 2, :, cols])

    def reduce_stage1(p):
        for gi in range(3 * p, 3 * p + 3):
            _, c, u0, nu = GROUPS[gi]
            rows = pl.ds(pl.multiple_of(core * 64 + coord[dims_of(c)[0]] * 32, 32), 32)
            for cp in rs0_copies(gi):
                cp.wait_recv()
            for u in range(u0, u0 + nu):
                s1[p, u] = ((delta[p, u, rows, :].astype(F32) + raw[0, p, u].astype(F32))
                            + (raw[1, p, u].astype(F32) + raw[2, p, u].astype(F32)))
            stage_copy(RS1, gi).start()

    def reduce_stage2(p):
        for gi in range(3 * p, 3 * p + 3):
            _, c, u0, nu = GROUPS[gi]
            rows = pl.ds(pl.multiple_of(coord[dims_of(c)[1]] * 16, 16), 16)
            stage_copy(RS1, gi).wait_recv()
            for u in range(u0, u0 + nu):
                s2[p, u] = s1[p, u, rows, :] + r1[p, u]
            stage_copy(X2, gi).start()

    def reduce_stage3(p):
        for gi in range(3 * p, 3 * p + 3):
            _, c, u0, nu = GROUPS[gi]
            d0, d1, d2 = dims_of(c)
            rows = pl.ds(pl.multiple_of(core * 64 + coord[d0] * 32 + coord[d1] * 16, 16), 16)
            stage_copy(X2, gi).wait_recv()
            for u in range(u0, u0 + nu):
                full[p, u, rows, :] = s2[p, u] + r2[p, u]
            stage_copy(AG1, gi).start()

    def gather_stage2(p):
        for gi in range(3 * p, 3 * p + 3):
            stage_copy(AG1, gi).wait_recv()
            stage_copy(AG2, gi).start()
            stage_copy(DDA, gi).start()

    def gather_stage3(p):
        for gi in range(3 * p, 3 * p + 3):
            stage_copy(AG2, gi).wait_recv()
            stage_copy(DDB, gi).start()

    def outer_update(frag, p):
        part, mat = PIECES[p]
        lay = 2 * frag + part
        wr, wbr, gr, mr = (w1, w1b, g1, m1) if mat == 1 else (w2, w2b, g2, m2)
        m_load(mat, lay).wait()
        for gi in range(3 * p, 3 * p + 3):
            stage_copy(DDA, gi).wait_recv()
            stage_copy(DDB, gi).wait_recv()
        for u in range(8):
            rows, cols = unit_slice(mat, u)
            mean = full[p, u] * (1.0 / N_ALL)
            mom = OUTER_MOM * mr[lay, rows, cols] + mean
            glob = gr[lay, rows, cols] - OUTER_LR * (OUTER_MOM * mom + mean)
            mr[lay, rows, cols] = mom
            gr[lay, rows, cols] = glob
            merged = MERGE_MIX * wr[0, lay, rows, cols] + (1.0 - MERGE_MIX) * glob
            wr[0, lay, rows, cols] = merged
            wbr[lay, rows, cols] = merged.astype(BF16)

    last_piece = GATHER_ORDER[-1]

    def finish(frag):
        outer_update(frag, last_piece)
        for gi in range(12):
            for cp in rs0_copies(gi):
                cp.wait_send()
            for stage in range(6):
                stage_copy(stage, gi).wait_send()

    def sync(frag):
        reduce_stage1(3)
        for p in range(4):
            reduce_stage2(p)
        for p in range(4):
            reduce_stage3(p)
        for p in GATHER_ORDER:
            gather_stage2(p)
        prev = None
        for p in GATHER_ORDER:
            gather_stage3(p)
            if prev is not None:
                outer_update(frag, prev)
            prev = p

    def layers(lo, body):
        def run(i, _):
            body(i, lo - i)
            return 0
        return run

    def send_layer(lay, part):
        for p in (0, 2):
            @pl.when(part == PIECES[p][0])
            def _(p=p):
                make_delta(p, lay)
                make_delta(p + 1, lay)

    forward(0)
    for part, mat in PIECES:
        m_load(mat, part).start()
    for part, mat in PIECES:
        g_load(mat, 2 + part).start()
        m_load(mat, 2 + part).start()
    pl.semaphore_wait(bar, 7)
    loss_grad(0)
    lax.fori_loop(0, 2, layers(3, lambda i, lay: back_chain(lay)), 0)

    def back_send_0(i, lay):
        back_full(lay)
        send_layer(lay, lay)

    lax.fori_loop(0, 2, layers(1, back_send_0), 0)
    lax.fori_loop(0, 2, layers(3, lambda i, lay: back_weights(lay)), 0)

    def back_hook(i, lay):
        back_full(lay)

        @pl.when(i == 0)
        def _():
            reduce_stage1(0)
            reduce_stage1(1)

        @pl.when(i == 2)
        def _():
            reduce_stage1(2)

    forward(1)
    loss_grad(1)
    lax.fori_loop(0, L, layers(3, back_hook), 0)
    sync(0)

    forward(2, lambda: finish(0))
    loss_grad(2)

    def back_send_1(i, lay):
        back_full(lay)
        pl.when(i < 2)(lambda: send_layer(lay, lay - 2))

    lax.fori_loop(0, L, layers(3, back_send_1), 0)

    forward(3)
    loss_grad(3)
    lax.fori_loop(0, L, layers(3, back_hook), 0)
    sync(1)
    finish(1)


def write_body(*refs):
    srcs, dsts, sem = refs[:6], refs[6:12], refs[12]
    cps = []
    for i in range(6):
        for lay in range(L):
            src = srcs[i].at[0, lay] if i < 2 else srcs[i].at[lay]
            dst = dsts[i].at[0, lay] if i < 2 else dsts[i].at[lay]
            cps.append(pltpu.make_async_copy(src, dst, sem.at[i, lay]))
    for cp in cps:
        cp.start()
    for cp in cps:
        cp.wait()


def solution(mesh):
    def device_fn(w1_loc, w2_loc, w1_glb, w2_glb, mom1, mom2, x_loc, y_loc):
        arrays = (w1_loc, w2_loc, w1_glb, w2_glb, mom1, mom2)
        shapes = [jax.ShapeDtypeStruct(a.shape, F32) for a in arrays]
        dma = pltpu.SemaphoreType.DMA
        work = pl.pallas_call(
            main_body,
            out_shape=shapes,
            in_specs=[HBM] * 8,
            out_specs=[VMEM] * 6,
            scratch_shapes=[
                pltpu.VMEM((H, B, D), BF16), pltpu.VMEM((H, B, D), BF16),
                pltpu.VMEM((L, D, FF), BF16), pltpu.VMEM((L, FF, D), BF16),
                pltpu.VMEM((L, B, D), BF16), pltpu.VMEM((L, B, FF), BF16), pltpu.VMEM((L, B, FF), F32),
                pltpu.VMEM((B, D), F32), pltpu.VMEM((B, D), F32),
                pltpu.VMEM((2, B, D), BF16), pltpu.VMEM((2, B, FF), BF16),
                pltpu.VMEM((4, 8, 128, 256), BF16), pltpu.VMEM((3, 4, 8, 32, 256), BF16),
                pltpu.VMEM((4, 8, 32, 256), F32), pltpu.VMEM((4, 8, 16, 256), F32),
                pltpu.VMEM((4, 8, 16, 256), F32), pltpu.VMEM((4, 8, 16, 256), F32),
                pltpu.VMEM((4, 8, 128, 256), F32),
                dma((26,)), dma((12, 3)), dma((12, 3)), dma((6, 12)), dma((6, 12)),
            ],
            compiler_params=pltpu.CompilerParams(
                collective_id=0, has_side_effects=True, vmem_limit_bytes=28 * 2**20),
            name='diloco_round',
        )(*[pltpu.with_memory_space_constraint(a, pltpu.HBM) for a in (*arrays, x_loc, y_loc)])
        outs = pl.pallas_call(
            write_body,
            out_shape=shapes,
            in_specs=[VMEM] * 6,
            out_specs=[HBM] * 6,
            scratch_shapes=[dma((6, L))],
            compiler_params=pltpu.CompilerParams(vmem_limit_bytes=2 * 2**20),
            name='write_out',
        )(*work)
        return tuple(outs)

    local_spec = P(('shard', 'worker'))
    whole_spec = P()
    return jax.shard_map(device_fn, mesh=mesh, in_specs=(local_spec, local_spec, whole_spec, whole_spec, whole_spec, whole_spec, local_spec, local_spec), out_specs=(local_spec, local_spec, whole_spec, whole_spec, whole_spec, whole_spec), check_vma=False)
```

```python
import jax
import jax.numpy as jnp
from jax import lax
from jax.experimental import pallas as pl
from jax.experimental.pallas import tpu as pltpu
from jax.sharding import PartitionSpec as P

OUTER_LR = 0.7
OUTER_MOM = 0.9
MERGE_MIX = 0.5

L = 4
H = 4
D = 256
FF = 1024
B = 128
NB = FF // D
INNER_LR = 2.0 * D / (FF * L)
N_ALL = 16
F32 = jnp.float32
BF16 = jnp.bfloat16
MESH = pl.DeviceIdType.MESH
HBM = pl.BlockSpec(memory_space=pltpu.HBM)
VMEM = pl.BlockSpec(memory_space=pltpu.VMEM)

PIECES = ((1, 2), (1, 1), (0, 2), (0, 1))
COLOR_UNITS = ((3, 3, 2), (3, 2, 3), (2, 3, 3), (3, 3, 2))
GROUPS = []
for piece_idx in range(4):
    first_unit = 0
    for color in range(3):
        GROUPS.append((piece_idx, color, first_unit, COLOR_UNITS[piece_idx][color]))
        first_unit += COLOR_UNITS[piece_idx][color]
GATHER_ORDER = (0, 2, 3, 1)
RS1, X2, AG1, AG2, DDA, DDB = range(6)


def dot(a, b, ca, cb):
    return lax.dot_general(a, b, (((ca,), (cb,)), ((), ())), preferred_element_type=F32)


def gelu_pair(a):
    k0 = 0.7978845608028654
    k1 = k0 * 0.044715
    a2 = a * a
    t = jnp.tanh(a * (k0 + k1 * a2))
    h = 0.5 + 0.5 * t
    u = a * h
    du = h + (u * (1.0 - h)) * (2.0 * k0 + (6.0 * k1) * a2)
    return u, du


def unit_slice(mat, u):
    if mat == 2:
        return pl.ds(u * 128, 128), pl.ds(0, 256)
    return pl.ds((u % 2) * 128, 128), pl.ds((u // 2) * 256, 256)


def main_body(w1_in, w2_in, g1_in, g2_in, m1_in, m2_in, x_in, y_in,
              w1, w2, g1, g2, m1, m2, full,
              xb, yb, w1b, w2b, hb, ub, du, hid, dhid, eb, cb,
              delta, raw, s1, r1, s2, r2,
              ld_sem, s0_send, s0_recv, st_send, st_recv):
    zc = lax.axis_index('shard')
    wk = lax.axis_index('worker')
    core = lax.rem(wk, 2)
    xc = lax.rem(wk // 2, 2)
    yc = wk // 4
    coord = (xc, yc, zc)

    def chip_peer(dim, same_core=True):
        w = wk
        s = zc
        if dim == 0:
            w = wk + 2 - 4 * xc
        elif dim == 1:
            w = wk + 4 - 8 * yc
        elif dim == 2:
            s = 1 - zc
        if not same_core:
            w = w + 1 - 2 * core
        return (s, w)

    partner = chip_peer(3, False)

    bar = pltpu.get_barrier_semaphore()
    pl.semaphore_signal(bar, inc=1, device_id=partner, device_id_type=MESH)
    for dim in range(3):
        for same in (True, False):
            pl.semaphore_signal(bar, inc=1, device_id=chip_peer(dim, same), device_id_type=MESH)

    def w_load(lay):
        return (pltpu.make_async_copy(w1_in.at[0, lay], w1.at[0, lay], ld_sem.at[lay]),
                pltpu.make_async_copy(w2_in.at[0, lay], w2.at[0, lay], ld_sem.at[L + lay]))

    def g_load(mat, lay):
        if mat == 1:
            return pltpu.make_async_copy(g1_in.at[lay], g1.at[lay], ld_sem.at[2 * L + lay])
        return pltpu.make_async_copy(g2_in.at[lay], g2.at[lay], ld_sem.at[3 * L + lay])

    def m_load(mat, lay):
        if mat == 1:
            return pltpu.make_async_copy(m1_in.at[lay], m1.at[lay], ld_sem.at[4 * L + lay])
        return pltpu.make_async_copy(m2_in.at[lay], m2.at[lay], ld_sem.at[5 * L + lay])

    x_load = pltpu.make_async_copy(x_in.at[0], xb, ld_sem.at[6 * L])
    y_load = pltpu.make_async_copy(y_in.at[0], yb, ld_sem.at[6 * L + 1])
    x_load.start()
    for cp in w_load(0):
        cp.start()
    y_load.start()
    for lay in range(1, L):
        for cp in w_load(lay):
            cp.start()
    for lay in range(L):
        for mat in (1, 2):
            g_load(mat, lay).start()
    for lay in range(L):
        for mat in (1, 2):
            m_load(mat, lay).start()
    x_load.wait()
    y_load.wait()

    def dims_of(color_idx):
        return color_idx % 3, (color_idx + 1) % 3, (color_idx + 2) % 3

    def rs0_copies(gi):
        p, c, u0, nu = GROUPS[gi]
        d0 = dims_of(c)[0]
        k0 = coord[d0]
        us = pl.ds(u0, nu)
        other = 1 - core

        def rows(tc, blk):
            return pl.ds(pl.multiple_of(tc * 64 + blk * 32, 32), 32)

        out = []
        for idx, (tc, blk, dev) in enumerate(((other, k0, partner),
                                               (core, 1 - k0, chip_peer(d0, True)),
                                               (other, 1 - k0, chip_peer(d0, False)))):
            out.append(pltpu.make_async_remote_copy(
                src_ref=delta.at[p, us, rows(tc, blk)], dst_ref=raw.at[idx, p, us],
                send_sem=s0_send.at[gi, idx], recv_sem=s0_recv.at[gi, idx],
                device_id=dev, device_id_type=MESH))
        return out

    def stage_copy(stage, gi):
        p, c, u0, nu = GROUPS[gi]
        d0, d1, d2 = dims_of(c)
        k0, k1, k2 = coord[d0], coord[d1], coord[d2]
        us = pl.ds(u0, nu)
        if stage == RS1:
            src, dst, dev = s1.at[p, us, pl.ds(pl.multiple_of((1 - k1) * 16, 16), 16)], r1.at[p, us], chip_peer(d1)
        elif stage == X2:
            src, dst, dev = s2.at[p, us], r2.at[p, us], chip_peer(d2)
        else:
            base = core * 64
            if stage == AG1:
                off, n, dev = base + k0 * 32 + k1 * 16, 16, chip_peer(d1)
            elif stage == AG2:
                off, n, dev = base + k0 * 32, 32, chip_peer(d0)
            elif stage == DDA:
                off, n, dev = base + k0 * 32, 32, partner
            else:
                off, n, dev = base + (1 - k0) * 32, 32, partner
            src = full.at[p, us, pl.ds(pl.multiple_of(off, 16), n)]
            dst = src
        return pltpu.make_async_remote_copy(
            src_ref=src, dst_ref=dst, send_sem=st_send.at[stage, gi], recv_sem=st_recv.at[stage, gi],
            device_id=dev, device_id_type=MESH)

    def forward(k, before_layer_1=None):
        hid[...] = xb[k].astype(F32)

        def layer(lay, _):
            if k == 0:
                for cp in w_load(lay):
                    cp.wait()
            if before_layer_1 is not None:
                pl.when(lay == 1)(before_layer_1)
            h_bf = hid[...].astype(BF16)
            hb[lay] = h_bf
            acc = hid[...]
            for j in range(NB):
                cols = slice(j * D, (j + 1) * D)
                if k == 0:
                    w1b[lay, :, cols] = w1[0, lay, :, cols].astype(BF16)
                    w2b[lay, cols, :] = w2[0, lay, cols, :].astype(BF16)
                a = dot(h_bf, w1b[lay, :, cols], 1, 0)
                u, dg = gelu_pair(a)
                u_bf = u.astype(BF16)
                ub[lay, :, cols] = u_bf
                du[lay, :, cols] = dg
                acc = acc + dot(u_bf, w2b[lay, cols, :], 1, 0)
            hid[...] = acc
            return 0

        lax.fori_loop(0, L, layer, 0)

    def loss_grad(k):
        dhid[...] = (2.0 / (B * D)) * (hid[...] - yb[k].astype(F32))

    def update2(lay, cols, u_j, e):
        new2 = w2[0, lay, cols, :] - INNER_LR * dot(u_j, e, 0, 0)
        w2[0, lay, cols, :] = new2
        w2b[lay, cols, :] = new2.astype(BF16)

    def update1(lay, cols, h_bf, c):
        new1 = w1[0, lay, :, cols] - INNER_LR * dot(h_bf, c, 0, 0)
        w1[0, lay, :, cols] = new1
        w1b[lay, :, cols] = new1.astype(BF16)

    def send_piece(i, which):
        for p in (which, 2 + which):
            @pl.when(i == p // 2)
            def _(p=p):
                for gi in range(3 * p, 3 * p + 3):
                    for cp in rs0_copies(gi):
                        cp.start()

    def back_send(i, lay):
        p = 2 * i
        e = dhid[...].astype(BF16)
        h_bf = hb[lay]
        g_load(2, lay).wait()
        for j in range(NB):
            cols = slice(j * D, (j + 1) * D)
            new2 = w2[0, lay, cols, :] - INNER_LR * dot(ub[lay, :, cols], e, 0, 0)
            w2[0, lay, cols, :] = new2
            dl = (g2[lay, cols, :] - new2).astype(BF16)
            delta[p, 2 * j] = dl[:128]
            delta[p, 2 * j + 1] = dl[128:]
        send_piece(i, 0)
        g_load(1, lay).wait()
        acc = dhid[...]
        for j in range(NB):
            cols = slice(j * D, (j + 1) * D)
            d_u = dot(e, w2b[lay, cols, :], 1, 1)
            c = (du[lay, :, cols] * d_u).astype(BF16)
            acc = acc + dot(c, w1b[lay, :, cols], 1, 1)
            new1 = w1[0, lay, :, cols] - INNER_LR * dot(h_bf, c, 0, 0)
            w1[0, lay, :, cols] = new1
            w1b[lay, :, cols] = new1.astype(BF16)
            dl = (g1[lay, :, cols] - new1).astype(BF16)
            delta[p + 1, 2 * j] = dl[:128]
            delta[p + 1, 2 * j + 1] = dl[128:]
        dhid[...] = acc
        send_piece(i, 1)
        w2b[lay] = w2[0, lay].astype(BF16)

    def back_full(lay):
        e = dhid[...].astype(BF16)
        h_bf = hb[lay]
        acc = dhid[...]
        for j in range(NB):
            cols = slice(j * D, (j + 1) * D)
            d_u = dot(e, w2b[lay, cols, :], 1, 1)
            c = (du[lay, :, cols] * d_u).astype(BF16)
            update2(lay, cols, ub[lay, :, cols], e)
            acc = acc + dot(c, w1b[lay, :, cols], 1, 1)
            update1(lay, cols, h_bf, c)
        dhid[...] = acc

    def back_chain(lay):
        e = dhid[...].astype(BF16)
        eb[lay - 2] = e
        acc = dhid[...]
        for j in range(NB):
            cols = slice(j * D, (j + 1) * D)
            d_u = dot(e, w2b[lay, cols, :], 1, 1)
            c = (du[lay, :, cols] * d_u).astype(BF16)
            cb[lay - 2, :, cols] = c
            acc = acc + dot(c, w1b[lay, :, cols], 1, 1)
        dhid[...] = acc

    def back_weights(lay):
        e = eb[lay - 2]
        h_bf = hb[lay]
        for j in range(NB):
            cols = slice(j * D, (j + 1) * D)
            update2(lay, cols, ub[lay, :, cols], e)
            update1(lay, cols, h_bf, cb[lay - 2, :, cols])

    def reduce_stage1(p):
        for gi in range(3 * p, 3 * p + 3):
            _, c, u0, nu = GROUPS[gi]
            rows = pl.ds(pl.multiple_of(core * 64 + coord[dims_of(c)[0]] * 32, 32), 32)
            for cp in rs0_copies(gi):
                cp.wait_recv()
            for u in range(u0, u0 + nu):
                s1[p, u] = ((delta[p, u, rows, :].astype(F32) + raw[0, p, u].astype(F32))
                            + (raw[1, p, u].astype(F32) + raw[2, p, u].astype(F32)))
            stage_copy(RS1, gi).start()

    def reduce_stage2(p):
        for gi in range(3 * p, 3 * p + 3):
            _, c, u0, nu = GROUPS[gi]
            rows = pl.ds(pl.multiple_of(coord[dims_of(c)[1]] * 16, 16), 16)
            stage_copy(RS1, gi).wait_recv()
            for u in range(u0, u0 + nu):
                s2[p, u] = s1[p, u, rows, :] + r1[p, u]
            stage_copy(X2, gi).start()

    def reduce_stage3(p):
        for gi in range(3 * p, 3 * p + 3):
            _, c, u0, nu = GROUPS[gi]
            d0, d1, d2 = dims_of(c)
            rows = pl.ds(pl.multiple_of(core * 64 + coord[d0] * 32 + coord[d1] * 16, 16), 16)
            stage_copy(X2, gi).wait_recv()
            for u in range(u0, u0 + nu):
                full[p, u, rows, :] = s2[p, u] + r2[p, u]
            stage_copy(AG1, gi).start()

    def gather_stage2(p):
        for gi in range(3 * p, 3 * p + 3):
            stage_copy(AG1, gi).wait_recv()
            stage_copy(AG2, gi).start()
            stage_copy(DDA, gi).start()

    def gather_stage3(p):
        for gi in range(3 * p, 3 * p + 3):
            stage_copy(AG2, gi).wait_recv()
            stage_copy(DDB, gi).start()

    def outer_update(frag, p):
        part, mat = PIECES[p]
        lay = 2 * frag + part
        wr, wbr, gr, mr = (w1, w1b, g1, m1) if mat == 1 else (w2, w2b, g2, m2)
        m_load(mat, lay).wait()
        wait_gathered(p)
        for u in range(8):
            rows, cols = unit_slice(mat, u)
            mean = full[p, u] * (1.0 / N_ALL)
            mom = OUTER_MOM * mr[lay, rows, cols] + mean
            glob = gr[lay, rows, cols] - OUTER_LR * (OUTER_MOM * mom + mean)
            mr[lay, rows, cols] = mom
            gr[lay, rows, cols] = glob
            merged = MERGE_MIX * wr[0, lay, rows, cols] + (1.0 - MERGE_MIX) * glob
            wr[0, lay, rows, cols] = merged
            wbr[lay, rows, cols] = merged.astype(BF16)

    last_piece = GATHER_ORDER[-1]

    def wait_gathered(p):
        for gi in range(3 * p, 3 * p + 3):
            stage_copy(DDA, gi).wait_recv()
            stage_copy(DDB, gi).wait_recv()

    def finish(frag):
        if frag == 0:
            outer_update(frag, last_piece)
        else:
            for p, (part, mat) in enumerate(PIECES):
                m_load(mat, 2 + part).wait()
                wait_gathered(p)
        for gi in range(12):
            for cp in rs0_copies(gi):
                cp.wait_send()
            for stage in range(6):
                stage_copy(stage, gi).wait_send()

    def sync(frag):
        reduce_stage1(3)
        for p in range(4):
            reduce_stage2(p)
        for p in range(4):
            reduce_stage3(p)
        for p in GATHER_ORDER:
            gather_stage2(p)
        prev = None
        for p in GATHER_ORDER:
            gather_stage3(p)
            if prev is not None and frag == 0:
                outer_update(frag, prev)
            prev = p

    def layers(lo, body):
        def run(i, _):
            body(i, lo - i)
            return 0
        return run

    forward(0)
    pl.semaphore_wait(bar, 7)
    loss_grad(0)
    lax.fori_loop(0, 2, layers(3, lambda i, lay: back_chain(lay)), 0)

    lax.fori_loop(0, 2, layers(1, back_send), 0)
    lax.fori_loop(0, 2, layers(3, lambda i, lay: back_weights(lay)), 0)

    def back_hook(i, lay):
        back_full(lay)

        @pl.when(i == 0)
        def _():
            reduce_stage1(0)
            reduce_stage1(1)

        @pl.when(i == 2)
        def _():
            reduce_stage1(2)

    forward(1)
    loss_grad(1)
    lax.fori_loop(0, L, layers(3, back_hook), 0)
    sync(0)

    forward(2, lambda: finish(0))
    loss_grad(2)

    lax.fori_loop(0, 2, layers(3, back_send), 0)
    lax.fori_loop(0, 2, layers(1, lambda i, lay: back_full(lay)), 0)

    forward(3)
    loss_grad(3)
    lax.fori_loop(0, L, layers(3, back_hook), 0)
    sync(1)
    finish(1)


def write_body(w1, w2, g1, g2, m1, m2, full, *refs):
    dsts, stages, sem = refs[:6], refs[6:12], refs[12]
    srcs = (w1, w2, g1, g2, m1, m2)
    cps = []

    def put(src, i, lay):
        dst = dsts[i].at[0, lay] if i < 2 else dsts[i].at[lay]
        cp = pltpu.make_async_copy(src, dst, sem.at[i, lay])
        cp.start()
        cps.append(cp)

    for lay in range(2):
        for i in range(6):
            put(srcs[i].at[0, lay] if i < 2 else srcs[i].at[lay], i, lay)
    for p, (part, mat) in enumerate(PIECES):
        lay = 2 + part
        k = mat - 1
        wr, gr, mr = srcs[k], srcs[2 + k], srcs[4 + k]
        ws, gs, ms = stages[k], stages[2 + k], stages[4 + k]
        for u in range(8):
            rows, cols = unit_slice(mat, u)
            mean = full[p, u] * (1.0 / N_ALL)
            mom = OUTER_MOM * mr[lay, rows, cols] + mean
            glob = gr[lay, rows, cols] - OUTER_LR * (OUTER_MOM * mom + mean)
            ms[part, rows, cols] = mom
            gs[part, rows, cols] = glob
            ws[part, rows, cols] = MERGE_MIX * wr[0, lay, rows, cols] + (1.0 - MERGE_MIX) * glob
        for idx, st in enumerate((ws, gs, ms)):
            put(st.at[part], 2 * idx + k, lay)
    for cp in cps:
        cp.wait()


def solution(mesh):
    def device_fn(w1_loc, w2_loc, w1_glb, w2_glb, mom1, mom2, x_loc, y_loc):
        arrays = (w1_loc, w2_loc, w1_glb, w2_glb, mom1, mom2)
        shapes = [jax.ShapeDtypeStruct(a.shape, F32) for a in arrays]
        dma = pltpu.SemaphoreType.DMA
        work = pl.pallas_call(
            main_body,
            out_shape=shapes + [jax.ShapeDtypeStruct((4, 8, 128, 256), F32)],
            in_specs=[HBM] * 8,
            out_specs=[VMEM] * 7,
            scratch_shapes=[
                pltpu.VMEM((H, B, D), BF16), pltpu.VMEM((H, B, D), BF16),
                pltpu.VMEM((L, D, FF), BF16), pltpu.VMEM((L, FF, D), BF16),
                pltpu.VMEM((L, B, D), BF16), pltpu.VMEM((L, B, FF), BF16), pltpu.VMEM((L, B, FF), F32),
                pltpu.VMEM((B, D), F32), pltpu.VMEM((B, D), F32),
                pltpu.VMEM((2, B, D), BF16), pltpu.VMEM((2, B, FF), BF16),
                pltpu.VMEM((4, 8, 128, 256), BF16), pltpu.VMEM((3, 4, 8, 32, 256), BF16),
                pltpu.VMEM((4, 8, 32, 256), F32), pltpu.VMEM((4, 8, 16, 256), F32),
                pltpu.VMEM((4, 8, 16, 256), F32), pltpu.VMEM((4, 8, 16, 256), F32),
                dma((26,)), dma((12, 3)), dma((12, 3)), dma((6, 12)), dma((6, 12)),
            ],
            compiler_params=pltpu.CompilerParams(
                collective_id=0, has_side_effects=True, vmem_limit_bytes=22 * 2**20),
            name='diloco_round',
        )(*[pltpu.with_memory_space_constraint(a, pltpu.HBM) for a in (*arrays, x_loc, y_loc)])
        outs = pl.pallas_call(
            write_body,
            out_shape=shapes,
            in_specs=[VMEM] * 7,
            out_specs=[HBM] * 6,
            scratch_shapes=[pltpu.VMEM((2, D, FF), F32), pltpu.VMEM((2, FF, D), F32)] * 3 + [dma((6, L))],
            compiler_params=pltpu.CompilerParams(vmem_limit_bytes=16 * 2**20),
            name='write_out',
        )(*work)
        return tuple(outs)

    local_spec = P(('shard', 'worker'))
    whole_spec = P()
    return jax.shard_map(device_fn, mesh=mesh, in_specs=(local_spec, local_spec, whole_spec, whole_spec, whole_spec, whole_spec, local_spec, local_spec), out_specs=(local_spec, local_spec, whole_spec, whole_spec, whole_spec, whole_spec), check_vma=False)
```

```python
import jax
import jax.numpy as jnp
from jax import lax
from jax.experimental import pallas as pl
from jax.experimental.pallas import tpu as pltpu
from jax.sharding import PartitionSpec as P

OUTER_LR = 0.7
OUTER_MOM = 0.9
MERGE_MIX = 0.5

L = 4
H = 4
D = 256
FF = 1024
B = 128
NB = FF // D
INNER_LR = 2.0 * D / (FF * L)
N_ALL = 16
F32 = jnp.float32
BF16 = jnp.bfloat16
MESH = pl.DeviceIdType.MESH
HBM = pl.BlockSpec(memory_space=pltpu.HBM)
VMEM = pl.BlockSpec(memory_space=pltpu.VMEM)

PIECES = ((1, 2), (1, 1), (0, 2), (0, 1))
COLOR_UNITS = ((3, 3, 2), (3, 2, 3), (2, 3, 3), (3, 3, 2))
GROUPS = []
for piece_idx in range(4):
    first_unit = 0
    for color in range(3):
        GROUPS.append((piece_idx, color, first_unit, COLOR_UNITS[piece_idx][color]))
        first_unit += COLOR_UNITS[piece_idx][color]
GATHER_ORDER = (0, 2, 3, 1)
RS1, X2, AG1, AG2, DDA, DDB = range(6)


def dot(a, b, ca, cb):
    return lax.dot_general(a, b, (((ca,), (cb,)), ((), ())), preferred_element_type=F32)


def gelu_pair(a):
    k0 = 0.7978845608028654
    k1 = k0 * 0.044715
    a2 = a * a
    t = jnp.tanh(a * (k0 + k1 * a2))
    h = 0.5 + 0.5 * t
    u = a * h
    du = h + (u * (1.0 - h)) * (2.0 * k0 + (6.0 * k1) * a2)
    return u, du


def unit_slice(mat, u):
    if mat == 2:
        return pl.ds(u * 128, 128), pl.ds(0, 256)
    return pl.ds((u % 2) * 128, 128), pl.ds((u // 2) * 256, 256)


def main_body(w1_in, w2_in, g1_in, g2_in, m1_in, m2_in, x_in, y_in,
              w1, w2, g1, g2, m1, m2, full,
              xb, yb, w1b, w2b, hb, ub, du, hid, dhid, eb, cb,
              delta, raw, s1, r1, s2, r2,
              ld_sem, s0_send, s0_recv, st_send, st_recv):
    zc = lax.axis_index('shard')
    wk = lax.axis_index('worker')
    core = lax.rem(wk, 2)
    xc = lax.rem(wk // 2, 2)
    yc = wk // 4
    coord = (xc, yc, zc)

    def chip_peer(dim, same_core=True):
        w = wk
        s = zc
        if dim == 0:
            w = wk + 2 - 4 * xc
        elif dim == 1:
            w = wk + 4 - 8 * yc
        elif dim == 2:
            s = 1 - zc
        if not same_core:
            w = w + 1 - 2 * core
        return (s, w)

    partner = chip_peer(3, False)

    bar = pltpu.get_barrier_semaphore()
    pl.semaphore_signal(bar, inc=1, device_id=partner, device_id_type=MESH)
    for dim in range(3):
        for same in (True, False):
            pl.semaphore_signal(bar, inc=1, device_id=chip_peer(dim, same), device_id_type=MESH)

    def w_load(lay):
        return (pltpu.make_async_copy(w1_in.at[0, lay], w1.at[0, lay], ld_sem.at[lay]),
                pltpu.make_async_copy(w2_in.at[0, lay], w2.at[0, lay], ld_sem.at[L + lay]))

    def g_load(mat, lay):
        if mat == 1:
            return pltpu.make_async_copy(g1_in.at[lay], g1.at[lay], ld_sem.at[2 * L + lay])
        return pltpu.make_async_copy(g2_in.at[lay], g2.at[lay], ld_sem.at[3 * L + lay])

    def m_load(mat, lay):
        if mat == 1:
            return pltpu.make_async_copy(m1_in.at[lay], m1.at[lay], ld_sem.at[4 * L + lay])
        return pltpu.make_async_copy(m2_in.at[lay], m2.at[lay], ld_sem.at[5 * L + lay])

    x_load = pltpu.make_async_copy(x_in.at[0], xb, ld_sem.at[6 * L])
    y_load = pltpu.make_async_copy(y_in.at[0], yb, ld_sem.at[6 * L + 1])
    x_load.start()
    for cp in w_load(0):
        cp.start()
    y_load.start()
    for lay in range(1, L):
        for cp in w_load(lay):
            cp.start()
    for lay in range(L):
        for mat in (1, 2):
            g_load(mat, lay).start()
    for lay in range(L):
        for mat in (1, 2):
            m_load(mat, lay).start()
    x_load.wait()
    y_load.wait()

    def dims_of(color_idx):
        return color_idx % 3, (color_idx + 1) % 3, (color_idx + 2) % 3

    def rs0_copies(gi):
        p, c, u0, nu = GROUPS[gi]
        d0 = dims_of(c)[0]
        k0 = coord[d0]
        us = pl.ds(u0, nu)
        other = 1 - core

        def rows(tc, blk):
            return pl.ds(pl.multiple_of(tc * 64 + blk * 32, 32), 32)

        out = []
        for idx, (tc, blk, dev) in enumerate(((other, k0, partner),
                                               (core, 1 - k0, chip_peer(d0, True)),
                                               (other, 1 - k0, chip_peer(d0, False)))):
            out.append(pltpu.make_async_remote_copy(
                src_ref=delta.at[p, us, rows(tc, blk)], dst_ref=raw.at[idx, p, us],
                send_sem=s0_send.at[gi, idx], recv_sem=s0_recv.at[gi, idx],
                device_id=dev, device_id_type=MESH))
        return out

    def stage_copy(stage, gi):
        p, c, u0, nu = GROUPS[gi]
        d0, d1, d2 = dims_of(c)
        k0, k1, k2 = coord[d0], coord[d1], coord[d2]
        us = pl.ds(u0, nu)
        if stage == RS1:
            src, dst, dev = s1.at[p, us, pl.ds(pl.multiple_of((1 - k1) * 16, 16), 16)], r1.at[p, us], chip_peer(d1)
        elif stage == X2:
            src, dst, dev = s2.at[p, us], r2.at[p, us], chip_peer(d2)
        else:
            base = core * 64
            if stage == AG1:
                off, n, dev = base + k0 * 32 + k1 * 16, 16, chip_peer(d1)
            elif stage == AG2:
                off, n, dev = base + k0 * 32, 32, chip_peer(d0)
            elif stage == DDA:
                off, n, dev = base + k0 * 32, 32, partner
            else:
                off, n, dev = base + (1 - k0) * 32, 32, partner
            src = full.at[p, us, pl.ds(pl.multiple_of(off, 16), n)]
            dst = src
        return pltpu.make_async_remote_copy(
            src_ref=src, dst_ref=dst, send_sem=st_send.at[stage, gi], recv_sem=st_recv.at[stage, gi],
            device_id=dev, device_id_type=MESH)

    def forward(k, before_layer_1=None):
        hid[...] = xb[k].astype(F32)

        def layer(lay, _):
            if k == 0:
                for cp in w_load(lay):
                    cp.wait()
            if before_layer_1 is not None:
                pl.when(lay == 1)(before_layer_1)
            h_bf = hid[...].astype(BF16)
            hb[lay] = h_bf
            acc = hid[...]
            for j in range(NB):
                cols = slice(j * D, (j + 1) * D)
                if k == 0:
                    w1b[lay, :, cols] = w1[0, lay, :, cols].astype(BF16)
                    w2b[lay, cols, :] = w2[0, lay, cols, :].astype(BF16)
                a = dot(h_bf, w1b[lay, :, cols], 1, 0)
                u, dg = gelu_pair(a)
                u_bf = u.astype(BF16)
                ub[lay, :, cols] = u_bf
                du[lay, :, cols] = dg
                acc = acc + dot(u_bf, w2b[lay, cols, :], 1, 0)
            hid[...] = acc
            return 0

        lax.fori_loop(0, L, layer, 0)

    def loss_grad(k):
        dhid[...] = (2.0 / (B * D)) * (hid[...] - yb[k].astype(F32))

    def update2(lay, cols, u_j, e):
        new2 = w2[0, lay, cols, :] - INNER_LR * dot(u_j, e, 0, 0)
        w2[0, lay, cols, :] = new2
        w2b[lay, cols, :] = new2.astype(BF16)

    def update1(lay, cols, h_bf, c):
        new1 = w1[0, lay, :, cols] - INNER_LR * dot(h_bf, c, 0, 0)
        w1[0, lay, :, cols] = new1
        w1b[lay, :, cols] = new1.astype(BF16)

    def send_piece(i, which):
        for p in (which, 2 + which):
            @pl.when(i == p // 2)
            def _(p=p):
                for gi in range(3 * p, 3 * p + 3):
                    for cp in rs0_copies(gi):
                        cp.start()

    def back_send(i, lay):
        p = 2 * i
        e = dhid[...].astype(BF16)
        h_bf = hb[lay]
        g_load(2, lay).wait()
        for j in range(NB):
            cols = slice(j * D, (j + 1) * D)
            new2 = w2[0, lay, cols, :] - INNER_LR * dot(ub[lay, :, cols], e, 0, 0)
            w2[0, lay, cols, :] = new2
            dl = (g2[lay, cols, :] - new2).astype(BF16)
            delta[p, 2 * j] = dl[:128]
            delta[p, 2 * j + 1] = dl[128:]
        send_piece(i, 0)
        g_load(1, lay).wait()
        acc = dhid[...]
        for j in range(NB):
            cols = slice(j * D, (j + 1) * D)
            d_u = dot(e, w2b[lay, cols, :], 1, 1)
            c = (du[lay, :, cols] * d_u).astype(BF16)
            acc = acc + dot(c, w1b[lay, :, cols], 1, 1)
            new1 = w1[0, lay, :, cols] - INNER_LR * dot(h_bf, c, 0, 0)
            w1[0, lay, :, cols] = new1
            w1b[lay, :, cols] = new1.astype(BF16)
            dl = (g1[lay, :, cols] - new1).astype(BF16)
            delta[p + 1, 2 * j] = dl[:128]
            delta[p + 1, 2 * j + 1] = dl[128:]
        dhid[...] = acc
        send_piece(i, 1)
        w2b[lay] = w2[0, lay].astype(BF16)

    def back_full(lay):
        e = dhid[...].astype(BF16)
        h_bf = hb[lay]
        acc = dhid[...]
        for j in range(NB):
            cols = slice(j * D, (j + 1) * D)
            d_u = dot(e, w2b[lay, cols, :], 1, 1)
            c = (du[lay, :, cols] * d_u).astype(BF16)
            update2(lay, cols, ub[lay, :, cols], e)
            acc = acc + dot(c, w1b[lay, :, cols], 1, 1)
            update1(lay, cols, h_bf, c)
        dhid[...] = acc

    def back_chain(lay):
        e = dhid[...].astype(BF16)
        eb[lay - 2] = e
        acc = dhid[...]
        for j in range(NB):
            cols = slice(j * D, (j + 1) * D)
            d_u = dot(e, w2b[lay, cols, :], 1, 1)
            c = (du[lay, :, cols] * d_u).astype(BF16)
            cb[lay - 2, :, cols] = c
            acc = acc + dot(c, w1b[lay, :, cols], 1, 1)
        dhid[...] = acc

    def back_weights(lay):
        e = eb[lay - 2]
        h_bf = hb[lay]
        for j in range(NB):
            cols = slice(j * D, (j + 1) * D)
            update2(lay, cols, ub[lay, :, cols], e)
            update1(lay, cols, h_bf, cb[lay - 2, :, cols])

    def reduce_stage1(p):
        for gi in range(3 * p, 3 * p + 3):
            _, c, u0, nu = GROUPS[gi]
            rows = pl.ds(pl.multiple_of(core * 64 + coord[dims_of(c)[0]] * 32, 32), 32)
            for cp in rs0_copies(gi):
                cp.wait_recv()
            for u in range(u0, u0 + nu):
                s1[p, u] = ((delta[p, u, rows, :].astype(F32) + raw[0, p, u].astype(F32))
                            + (raw[1, p, u].astype(F32) + raw[2, p, u].astype(F32)))
            stage_copy(RS1, gi).start()

    def reduce_stage2(p):
        for gi in range(3 * p, 3 * p + 3):
            _, c, u0, nu = GROUPS[gi]
            rows = pl.ds(pl.multiple_of(coord[dims_of(c)[1]] * 16, 16), 16)
            stage_copy(RS1, gi).wait_recv()
            for u in range(u0, u0 + nu):
                s2[p, u] = s1[p, u, rows, :] + r1[p, u]
            stage_copy(X2, gi).start()

    def reduce_stage3(p):
        for gi in range(3 * p, 3 * p + 3):
            _, c, u0, nu = GROUPS[gi]
            d0, d1, d2 = dims_of(c)
            rows = pl.ds(pl.multiple_of(core * 64 + coord[d0] * 32 + coord[d1] * 16, 16), 16)
            stage_copy(X2, gi).wait_recv()
            for u in range(u0, u0 + nu):
                full[p, u, rows, :] = s2[p, u] + r2[p, u]
            stage_copy(AG1, gi).start()

    def gather_stage2(p):
        for gi in range(3 * p, 3 * p + 3):
            stage_copy(AG1, gi).wait_recv()
            stage_copy(AG2, gi).start()
            stage_copy(DDA, gi).start()

    def gather_stage3(p):
        for gi in range(3 * p, 3 * p + 3):
            stage_copy(AG2, gi).wait_recv()
            stage_copy(DDB, gi).start()

    def outer_update(frag, p):
        part, mat = PIECES[p]
        lay = 2 * frag + part
        wr, wbr, gr, mr = (w1, w1b, g1, m1) if mat == 1 else (w2, w2b, g2, m2)
        m_load(mat, lay).wait()
        wait_gathered(p)
        for u in range(8):
            rows, cols = unit_slice(mat, u)
            mean = full[p, u] * (1.0 / N_ALL)
            mom = OUTER_MOM * mr[lay, rows, cols] + mean
            glob = gr[lay, rows, cols] - OUTER_LR * (OUTER_MOM * mom + mean)
            mr[lay, rows, cols] = mom
            gr[lay, rows, cols] = glob
            merged = MERGE_MIX * wr[0, lay, rows, cols] + (1.0 - MERGE_MIX) * glob
            wr[0, lay, rows, cols] = merged
            wbr[lay, rows, cols] = merged.astype(BF16)

    last_piece = GATHER_ORDER[-1]

    def wait_gathered(p):
        for gi in range(3 * p, 3 * p + 3):
            stage_copy(DDA, gi).wait_recv()
            stage_copy(DDB, gi).wait_recv()

    def finish(frag):
        if frag == 0:
            outer_update(frag, last_piece)
        else:
            for p, (part, mat) in enumerate(PIECES):
                m_load(mat, 2 + part).wait()
                wait_gathered(p)
        for gi in range(12):
            for cp in rs0_copies(gi):
                cp.wait_send()
            for stage in range(6):
                stage_copy(stage, gi).wait_send()

    def sync(frag):
        for p in range(4):
            reduce_stage2(p)
        for p in range(4):
            reduce_stage3(p)
        for p in GATHER_ORDER:
            gather_stage2(p)
        prev = None
        for p in GATHER_ORDER:
            gather_stage3(p)
            if prev is not None and frag == 0:
                outer_update(frag, prev)
            prev = p

    def layers(lo, body):
        def run(i, _):
            body(i, lo - i)
            return 0
        return run

    forward(0)
    pl.semaphore_wait(bar, 7)
    loss_grad(0)
    lax.fori_loop(0, 2, layers(3, lambda i, lay: back_chain(lay)), 0)

    lax.fori_loop(0, 2, layers(1, back_send), 0)
    lax.fori_loop(0, 2, layers(3, lambda i, lay: back_weights(lay)), 0)

    def back_hook(i, lay):
        back_full(lay)

        for p in range(1, 4):
            @pl.when(i == p - 1)
            def _(p=p):
                reduce_stage1(p)

    forward(1)
    loss_grad(1)
    reduce_stage1(0)
    lax.fori_loop(0, L, layers(3, back_hook), 0)
    sync(0)

    forward(2, lambda: finish(0))
    loss_grad(2)

    lax.fori_loop(0, 2, layers(3, back_send), 0)
    lax.fori_loop(0, 2, layers(1, lambda i, lay: back_full(lay)), 0)

    forward(3)
    loss_grad(3)
    reduce_stage1(0)
    lax.fori_loop(0, L, layers(3, back_hook), 0)
    sync(1)
    finish(1)


def write_body(w1, w2, g1, g2, m1, m2, full, *refs):
    dsts, stages, sem = refs[:6], refs[6:12], refs[12]
    srcs = (w1, w2, g1, g2, m1, m2)
    cps = []

    def put(src, i, lay):
        dst = dsts[i].at[0, lay] if i < 2 else dsts[i].at[lay]
        cp = pltpu.make_async_copy(src, dst, sem.at[i, lay])
        cp.start()
        cps.append(cp)

    for lay in range(2):
        for i in range(6):
            put(srcs[i].at[0, lay] if i < 2 else srcs[i].at[lay], i, lay)
    for p, (part, mat) in enumerate(PIECES):
        lay = 2 + part
        k = mat - 1
        wr, gr, mr = srcs[k], srcs[2 + k], srcs[4 + k]
        ws, gs, ms = stages[k], stages[2 + k], stages[4 + k]
        for u in range(8):
            rows, cols = unit_slice(mat, u)
            mean = full[p, u] * (1.0 / N_ALL)
            mom = OUTER_MOM * mr[lay, rows, cols] + mean
            glob = gr[lay, rows, cols] - OUTER_LR * (OUTER_MOM * mom + mean)
            ms[part, rows, cols] = mom
            gs[part, rows, cols] = glob
            ws[part, rows, cols] = MERGE_MIX * wr[0, lay, rows, cols] + (1.0 - MERGE_MIX) * glob
        for idx, st in enumerate((ws, gs, ms)):
            put(st.at[part], 2 * idx + k, lay)
    for cp in cps:
        cp.wait()


def solution(mesh):
    def device_fn(w1_loc, w2_loc, w1_glb, w2_glb, mom1, mom2, x_loc, y_loc):
        arrays = (w1_loc, w2_loc, w1_glb, w2_glb, mom1, mom2)
        shapes = [jax.ShapeDtypeStruct(a.shape, F32) for a in arrays]
        dma = pltpu.SemaphoreType.DMA
        work = pl.pallas_call(
            main_body,
            out_shape=shapes + [jax.ShapeDtypeStruct((4, 8, 128, 256), F32)],
            in_specs=[HBM] * 8,
            out_specs=[VMEM] * 7,
            scratch_shapes=[
                pltpu.VMEM((H, B, D), BF16), pltpu.VMEM((H, B, D), BF16),
                pltpu.VMEM((L, D, FF), BF16), pltpu.VMEM((L, FF, D), BF16),
                pltpu.VMEM((L, B, D), BF16), pltpu.VMEM((L, B, FF), BF16), pltpu.VMEM((L, B, FF), F32),
                pltpu.VMEM((B, D), F32), pltpu.VMEM((B, D), F32),
                pltpu.VMEM((2, B, D), BF16), pltpu.VMEM((2, B, FF), BF16),
                pltpu.VMEM((4, 8, 128, 256), BF16), pltpu.VMEM((3, 4, 8, 32, 256), BF16),
                pltpu.VMEM((4, 8, 32, 256), F32), pltpu.VMEM((4, 8, 16, 256), F32),
                pltpu.VMEM((4, 8, 16, 256), F32), pltpu.VMEM((4, 8, 16, 256), F32),
                dma((26,)), dma((12, 3)), dma((12, 3)), dma((6, 12)), dma((6, 12)),
            ],
            compiler_params=pltpu.CompilerParams(
                collective_id=0, has_side_effects=True, vmem_limit_bytes=22 * 2**20),
            name='diloco_round',
        )(*[pltpu.with_memory_space_constraint(a, pltpu.HBM) for a in (*arrays, x_loc, y_loc)])
        outs = pl.pallas_call(
            write_body,
            out_shape=shapes,
            in_specs=[VMEM] * 7,
            out_specs=[HBM] * 6,
            scratch_shapes=[pltpu.VMEM((2, D, FF), F32), pltpu.VMEM((2, FF, D), F32)] * 3 + [dma((6, L))],
            compiler_params=pltpu.CompilerParams(vmem_limit_bytes=16 * 2**20),
            name='write_out',
        )(*work)
        return tuple(outs)

    local_spec = P(('shard', 'worker'))
    whole_spec = P()
    return jax.shard_map(device_fn, mesh=mesh, in_specs=(local_spec, local_spec, whole_spec, whole_spec, whole_spec, whole_spec, local_spec, local_spec), out_specs=(local_spec, local_spec, whole_spec, whole_spec, whole_spec, whole_spec), check_vma=False)
```

```python
import jax
import jax.numpy as jnp
from jax import lax
from jax.experimental import pallas as pl
from jax.experimental.pallas import tpu as pltpu
from jax.sharding import PartitionSpec as P

OUTER_LR = 0.7
OUTER_MOM = 0.9
MERGE_MIX = 0.5

L = 4
H = 4
D = 256
FF = 1024
B = 128
NB = FF // D
INNER_LR = 2.0 * D / (FF * L)
N_ALL = 16
F32 = jnp.float32
BF16 = jnp.bfloat16
MESH = pl.DeviceIdType.MESH
HBM = pl.BlockSpec(memory_space=pltpu.HBM)
VMEM = pl.BlockSpec(memory_space=pltpu.VMEM)

PIECES = ((1, 2), (1, 1), (0, 2), (0, 1))
COLOR_UNITS = ((3, 3, 2), (3, 2, 3), (2, 3, 3), (3, 3, 2))
GROUPS = []
for piece_idx in range(4):
    first_unit = 0
    for color in range(3):
        GROUPS.append((piece_idx, color, first_unit, COLOR_UNITS[piece_idx][color]))
        first_unit += COLOR_UNITS[piece_idx][color]
GATHER_ORDER = (0, 2, 3, 1)
RS1, X2, AG1, AG2, DDA, DDB = range(6)


def dot(a, b, ca, cb):
    return lax.dot_general(a, b, (((ca,), (cb,)), ((), ())), preferred_element_type=F32)


def gelu_pair(a):
    k0 = 0.7978845608028654
    k1 = k0 * 0.044715
    a2 = a * a
    t = jnp.tanh(a * (k0 + k1 * a2))
    h = 0.5 + 0.5 * t
    u = a * h
    du = h + (u * (1.0 - h)) * (2.0 * k0 + (6.0 * k1) * a2)
    return u, du


def unit_slice(mat, u):
    if mat == 2:
        return pl.ds(u * 128, 128), pl.ds(0, 256)
    return pl.ds((u % 2) * 128, 128), pl.ds((u // 2) * 256, 256)


def main_body(w1_in, w2_in, g1_in, g2_in, m1_in, m2_in, x_in, y_in,
              w1, w2, g1, g2, m1, m2, full,
              xb, yb, w1b, w2b, hb, ub, du, hid, dhid, eb, cb,
              delta, raw, s1, r1, s2, r2,
              ld_sem, s0_send, s0_recv, st_send, st_recv):
    zc = lax.axis_index('shard')
    wk = lax.axis_index('worker')
    core = lax.rem(wk, 2)
    xc = lax.rem(wk // 2, 2)
    yc = wk // 4
    coord = (xc, yc, zc)

    def chip_peer(dim, same_core=True):
        w = wk
        s = zc
        if dim == 0:
            w = wk + 2 - 4 * xc
        elif dim == 1:
            w = wk + 4 - 8 * yc
        elif dim == 2:
            s = 1 - zc
        if not same_core:
            w = w + 1 - 2 * core
        return (s, w)

    partner = chip_peer(3, False)

    bar = pltpu.get_barrier_semaphore()
    pl.semaphore_signal(bar, inc=1, device_id=partner, device_id_type=MESH)
    for dim in range(3):
        for same in (True, False):
            pl.semaphore_signal(bar, inc=1, device_id=chip_peer(dim, same), device_id_type=MESH)

    def w_load(lay):
        return (pltpu.make_async_copy(w1_in.at[0, lay], w1.at[0, lay], ld_sem.at[lay]),
                pltpu.make_async_copy(w2_in.at[0, lay], w2.at[0, lay], ld_sem.at[L + lay]))

    def g_load(mat, lay):
        if mat == 1:
            return pltpu.make_async_copy(g1_in.at[lay], g1.at[lay], ld_sem.at[2 * L + lay])
        return pltpu.make_async_copy(g2_in.at[lay], g2.at[lay], ld_sem.at[3 * L + lay])

    def m_load(mat, lay):
        if mat == 1:
            return pltpu.make_async_copy(m1_in.at[lay], m1.at[lay], ld_sem.at[4 * L + lay])
        return pltpu.make_async_copy(m2_in.at[lay], m2.at[lay], ld_sem.at[5 * L + lay])

    x_load = pltpu.make_async_copy(x_in.at[0], xb, ld_sem.at[6 * L])
    y_load = pltpu.make_async_copy(y_in.at[0], yb, ld_sem.at[6 * L + 1])
    x_load.start()
    for cp in w_load(0):
        cp.start()
    y_load.start()
    for lay in range(1, L):
        for cp in w_load(lay):
            cp.start()
    for lay in range(L):
        for mat in (1, 2):
            g_load(mat, lay).start()
    for lay in range(L):
        for mat in (1, 2):
            m_load(mat, lay).start()
    x_load.wait()
    y_load.wait()

    def dims_of(color_idx):
        return color_idx % 3, (color_idx + 1) % 3, (color_idx + 2) % 3

    def rs0_copies(gi):
        p, c, u0, nu = GROUPS[gi]
        d0 = dims_of(c)[0]
        k0 = coord[d0]
        us = pl.ds(u0, nu)
        other = 1 - core

        def rows(tc, blk):
            return pl.ds(pl.multiple_of(tc * 64 + blk * 32, 32), 32)

        out = []
        for idx, (tc, blk, dev) in enumerate(((other, k0, partner),
                                               (core, 1 - k0, chip_peer(d0, True)),
                                               (other, 1 - k0, chip_peer(d0, False)))):
            out.append(pltpu.make_async_remote_copy(
                src_ref=delta.at[p, us, rows(tc, blk)], dst_ref=raw.at[idx, p, us],
                send_sem=s0_send.at[gi, idx], recv_sem=s0_recv.at[gi, idx],
                device_id=dev, device_id_type=MESH))
        return out

    def stage_copy(stage, gi):
        p, c, u0, nu = GROUPS[gi]
        d0, d1, d2 = dims_of(c)
        k0, k1, k2 = coord[d0], coord[d1], coord[d2]
        us = pl.ds(u0, nu)
        if stage == RS1:
            src, dst, dev = s1.at[p, us, pl.ds(pl.multiple_of((1 - k1) * 16, 16), 16)], r1.at[p, us], chip_peer(d1)
        elif stage == X2:
            src, dst, dev = s2.at[p, us], r2.at[p, us], chip_peer(d2)
        else:
            base = core * 64
            if stage == AG1:
                off, n, dev = base + k0 * 32 + k1 * 16, 16, chip_peer(d1)
            elif stage == AG2:
                off, n, dev = base + k0 * 32, 32, chip_peer(d0)
            elif stage == DDA:
                off, n, dev = base + k0 * 32, 32, partner
            else:
                off, n, dev = base + (1 - k0) * 32, 32, partner
            src = full.at[p, us, pl.ds(pl.multiple_of(off, 16), n)]
            dst = src
        return pltpu.make_async_remote_copy(
            src_ref=src, dst_ref=dst, send_sem=st_send.at[stage, gi], recv_sem=st_recv.at[stage, gi],
            device_id=dev, device_id_type=MESH)

    def forward(k, before_layer_1=None):
        hid[...] = xb[k].astype(F32)

        def layer(lay, _):
            if k == 0:
                for cp in w_load(lay):
                    cp.wait()
            if before_layer_1 is not None:
                pl.when(lay == 1)(before_layer_1)
            h_bf = hid[...].astype(BF16)
            hb[lay] = h_bf
            acc = hid[...]
            for j in range(NB):
                cols = slice(j * D, (j + 1) * D)
                if k == 0:
                    w1b[lay, :, cols] = w1[0, lay, :, cols].astype(BF16)
                    w2b[lay, cols, :] = w2[0, lay, cols, :].astype(BF16)
                a = dot(h_bf, w1b[lay, :, cols], 1, 0)
                u, dg = gelu_pair(a)
                u_bf = u.astype(BF16)
                ub[lay, :, cols] = u_bf
                du[lay, :, cols] = dg
                acc = acc + dot(u_bf, w2b[lay, cols, :], 1, 0)
            hid[...] = acc
            return 0

        lax.fori_loop(0, L, layer, 0)

    def loss_grad(k):
        dhid[...] = (2.0 / (B * D)) * (hid[...] - yb[k].astype(F32))

    def update2(lay, cols, u_j, e):
        new2 = w2[0, lay, cols, :] - INNER_LR * dot(u_j, e, 0, 0)
        w2[0, lay, cols, :] = new2
        w2b[lay, cols, :] = new2.astype(BF16)

    def update1(lay, cols, h_bf, c):
        new1 = w1[0, lay, :, cols] - INNER_LR * dot(h_bf, c, 0, 0)
        w1[0, lay, :, cols] = new1
        w1b[lay, :, cols] = new1.astype(BF16)

    def send_piece(i, which):
        for p in (which, 2 + which):
            @pl.when(i == p // 2)
            def _(p=p):
                for gi in range(3 * p, 3 * p + 3):
                    for cp in rs0_copies(gi):
                        cp.start()

    def back_send(i, lay, after_first=None):
        p = 2 * i
        e = dhid[...].astype(BF16)
        h_bf = hb[lay]
        g_load(2, lay).wait()
        for j in range(NB):
            cols = slice(j * D, (j + 1) * D)
            new2 = w2[0, lay, cols, :] - INNER_LR * dot(ub[lay, :, cols], e, 0, 0)
            w2[0, lay, cols, :] = new2
            dl = (g2[lay, cols, :] - new2).astype(BF16)
            delta[p, 2 * j] = dl[:128]
            delta[p, 2 * j + 1] = dl[128:]
        send_piece(i, 0)
        if after_first is not None:
            pl.when(i == 0)(after_first)
        g_load(1, lay).wait()
        acc = dhid[...]
        for j in range(NB):
            cols = slice(j * D, (j + 1) * D)
            d_u = dot(e, w2b[lay, cols, :], 1, 1)
            c = (du[lay, :, cols] * d_u).astype(BF16)
            acc = acc + dot(c, w1b[lay, :, cols], 1, 1)
            new1 = w1[0, lay, :, cols] - INNER_LR * dot(h_bf, c, 0, 0)
            w1[0, lay, :, cols] = new1
            w1b[lay, :, cols] = new1.astype(BF16)
            dl = (g1[lay, :, cols] - new1).astype(BF16)
            delta[p + 1, 2 * j] = dl[:128]
            delta[p + 1, 2 * j + 1] = dl[128:]
        dhid[...] = acc
        send_piece(i, 1)
        w2b[lay] = w2[0, lay].astype(BF16)

    def back_full(lay, need_input_grad=True):
        e = dhid[...].astype(BF16)
        h_bf = hb[lay]
        acc = dhid[...]
        for j in range(NB):
            cols = slice(j * D, (j + 1) * D)
            d_u = dot(e, w2b[lay, cols, :], 1, 1)
            c = (du[lay, :, cols] * d_u).astype(BF16)
            update2(lay, cols, ub[lay, :, cols], e)
            if need_input_grad:
                acc = acc + dot(c, w1b[lay, :, cols], 1, 1)
            update1(lay, cols, h_bf, c)
        if need_input_grad:
            dhid[...] = acc

    def back_chain(lay):
        e = dhid[...].astype(BF16)
        eb[lay - 2] = e
        acc = dhid[...]
        for j in range(NB):
            cols = slice(j * D, (j + 1) * D)
            d_u = dot(e, w2b[lay, cols, :], 1, 1)
            c = (du[lay, :, cols] * d_u).astype(BF16)
            cb[lay - 2, :, cols] = c
            acc = acc + dot(c, w1b[lay, :, cols], 1, 1)
        dhid[...] = acc

    def back_weights(lay):
        e = eb[lay - 2]
        h_bf = hb[lay]
        for j in range(NB):
            cols = slice(j * D, (j + 1) * D)
            update2(lay, cols, ub[lay, :, cols], e)
            update1(lay, cols, h_bf, cb[lay - 2, :, cols])

    def reduce_stage1(p):
        for gi in range(3 * p, 3 * p + 3):
            _, c, u0, nu = GROUPS[gi]
            rows = pl.ds(pl.multiple_of(core * 64 + coord[dims_of(c)[0]] * 32, 32), 32)
            for cp in rs0_copies(gi):
                cp.wait_recv()
            for u in range(u0, u0 + nu):
                s1[p, u] = ((delta[p, u, rows, :].astype(F32) + raw[0, p, u].astype(F32))
                            + (raw[1, p, u].astype(F32) + raw[2, p, u].astype(F32)))
            stage_copy(RS1, gi).start()

    def reduce_stage2(p):
        for gi in range(3 * p, 3 * p + 3):
            _, c, u0, nu = GROUPS[gi]
            rows = pl.ds(pl.multiple_of(coord[dims_of(c)[1]] * 16, 16), 16)
            stage_copy(RS1, gi).wait_recv()
            for u in range(u0, u0 + nu):
                s2[p, u] = s1[p, u, rows, :] + r1[p, u]
            stage_copy(X2, gi).start()

    def reduce_stage3(p):
        for gi in range(3 * p, 3 * p + 3):
            _, c, u0, nu = GROUPS[gi]
            d0, d1, d2 = dims_of(c)
            rows = pl.ds(pl.multiple_of(core * 64 + coord[d0] * 32 + coord[d1] * 16, 16), 16)
            stage_copy(X2, gi).wait_recv()
            for u in range(u0, u0 + nu):
                full[p, u, rows, :] = s2[p, u] + r2[p, u]
            stage_copy(AG1, gi).start()

    def gather_stage2(p):
        for gi in range(3 * p, 3 * p + 3):
            stage_copy(AG1, gi).wait_recv()
            stage_copy(AG2, gi).start()
            stage_copy(DDA, gi).start()

    def gather_stage3(p):
        for gi in range(3 * p, 3 * p + 3):
            stage_copy(AG2, gi).wait_recv()
            stage_copy(DDB, gi).start()

    def outer_update(p, merge=True, outer=True):
        lay, mat = PIECES[p]
        wr, wbr, gr, mr = (w1, w1b, g1, m1) if mat == 1 else (w2, w2b, g2, m2)
        if merge:
            m_load(mat, lay).wait()
            wait_gathered(p)
        for u in range(8):
            rows, cols = unit_slice(mat, u)
            mean = full[p, u] * (1.0 / N_ALL)
            mom = OUTER_MOM * mr[lay, rows, cols] + mean
            glob = gr[lay, rows, cols] - OUTER_LR * (OUTER_MOM * mom + mean)
            if outer:
                mr[lay, rows, cols] = mom
                gr[lay, rows, cols] = glob
            if merge:
                merged = MERGE_MIX * wr[0, lay, rows, cols] + (1.0 - MERGE_MIX) * glob
                wr[0, lay, rows, cols] = merged
                wbr[lay, rows, cols] = merged.astype(BF16)

    last_piece = GATHER_ORDER[-1]

    def wait_gathered(p):
        for gi in range(3 * p, 3 * p + 3):
            stage_copy(DDA, gi).wait_recv()
            stage_copy(DDB, gi).wait_recv()

    def finish(frag):
        if frag == 0:
            outer_update(last_piece, outer=False)
        else:
            for p, (part, mat) in enumerate(PIECES):
                m_load(mat, 2 + part).wait()
                wait_gathered(p)
        for gi in range(12):
            for cp in rs0_copies(gi):
                cp.wait_send()
            for stage in range(6):
                stage_copy(stage, gi).wait_send()

    def sync(frag):
        for p in range(4):
            reduce_stage2(p)
        for p in range(4):
            reduce_stage3(p)
        for p in GATHER_ORDER:
            gather_stage2(p)
        prev = None
        for p in GATHER_ORDER:
            gather_stage3(p)
            if prev is not None and frag == 0:
                outer_update(prev)
            prev = p

    def layers(lo, body):
        def run(i, _):
            body(i, lo - i)
            return 0
        return run

    forward(0)
    pl.semaphore_wait(bar, 7)
    loss_grad(0)
    lax.fori_loop(0, 2, layers(3, lambda i, lay: back_chain(lay)), 0)

    lax.fori_loop(0, 2, layers(1, back_send), 0)
    lax.fori_loop(0, 2, layers(3, lambda i, lay: back_weights(lay)), 0)

    def back_hook(i, lay):
        back_full(lay)

        for p in range(1, 4):
            @pl.when(i == p - 1)
            def _(p=p):
                reduce_stage1(p)

    forward(1)
    loss_grad(1)
    reduce_stage1(0)
    lax.fori_loop(0, 3, layers(3, back_hook), 0)
    back_full(0, False)
    sync(0)

    forward(2, lambda: finish(0))
    loss_grad(2)

    lax.fori_loop(0, 2, layers(3, lambda i, lay: back_send(
        i, lay, lambda: outer_update(last_piece, merge=False))), 0)
    back_full(1)
    back_full(0, False)

    forward(3)
    loss_grad(3)
    reduce_stage1(0)
    lax.fori_loop(0, 3, layers(3, back_hook), 0)
    back_full(0, False)
    sync(1)
    finish(1)


def write_body(w1, w2, g1, g2, m1, m2, full, *refs):
    dsts, stages, sem = refs[:6], refs[6:12], refs[12]
    srcs = (w1, w2, g1, g2, m1, m2)
    cps = []

    def put(src, i, lay):
        dst = dsts[i].at[0, lay] if i < 2 else dsts[i].at[lay]
        cp = pltpu.make_async_copy(src, dst, sem.at[i, lay])
        cp.start()
        cps.append(cp)

    for lay in range(2):
        for i in range(6):
            put(srcs[i].at[0, lay] if i < 2 else srcs[i].at[lay], i, lay)
    for p, (part, mat) in enumerate(PIECES):
        lay = 2 + part
        k = mat - 1
        wr, gr, mr = srcs[k], srcs[2 + k], srcs[4 + k]
        ws, gs, ms = stages[k], stages[2 + k], stages[4 + k]
        for u in range(8):
            rows, cols = unit_slice(mat, u)
            mean = full[p, u] * (1.0 / N_ALL)
            mom = OUTER_MOM * mr[lay, rows, cols] + mean
            glob = gr[lay, rows, cols] - OUTER_LR * (OUTER_MOM * mom + mean)
            ms[part, rows, cols] = mom
            gs[part, rows, cols] = glob
            ws[part, rows, cols] = MERGE_MIX * wr[0, lay, rows, cols] + (1.0 - MERGE_MIX) * glob
        for idx, st in enumerate((ws, gs, ms)):
            put(st.at[part], 2 * idx + k, lay)
    for cp in cps:
        cp.wait()


def solution(mesh):
    def device_fn(w1_loc, w2_loc, w1_glb, w2_glb, mom1, mom2, x_loc, y_loc):
        arrays = (w1_loc, w2_loc, w1_glb, w2_glb, mom1, mom2)
        shapes = [jax.ShapeDtypeStruct(a.shape, F32) for a in arrays]
        dma = pltpu.SemaphoreType.DMA
        work = pl.pallas_call(
            main_body,
            out_shape=shapes + [jax.ShapeDtypeStruct((4, 8, 128, 256), F32)],
            in_specs=[HBM] * 8,
            out_specs=[VMEM] * 7,
            scratch_shapes=[
                pltpu.VMEM((H, B, D), BF16), pltpu.VMEM((H, B, D), BF16),
                pltpu.VMEM((L, D, FF), BF16), pltpu.VMEM((L, FF, D), BF16),
                pltpu.VMEM((L, B, D), BF16), pltpu.VMEM((L, B, FF), BF16), pltpu.VMEM((L, B, FF), F32),
                pltpu.VMEM((B, D), F32), pltpu.VMEM((B, D), F32),
                pltpu.VMEM((2, B, D), BF16), pltpu.VMEM((2, B, FF), BF16),
                pltpu.VMEM((4, 8, 128, 256), BF16), pltpu.VMEM((3, 4, 8, 32, 256), BF16),
                pltpu.VMEM((4, 8, 32, 256), F32), pltpu.VMEM((4, 8, 16, 256), F32),
                pltpu.VMEM((4, 8, 16, 256), F32), pltpu.VMEM((4, 8, 16, 256), F32),
                dma((26,)), dma((12, 3)), dma((12, 3)), dma((6, 12)), dma((6, 12)),
            ],
            compiler_params=pltpu.CompilerParams(
                collective_id=0, has_side_effects=True, vmem_limit_bytes=22 * 2**20),
            name='diloco_round',
        )(*[pltpu.with_memory_space_constraint(a, pltpu.HBM) for a in (*arrays, x_loc, y_loc)])
        outs = pl.pallas_call(
            write_body,
            out_shape=shapes,
            in_specs=[VMEM] * 7,
            out_specs=[HBM] * 6,
            scratch_shapes=[pltpu.VMEM((2, D, FF), F32), pltpu.VMEM((2, FF, D), F32)] * 3 + [dma((6, L))],
            compiler_params=pltpu.CompilerParams(vmem_limit_bytes=16 * 2**20),
            name='write_out',
        )(*work)
        return tuple(outs)

    local_spec = P(('shard', 'worker'))
    whole_spec = P()
    return jax.shard_map(device_fn, mesh=mesh, in_specs=(local_spec, local_spec, whole_spec, whole_spec, whole_spec, whole_spec, local_spec, local_spec), out_specs=(local_spec, local_spec, whole_spec, whole_spec, whole_spec, whole_spec), check_vma=False)
```

```python
import jax
import jax.numpy as jnp
from jax import lax
from jax.experimental import pallas as pl
from jax.experimental.pallas import tpu as pltpu
from jax.sharding import PartitionSpec as P

OUTER_LR = 0.7
OUTER_MOM = 0.9
MERGE_MIX = 0.5

L = 4
H = 4
D = 256
FF = 1024
B = 128
NB = FF // D
INNER_LR = 2.0 * D / (FF * L)
N_ALL = 16
F32 = jnp.float32
BF16 = jnp.bfloat16
MESH = pl.DeviceIdType.MESH
HBM = pl.BlockSpec(memory_space=pltpu.HBM)
VMEM = pl.BlockSpec(memory_space=pltpu.VMEM)

PIECES = ((1, 2), (1, 1), (0, 2), (0, 1))
COLOR_UNITS = ((3, 3, 2), (3, 2, 3), (2, 3, 3), (3, 3, 2))
GROUPS = []
for piece_idx in range(4):
    first_unit = 0
    for color in range(3):
        GROUPS.append((piece_idx, color, first_unit, COLOR_UNITS[piece_idx][color]))
        first_unit += COLOR_UNITS[piece_idx][color]
GATHER_ORDER = (0, 2, 3, 1)
RS1, X2, AG1, AG2, DDA, DDB = range(6)


def dot(a, b, ca, cb):
    return lax.dot_general(a, b, (((ca,), (cb,)), ((), ())), preferred_element_type=F32)


def gelu_pair(a):
    k0 = 0.7978845608028654
    k1 = k0 * 0.044715
    a2 = a * a
    t = jnp.tanh(a * (k0 + k1 * a2))
    h = 0.5 + 0.5 * t
    u = a * h
    du = h + (u * (1.0 - h)) * (2.0 * k0 + (6.0 * k1) * a2)
    return u, du


def unit_slice(mat, u):
    if mat == 2:
        return pl.ds(u * 128, 128), pl.ds(0, 256)
    return pl.ds((u % 2) * 128, 128), pl.ds((u // 2) * 256, 256)


def main_body(w1_in, w2_in, g1_in, g2_in, m1_in, m2_in, x_in, y_in,
              w1, w2, g1, g2, m1, m2, full,
              xb, yb, w1b, w2b, hb, ub, du, hid, dhid, eb, cb,
              delta, raw, s1, r1, s2, r2,
              ld_sem, s0_send, s0_recv, st_send, st_recv):
    zc = lax.axis_index('shard')
    wk = lax.axis_index('worker')
    core = lax.rem(wk, 2)
    xc = lax.rem(wk // 2, 2)
    yc = wk // 4
    coord = (xc, yc, zc)

    def chip_peer(dim, same_core=True):
        w = wk
        s = zc
        if dim == 0:
            w = wk + 2 - 4 * xc
        elif dim == 1:
            w = wk + 4 - 8 * yc
        elif dim == 2:
            s = 1 - zc
        if not same_core:
            w = w + 1 - 2 * core
        return (s, w)

    partner = chip_peer(3, False)

    bar = pltpu.get_barrier_semaphore()
    pl.semaphore_signal(bar, inc=1, device_id=partner, device_id_type=MESH)
    for dim in range(3):
        for same in (True, False):
            pl.semaphore_signal(bar, inc=1, device_id=chip_peer(dim, same), device_id_type=MESH)

    def w_load(lay):
        return (pltpu.make_async_copy(w1_in.at[0, lay], w1.at[0, lay], ld_sem.at[lay]),
                pltpu.make_async_copy(w2_in.at[0, lay], w2.at[0, lay], ld_sem.at[L + lay]))

    def w_start(lay):
        for i in range(4):
            for src, dst, n, idx in ((w1_in, w1, D // 4, lay), (w2_in, w2, FF // 4, L + lay)):
                rows = pl.ds(i * n, n)
                pltpu.make_async_copy(src.at[0, lay, rows], dst.at[0, lay, rows], ld_sem.at[idx]).start()

    def g_load(mat, lay):
        if mat == 1:
            return pltpu.make_async_copy(g1_in.at[lay], g1.at[lay], ld_sem.at[2 * L + lay])
        return pltpu.make_async_copy(g2_in.at[lay], g2.at[lay], ld_sem.at[3 * L + lay])

    def m_load(mat, lay):
        if mat == 1:
            return pltpu.make_async_copy(m1_in.at[lay], m1.at[lay], ld_sem.at[4 * L + lay])
        return pltpu.make_async_copy(m2_in.at[lay], m2.at[lay], ld_sem.at[5 * L + lay])

    x_load = pltpu.make_async_copy(x_in.at[0], xb, ld_sem.at[6 * L])
    y_load = pltpu.make_async_copy(y_in.at[0], yb, ld_sem.at[6 * L + 1])
    x_load.start()
    w_start(0)
    y_load.start()
    for lay in range(1, L):
        w_start(lay)
    for lay in range(L):
        for mat in (1, 2):
            g_load(mat, lay).start()
    for lay in range(L):
        for mat in (1, 2):
            m_load(mat, lay).start()
    x_load.wait()
    y_load.wait()

    def dims_of(color_idx):
        return color_idx % 3, (color_idx + 1) % 3, (color_idx + 2) % 3

    def rs0_copies(gi):
        p, c, u0, nu = GROUPS[gi]
        d0 = dims_of(c)[0]
        k0 = coord[d0]
        us = pl.ds(u0, nu)
        other = 1 - core

        def rows(tc, blk):
            return pl.ds(pl.multiple_of(tc * 64 + blk * 32, 32), 32)

        out = []
        for idx, (tc, blk, dev) in enumerate(((other, k0, partner),
                                               (core, 1 - k0, chip_peer(d0, True)),
                                               (other, 1 - k0, chip_peer(d0, False)))):
            out.append(pltpu.make_async_remote_copy(
                src_ref=delta.at[p, us, rows(tc, blk)], dst_ref=raw.at[idx, p, us],
                send_sem=s0_send.at[gi, idx], recv_sem=s0_recv.at[gi, idx],
                device_id=dev, device_id_type=MESH))
        return out

    def stage_copy(stage, gi):
        p, c, u0, nu = GROUPS[gi]
        d0, d1, d2 = dims_of(c)
        k0, k1, k2 = coord[d0], coord[d1], coord[d2]
        us = pl.ds(u0, nu)
        if stage == RS1:
            src, dst, dev = s1.at[p, us, pl.ds(pl.multiple_of((1 - k1) * 16, 16), 16)], r1.at[p, us], chip_peer(d1)
        elif stage == X2:
            src, dst, dev = s2.at[p, us], r2.at[p, us], chip_peer(d2)
        else:
            base = core * 64
            if stage == AG1:
                off, n, dev = base + k0 * 32 + k1 * 16, 16, chip_peer(d1)
            elif stage == AG2:
                off, n, dev = base + k0 * 32, 32, chip_peer(d0)
            elif stage == DDA:
                off, n, dev = base + k0 * 32, 32, partner
            else:
                off, n, dev = base + (1 - k0) * 32, 32, partner
            src = full.at[p, us, pl.ds(pl.multiple_of(off, 16), n)]
            dst = src
        return pltpu.make_async_remote_copy(
            src_ref=src, dst_ref=dst, send_sem=st_send.at[stage, gi], recv_sem=st_recv.at[stage, gi],
            device_id=dev, device_id_type=MESH)

    def forward(k, before_layer_1=None):
        hid[...] = xb[k].astype(F32)

        def layer(lay, _):
            if k == 0:
                for cp in w_load(lay):
                    cp.wait()
            if before_layer_1 is not None and lay == 1:
                before_layer_1()
            h_bf = hid[...].astype(BF16)
            hb[lay] = h_bf
            acc = hid[...]
            for j in range(NB):
                cols = slice(j * D, (j + 1) * D)
                if k == 0:
                    w1b[lay, :, cols] = w1[0, lay, :, cols].astype(BF16)
                    w2b[lay, cols, :] = w2[0, lay, cols, :].astype(BF16)
                a = dot(h_bf, w1b[lay, :, cols], 1, 0)
                u, dg = gelu_pair(a)
                u_bf = u.astype(BF16)
                ub[lay, :, cols] = u_bf
                du[lay, :, cols] = dg
                acc = acc + dot(u_bf, w2b[lay, cols, :], 1, 0)
            hid[...] = acc
            return 0

        for lay in range(L):
            layer(lay, 0)

    def loss_grad(k):
        dhid[...] = (2.0 / (B * D)) * (hid[...] - yb[k].astype(F32))

    def update2(lay, cols, u_j, e):
        new2 = w2[0, lay, cols, :] - INNER_LR * dot(u_j, e, 0, 0)
        w2[0, lay, cols, :] = new2
        w2b[lay, cols, :] = new2.astype(BF16)

    def update1(lay, cols, h_bf, c):
        new1 = w1[0, lay, :, cols] - INNER_LR * dot(h_bf, c, 0, 0)
        w1[0, lay, :, cols] = new1
        w1b[lay, :, cols] = new1.astype(BF16)

    def send_piece(i, which):
        for p in (which, 2 + which):
            @pl.when(i == p // 2)
            def _(p=p):
                for gi in range(3 * p, 3 * p + 3):
                    for cp in rs0_copies(gi):
                        cp.start()

    def back_send(i, lay, after_first=None):
        p = 2 * i
        e = dhid[...].astype(BF16)
        h_bf = hb[lay]
        g_load(2, lay).wait()
        for j in range(NB):
            cols = slice(j * D, (j + 1) * D)
            new2 = w2[0, lay, cols, :] - INNER_LR * dot(ub[lay, :, cols], e, 0, 0)
            w2[0, lay, cols, :] = new2
            dl = (g2[lay, cols, :] - new2).astype(BF16)
            delta[p, 2 * j] = dl[:128]
            delta[p, 2 * j + 1] = dl[128:]
        send_piece(i, 0)
        if after_first is not None:
            pl.when(i == 0)(after_first)
        g_load(1, lay).wait()
        acc = dhid[...]
        for j in range(NB):
            cols = slice(j * D, (j + 1) * D)
            d_u = dot(e, w2b[lay, cols, :], 1, 1)
            c = (du[lay, :, cols] * d_u).astype(BF16)
            acc = acc + dot(c, w1b[lay, :, cols], 1, 1)
            new1 = w1[0, lay, :, cols] - INNER_LR * dot(h_bf, c, 0, 0)
            w1[0, lay, :, cols] = new1
            w1b[lay, :, cols] = new1.astype(BF16)
            dl = (g1[lay, :, cols] - new1).astype(BF16)
            delta[p + 1, 2 * j] = dl[:128]
            delta[p + 1, 2 * j + 1] = dl[128:]
        dhid[...] = acc
        send_piece(i, 1)
        w2b[lay] = w2[0, lay].astype(BF16)

    def back_full(lay, need_input_grad=True):
        e = dhid[...].astype(BF16)
        h_bf = hb[lay]
        acc = dhid[...]
        for j in range(NB):
            cols = slice(j * D, (j + 1) * D)
            d_u = dot(e, w2b[lay, cols, :], 1, 1)
            c = (du[lay, :, cols] * d_u).astype(BF16)
            update2(lay, cols, ub[lay, :, cols], e)
            if need_input_grad:
                acc = acc + dot(c, w1b[lay, :, cols], 1, 1)
            update1(lay, cols, h_bf, c)
        if need_input_grad:
            dhid[...] = acc

    def back_chain(lay):
        e = dhid[...].astype(BF16)
        eb[lay - 2] = e
        acc = dhid[...]
        for j in range(NB):
            cols = slice(j * D, (j + 1) * D)
            d_u = dot(e, w2b[lay, cols, :], 1, 1)
            c = (du[lay, :, cols] * d_u).astype(BF16)
            cb[lay - 2, :, cols] = c
            acc = acc + dot(c, w1b[lay, :, cols], 1, 1)
        dhid[...] = acc

    def back_weights(lay):
        e = eb[lay - 2]
        h_bf = hb[lay]
        for j in range(NB):
            cols = slice(j * D, (j + 1) * D)
            update2(lay, cols, ub[lay, :, cols], e)
            update1(lay, cols, h_bf, cb[lay - 2, :, cols])

    def reduce_stage1(p):
        for gi in range(3 * p, 3 * p + 3):
            _, c, u0, nu = GROUPS[gi]
            rows = pl.ds(pl.multiple_of(core * 64 + coord[dims_of(c)[0]] * 32, 32), 32)
            for cp in rs0_copies(gi):
                cp.wait_recv()
            for u in range(u0, u0 + nu):
                s1[p, u] = ((delta[p, u, rows, :].astype(F32) + raw[0, p, u].astype(F32))
                            + (raw[1, p, u].astype(F32) + raw[2, p, u].astype(F32)))
            stage_copy(RS1, gi).start()

    def reduce_stage2(p):
        for gi in range(3 * p, 3 * p + 3):
            _, c, u0, nu = GROUPS[gi]
            rows = pl.ds(pl.multiple_of(coord[dims_of(c)[1]] * 16, 16), 16)
            stage_copy(RS1, gi).wait_recv()
            for u in range(u0, u0 + nu):
                s2[p, u] = s1[p, u, rows, :] + r1[p, u]
            stage_copy(X2, gi).start()

    def reduce_stage3(p):
        for gi in range(3 * p, 3 * p + 3):
            _, c, u0, nu = GROUPS[gi]
            d0, d1, d2 = dims_of(c)
            rows = pl.ds(pl.multiple_of(core * 64 + coord[d0] * 32 + coord[d1] * 16, 16), 16)
            stage_copy(X2, gi).wait_recv()
            for u in range(u0, u0 + nu):
                full[p, u, rows, :] = s2[p, u] + r2[p, u]
            stage_copy(AG1, gi).start()

    def gather_stage2(p):
        for gi in range(3 * p, 3 * p + 3):
            stage_copy(AG1, gi).wait_recv()
            stage_copy(AG2, gi).start()
            stage_copy(DDA, gi).start()

    def gather_stage3(p):
        for gi in range(3 * p, 3 * p + 3):
            stage_copy(AG2, gi).wait_recv()
            stage_copy(DDB, gi).start()

    def outer_update(p, merge=True, outer=True):
        lay, mat = PIECES[p]
        wr, wbr, gr, mr = (w1, w1b, g1, m1) if mat == 1 else (w2, w2b, g2, m2)
        if merge:
            m_load(mat, lay).wait()
            wait_gathered(p)
        for u in range(8):
            rows, cols = unit_slice(mat, u)
            mean = full[p, u] * (1.0 / N_ALL)
            mom = OUTER_MOM * mr[lay, rows, cols] + mean
            glob = gr[lay, rows, cols] - OUTER_LR * (OUTER_MOM * mom + mean)
            if outer:
                mr[lay, rows, cols] = mom
                gr[lay, rows, cols] = glob
            if merge:
                merged = MERGE_MIX * wr[0, lay, rows, cols] + (1.0 - MERGE_MIX) * glob
                wr[0, lay, rows, cols] = merged
                wbr[lay, rows, cols] = merged.astype(BF16)

    last_piece = GATHER_ORDER[-1]

    def wait_gathered(p):
        for gi in range(3 * p, 3 * p + 3):
            stage_copy(DDA, gi).wait_recv()
            stage_copy(DDB, gi).wait_recv()

    def finish(frag):
        if frag == 0:
            outer_update(last_piece, outer=False)
        else:
            for p, (part, mat) in enumerate(PIECES):
                m_load(mat, 2 + part).wait()
                wait_gathered(p)
        for gi in range(12):
            for cp in rs0_copies(gi):
                cp.wait_send()
            for stage in range(6):
                stage_copy(stage, gi).wait_send()

    def sync(frag):
        for p in range(4):
            reduce_stage2(p)
        for p in range(4):
            reduce_stage3(p)
        for p in GATHER_ORDER:
            gather_stage2(p)
        prev = None
        for p in GATHER_ORDER:
            gather_stage3(p)
            if prev is not None and frag == 0:
                outer_update(prev)
            prev = p

    def layers(lo, body):
        def run(i, _):
            body(i, lo - i)
            return 0
        return run

    forward(0)
    pl.semaphore_wait(bar, 7)
    loss_grad(0)
    back_chain(3)
    back_chain(2)

    lax.fori_loop(0, 2, layers(1, back_send), 0)
    lax.fori_loop(0, 2, layers(3, lambda i, lay: back_weights(lay)), 0)

    def back_hook(i, lay):
        back_full(lay)

        for p in range(1, 4):
            @pl.when(i == p - 1)
            def _(p=p):
                reduce_stage1(p)

    forward(1)
    loss_grad(1)
    reduce_stage1(0)
    lax.fori_loop(0, 3, layers(3, back_hook), 0)
    back_full(0, False)
    sync(0)

    forward(2, lambda: finish(0))
    loss_grad(2)

    lax.fori_loop(0, 2, layers(3, lambda i, lay: back_send(
        i, lay, lambda: outer_update(last_piece, merge=False))), 0)
    back_full(1)
    back_full(0, False)

    forward(3)
    loss_grad(3)
    reduce_stage1(0)
    lax.fori_loop(0, 3, layers(3, back_hook), 0)
    back_full(0, False)
    sync(1)
    finish(1)


def write_body(w1, w2, g1, g2, m1, m2, full, *refs):
    dsts, stages, sem = refs[:6], refs[6:12], refs[12]
    srcs = (w1, w2, g1, g2, m1, m2)
    cps = []

    def put(src, i, lay):
        dst = dsts[i].at[0, lay] if i < 2 else dsts[i].at[lay]
        half = src.shape[0] // 2
        for rows in (pl.ds(0, half), pl.ds(half, half)):
            pltpu.make_async_copy(src.at[rows], dst.at[rows], sem.at[i, lay]).start()
        cps.append(pltpu.make_async_copy(src, dst, sem.at[i, lay]))

    for lay in range(2):
        for i in range(6):
            put(srcs[i].at[0, lay] if i < 2 else srcs[i].at[lay], i, lay)
    for p, (part, mat) in enumerate(PIECES):
        lay = 2 + part
        k = mat - 1
        wr, gr, mr = srcs[k], srcs[2 + k], srcs[4 + k]
        ws, gs, ms = stages[k], stages[2 + k], stages[4 + k]
        for u in range(8):
            rows, cols = unit_slice(mat, u)
            mean = full[p, u] * (1.0 / N_ALL)
            mom = OUTER_MOM * mr[lay, rows, cols] + mean
            glob = gr[lay, rows, cols] - OUTER_LR * (OUTER_MOM * mom + mean)
            ms[part, rows, cols] = mom
            gs[part, rows, cols] = glob
            ws[part, rows, cols] = MERGE_MIX * wr[0, lay, rows, cols] + (1.0 - MERGE_MIX) * glob
        for idx, st in enumerate((ws, gs, ms)):
            put(st.at[part], 2 * idx + k, lay)
    for cp in cps:
        cp.wait()


def solution(mesh):
    def device_fn(w1_loc, w2_loc, w1_glb, w2_glb, mom1, mom2, x_loc, y_loc):
        arrays = (w1_loc, w2_loc, w1_glb, w2_glb, mom1, mom2)
        shapes = [jax.ShapeDtypeStruct(a.shape, F32) for a in arrays]
        dma = pltpu.SemaphoreType.DMA
        work = pl.pallas_call(
            main_body,
            out_shape=shapes + [jax.ShapeDtypeStruct((4, 8, 128, 256), F32)],
            in_specs=[HBM] * 8,
            out_specs=[VMEM] * 7,
            scratch_shapes=[
                pltpu.VMEM((H, B, D), BF16), pltpu.VMEM((H, B, D), BF16),
                pltpu.VMEM((L, D, FF), BF16), pltpu.VMEM((L, FF, D), BF16),
                pltpu.VMEM((L, B, D), BF16), pltpu.VMEM((L, B, FF), BF16), pltpu.VMEM((L, B, FF), F32),
                pltpu.VMEM((B, D), F32), pltpu.VMEM((B, D), F32),
                pltpu.VMEM((2, B, D), BF16), pltpu.VMEM((2, B, FF), BF16),
                pltpu.VMEM((4, 8, 128, 256), BF16), pltpu.VMEM((3, 4, 8, 32, 256), BF16),
                pltpu.VMEM((4, 8, 32, 256), F32), pltpu.VMEM((4, 8, 16, 256), F32),
                pltpu.VMEM((4, 8, 16, 256), F32), pltpu.VMEM((4, 8, 16, 256), F32),
                dma((26,)), dma((12, 3)), dma((12, 3)), dma((6, 12)), dma((6, 12)),
            ],
            compiler_params=pltpu.CompilerParams(
                collective_id=0, has_side_effects=True, vmem_limit_bytes=22 * 2**20),
            name='diloco_round',
        )(*[pltpu.with_memory_space_constraint(a, pltpu.HBM) for a in (*arrays, x_loc, y_loc)])
        outs = pl.pallas_call(
            write_body,
            out_shape=shapes,
            in_specs=[VMEM] * 7,
            out_specs=[HBM] * 6,
            scratch_shapes=[pltpu.VMEM((2, D, FF), F32), pltpu.VMEM((2, FF, D), F32)] * 3 + [dma((6, L))],
            compiler_params=pltpu.CompilerParams(vmem_limit_bytes=16 * 2**20),
            name='write_out',
        )(*work)
        return tuple(outs)

    local_spec = P(('shard', 'worker'))
    whole_spec = P()
    return jax.shard_map(device_fn, mesh=mesh, in_specs=(local_spec, local_spec, whole_spec, whole_spec, whole_spec, whole_spec, local_spec, local_spec), out_specs=(local_spec, local_spec, whole_spec, whole_spec, whole_spec, whole_spec), check_vma=False)
```

```python
import jax
import jax.numpy as jnp
from jax import lax
from jax.experimental import pallas as pl
from jax.experimental.pallas import tpu as pltpu
from jax.sharding import PartitionSpec as P

OUTER_LR = 0.7
OUTER_MOM = 0.9
MERGE_MIX = 0.5

L = 4
H = 4
D = 256
FF = 1024
B = 128
NB = FF // D
INNER_LR = 2.0 * D / (FF * L)
N_ALL = 16
F32 = jnp.float32
BF16 = jnp.bfloat16
MESH = pl.DeviceIdType.MESH
HBM = pl.BlockSpec(memory_space=pltpu.HBM)
VMEM = pl.BlockSpec(memory_space=pltpu.VMEM)

PIECES = ((1, 2), (1, 1), (0, 2), (0, 1))
COLOR_UNITS = ((3, 3, 2), (3, 2, 3), (2, 3, 3), (3, 3, 2))
GROUPS = []
for piece_idx in range(4):
    first_unit = 0
    for color in range(3):
        GROUPS.append((piece_idx, color, first_unit, COLOR_UNITS[piece_idx][color]))
        first_unit += COLOR_UNITS[piece_idx][color]
GATHER_ORDER = (0, 2, 3, 1)
LAST = GATHER_ORDER[-1]
RS1, X2, AG1, AG2, DDA, DDB, XOWN, XPART = range(8)


def dot(a, b, ca, cb):
    return lax.dot_general(a, b, (((ca,), (cb,)), ((), ())), preferred_element_type=F32)


def gelu_pair(a):
    k0 = 0.7978845608028654
    k1 = k0 * 0.044715
    a2 = a * a
    t = jnp.tanh(a * (k0 + k1 * a2))
    h = 0.5 + 0.5 * t
    u = a * h
    du = h + (u * (1.0 - h)) * (2.0 * k0 + (6.0 * k1) * a2)
    return u, du


def unit_slice(mat, u):
    if mat == 2:
        return pl.ds(u * 128, 128), pl.ds(0, 256)
    return pl.ds((u % 2) * 128, 128), pl.ds((u // 2) * 256, 256)


def main_body(w1_in, w2_in, g1_in, g2_in, m1_in, m2_in, x_in, y_in,
              w1, w2, g1, g2, m1, m2, full,
              xb, yb, w1b, w2b, hb, ub, du, hid, dhid, eb, cb,
              delta, raw, s1, r1, s2, r2,
              ld_sem, s0_send, s0_recv, st_send, st_recv):
    zc = lax.axis_index('shard')
    wk = lax.axis_index('worker')
    core = lax.rem(wk, 2)
    xc = lax.rem(wk // 2, 2)
    yc = wk // 4
    coord = (xc, yc, zc)

    def chip_peer(dim, same_core=True):
        w = wk
        s = zc
        if dim == 0:
            w = wk + 2 - 4 * xc
        elif dim == 1:
            w = wk + 4 - 8 * yc
        elif dim == 2:
            s = 1 - zc
        if not same_core:
            w = w + 1 - 2 * core
        return (s, w)

    partner = chip_peer(3, False)

    bar = pltpu.get_barrier_semaphore()
    pl.semaphore_signal(bar, inc=1, device_id=partner, device_id_type=MESH)
    for dim in range(3):
        for same in (True, False):
            pl.semaphore_signal(bar, inc=1, device_id=chip_peer(dim, same), device_id_type=MESH)

    def w_load(lay):
        return (pltpu.make_async_copy(w1_in.at[0, lay], w1.at[0, lay], ld_sem.at[lay]),
                pltpu.make_async_copy(w2_in.at[0, lay], w2.at[0, lay], ld_sem.at[L + lay]))

    def w_start(lay):
        for i in range(4):
            for src, dst, n, idx in ((w1_in, w1, D // 4, lay), (w2_in, w2, FF // 4, L + lay)):
                rows = pl.ds(i * n, n)
                pltpu.make_async_copy(src.at[0, lay, rows], dst.at[0, lay, rows], ld_sem.at[idx]).start()

    def g_load(mat, lay):
        if mat == 1:
            return pltpu.make_async_copy(g1_in.at[lay], g1.at[lay], ld_sem.at[2 * L + lay])
        return pltpu.make_async_copy(g2_in.at[lay], g2.at[lay], ld_sem.at[3 * L + lay])

    def m_load(mat, lay):
        if mat == 1:
            return pltpu.make_async_copy(m1_in.at[lay], m1.at[lay], ld_sem.at[4 * L + lay])
        return pltpu.make_async_copy(m2_in.at[lay], m2.at[lay], ld_sem.at[5 * L + lay])

    x_load = pltpu.make_async_copy(x_in.at[0], xb, ld_sem.at[6 * L])
    y_load = pltpu.make_async_copy(y_in.at[0], yb, ld_sem.at[6 * L + 1])
    x_load.start()
    w_start(0)
    y_load.start()
    for lay in range(1, L):
        w_start(lay)
    for lay in range(L):
        for mat in (1, 2):
            g_load(mat, lay).start()
    for lay in range(L):
        for mat in (1, 2):
            m_load(mat, lay).start()
    x_load.wait()
    y_load.wait()

    def dims_of(color_idx):
        return color_idx % 3, (color_idx + 1) % 3, (color_idx + 2) % 3

    def rs0_copies(gi):
        p, c, u0, nu = GROUPS[gi]
        d0 = dims_of(c)[0]
        k0 = coord[d0]
        us = pl.ds(u0, nu)
        other = 1 - core

        def rows(tc, blk):
            return pl.ds(pl.multiple_of(tc * 64 + blk * 32, 32), 32)

        out = []
        for idx, (tc, blk, dev) in enumerate(((other, k0, partner),
                                               (core, 1 - k0, chip_peer(d0, True)),
                                               (other, 1 - k0, chip_peer(d0, False)))):
            out.append(pltpu.make_async_remote_copy(
                src_ref=delta.at[p, us, rows(tc, blk)], dst_ref=raw.at[idx, p, us],
                send_sem=s0_send.at[gi, idx], recv_sem=s0_recv.at[gi, idx],
                device_id=dev, device_id_type=MESH))
        return out

    def stage_copy(stage, gi):
        p, c, u0, nu = GROUPS[gi]
        d0, d1, d2 = dims_of(c)
        k0, k1, k2 = coord[d0], coord[d1], coord[d2]
        us = pl.ds(u0, nu)
        if p == LAST and stage in (AG2, DDB):
            us = pl.ds(u0, nu - 1)
        elif stage in (XOWN, XPART):
            us = pl.ds(u0 + nu - 1, 1)
        if stage == RS1:
            src, dst, dev = s1.at[p, us, pl.ds(pl.multiple_of((1 - k1) * 16, 16), 16)], r1.at[p, us], chip_peer(d1)
        elif stage == X2:
            src, dst, dev = s2.at[p, us], r2.at[p, us], chip_peer(d2)
        else:
            base = core * 64
            if stage == AG1:
                off, n, dev = base + k0 * 32 + k1 * 16, 16, chip_peer(d1)
            elif stage in (AG2, XOWN):
                off, n, dev = base + k0 * 32, 32, chip_peer(d0)
            elif stage == XPART:
                off, n, dev = (1 - core) * 64 + k0 * 32, 32, chip_peer(d0)
            elif stage == DDA:
                off, n, dev = base + k0 * 32, 32, partner
            else:
                off, n, dev = base + (1 - k0) * 32, 32, partner
            src = full.at[p, us, pl.ds(pl.multiple_of(off, 16), n)]
            dst = src
        return pltpu.make_async_remote_copy(
            src_ref=src, dst_ref=dst, send_sem=st_send.at[stage, gi], recv_sem=st_recv.at[stage, gi],
            device_id=dev, device_id_type=MESH)

    def forward(k, before_layer_1=None):
        hid[...] = xb[k].astype(F32)

        def layer(lay, _):
            if k == 0:
                for cp in w_load(lay):
                    cp.wait()
            if before_layer_1 is not None and lay == 1:
                before_layer_1()
            h_bf = hid[...].astype(BF16)
            hb[lay] = h_bf
            acc = hid[...]
            for j in range(NB):
                cols = slice(j * D, (j + 1) * D)
                if k == 0:
                    w1b[lay, :, cols] = w1[0, lay, :, cols].astype(BF16)
                    w2b[lay, cols, :] = w2[0, lay, cols, :].astype(BF16)
                a = dot(h_bf, w1b[lay, :, cols], 1, 0)
                u, dg = gelu_pair(a)
                u_bf = u.astype(BF16)
                ub[lay, :, cols] = u_bf
                du[lay, :, cols] = dg
                acc = acc + dot(u_bf, w2b[lay, cols, :], 1, 0)
            hid[...] = acc
            return 0

        for lay in range(L):
            layer(lay, 0)

    def loss_grad(k):
        dhid[...] = (2.0 / (B * D)) * (hid[...] - yb[k].astype(F32))

    def update2(lay, cols, u_j, e):
        new2 = w2[0, lay, cols, :] - INNER_LR * dot(u_j, e, 0, 0)
        w2[0, lay, cols, :] = new2
        w2b[lay, cols, :] = new2.astype(BF16)

    def update1(lay, cols, h_bf, c):
        new1 = w1[0, lay, :, cols] - INNER_LR * dot(h_bf, c, 0, 0)
        w1[0, lay, :, cols] = new1
        w1b[lay, :, cols] = new1.astype(BF16)

    def send_piece(i, which):
        for p in (which, 2 + which):
            @pl.when(i == p // 2)
            def _(p=p):
                for gi in range(3 * p, 3 * p + 3):
                    for cp in rs0_copies(gi):
                        cp.start()

    def back_send(i, lay, after_first=None):
        p = 2 * i
        e = dhid[...].astype(BF16)
        h_bf = hb[lay]
        g_load(2, lay).wait()
        for j in range(NB):
            cols = slice(j * D, (j + 1) * D)
            new2 = w2[0, lay, cols, :] - INNER_LR * dot(ub[lay, :, cols], e, 0, 0)
            w2[0, lay, cols, :] = new2
            dl = (g2[lay, cols, :] - new2).astype(BF16)
            delta[p, 2 * j] = dl[:128]
            delta[p, 2 * j + 1] = dl[128:]
        send_piece(i, 0)
        if after_first is not None:
            pl.when(i == 0)(after_first)
        g_load(1, lay).wait()
        acc = dhid[...]
        for j in range(NB):
            cols = slice(j * D, (j + 1) * D)
            d_u = dot(e, w2b[lay, cols, :], 1, 1)
            c = (du[lay, :, cols] * d_u).astype(BF16)
            acc = acc + dot(c, w1b[lay, :, cols], 1, 1)
            new1 = w1[0, lay, :, cols] - INNER_LR * dot(h_bf, c, 0, 0)
            w1[0, lay, :, cols] = new1
            w1b[lay, :, cols] = new1.astype(BF16)
            dl = (g1[lay, :, cols] - new1).astype(BF16)
            delta[p + 1, 2 * j] = dl[:128]
            delta[p + 1, 2 * j + 1] = dl[128:]
        dhid[...] = acc
        send_piece(i, 1)
        w2b[lay] = w2[0, lay].astype(BF16)

    def back_full(lay, need_input_grad=True):
        e = dhid[...].astype(BF16)
        h_bf = hb[lay]
        acc = dhid[...]
        for j in range(NB):
            cols = slice(j * D, (j + 1) * D)
            d_u = dot(e, w2b[lay, cols, :], 1, 1)
            c = (du[lay, :, cols] * d_u).astype(BF16)
            update2(lay, cols, ub[lay, :, cols], e)
            if need_input_grad:
                acc = acc + dot(c, w1b[lay, :, cols], 1, 1)
            update1(lay, cols, h_bf, c)
        if need_input_grad:
            dhid[...] = acc

    def back_chain(lay):
        e = dhid[...].astype(BF16)
        eb[lay - 2] = e
        acc = dhid[...]
        for j in range(NB):
            cols = slice(j * D, (j + 1) * D)
            d_u = dot(e, w2b[lay, cols, :], 1, 1)
            c = (du[lay, :, cols] * d_u).astype(BF16)
            cb[lay - 2, :, cols] = c
            acc = acc + dot(c, w1b[lay, :, cols], 1, 1)
        dhid[...] = acc

    def back_weights(lay):
        e = eb[lay - 2]
        h_bf = hb[lay]
        for j in range(NB):
            cols = slice(j * D, (j + 1) * D)
            update2(lay, cols, ub[lay, :, cols], e)
            update1(lay, cols, h_bf, cb[lay - 2, :, cols])

    def reduce_stage1(p):
        for gi in range(3 * p, 3 * p + 3):
            _, c, u0, nu = GROUPS[gi]
            rows = pl.ds(pl.multiple_of(core * 64 + coord[dims_of(c)[0]] * 32, 32), 32)
            for cp in rs0_copies(gi):
                cp.wait_recv()
            for u in range(u0, u0 + nu):
                s1[p, u] = ((delta[p, u, rows, :].astype(F32) + raw[0, p, u].astype(F32))
                            + (raw[1, p, u].astype(F32) + raw[2, p, u].astype(F32)))
            stage_copy(RS1, gi).start()

    def reduce_stage2(p):
        for gi in range(3 * p, 3 * p + 3):
            _, c, u0, nu = GROUPS[gi]
            rows = pl.ds(pl.multiple_of(coord[dims_of(c)[1]] * 16, 16), 16)
            stage_copy(RS1, gi).wait_recv()
            for u in range(u0, u0 + nu):
                s2[p, u] = s1[p, u, rows, :] + r1[p, u]
            stage_copy(X2, gi).start()

    def reduce_stage3(p):
        for gi in range(3 * p, 3 * p + 3):
            _, c, u0, nu = GROUPS[gi]
            d0, d1, d2 = dims_of(c)
            rows = pl.ds(pl.multiple_of(core * 64 + coord[d0] * 32 + coord[d1] * 16, 16), 16)
            stage_copy(X2, gi).wait_recv()
            for u in range(u0, u0 + nu):
                full[p, u, rows, :] = s2[p, u] + r2[p, u]
            stage_copy(AG1, gi).start()

    def gather_stage2(p):
        for gi in range(3 * p, 3 * p + 3):
            stage_copy(AG1, gi).wait_recv()
            stage_copy(AG2, gi).start()
            if p == LAST:
                stage_copy(XOWN, gi).start()
            stage_copy(DDA, gi).start()
        if p == LAST:
            for gi in range(3 * p, 3 * p + 3):
                stage_copy(DDA, gi).wait_recv()
                stage_copy(XPART, gi).start()

    def gather_stage3(p):
        for gi in range(3 * p, 3 * p + 3):
            stage_copy(AG2, gi).wait_recv()
            stage_copy(DDB, gi).start()

    def outer_update(p, merge=True, outer=True):
        lay, mat = PIECES[p]
        wr, wbr, gr, mr = (w1, w1b, g1, m1) if mat == 1 else (w2, w2b, g2, m2)
        if merge:
            m_load(mat, lay).wait()
            wait_gathered(p)
        for u in range(8):
            rows, cols = unit_slice(mat, u)
            mean = full[p, u] * (1.0 / N_ALL)
            mom = OUTER_MOM * mr[lay, rows, cols] + mean
            glob = gr[lay, rows, cols] - OUTER_LR * (OUTER_MOM * mom + mean)
            if outer:
                mr[lay, rows, cols] = mom
                gr[lay, rows, cols] = glob
            if merge:
                merged = MERGE_MIX * wr[0, lay, rows, cols] + (1.0 - MERGE_MIX) * glob
                wr[0, lay, rows, cols] = merged
                wbr[lay, rows, cols] = merged.astype(BF16)

    def wait_gathered(p):
        for gi in range(3 * p, 3 * p + 3):
            stage_copy(DDB, gi).wait_recv()
            for stage in (XOWN, XPART) if p == LAST else (DDA,):
                stage_copy(stage, gi).wait_recv()

    def finish(frag):
        if frag == 0:
            outer_update(LAST, outer=False)
        else:
            for p, (part, mat) in enumerate(PIECES):
                m_load(mat, 2 + part).wait()
                wait_gathered(p)
        for gi in range(12):
            for cp in rs0_copies(gi):
                cp.wait_send()
            for stage in range(8 if GROUPS[gi][0] == LAST else 6):
                stage_copy(stage, gi).wait_send()

    def sync(frag):
        for p in range(4):
            reduce_stage2(p)
        for p in range(4):
            reduce_stage3(p)
        for p in GATHER_ORDER:
            gather_stage2(p)
        prev = None
        for p in GATHER_ORDER:
            gather_stage3(p)
            if prev is not None and frag == 0:
                outer_update(prev)
            prev = p

    def layers(lo, body):
        def run(i, _):
            body(i, lo - i)
            return 0
        return run

    forward(0)
    pl.semaphore_wait(bar, 7)
    loss_grad(0)
    back_chain(3)
    back_chain(2)

    lax.fori_loop(0, 2, layers(1, back_send), 0)
    lax.fori_loop(0, 2, layers(3, lambda i, lay: back_weights(lay)), 0)

    def back_hook(i, lay):
        back_full(lay)

        for p in range(1, 4):
            @pl.when(i == p - 1)
            def _(p=p):
                reduce_stage1(p)

    forward(1)
    loss_grad(1)
    reduce_stage1(0)
    lax.fori_loop(0, 3, layers(3, back_hook), 0)
    back_full(0, False)
    sync(0)

    forward(2, lambda: finish(0))
    loss_grad(2)

    lax.fori_loop(0, 2, layers(3, lambda i, lay: back_send(
        i, lay, lambda: outer_update(LAST, merge=False))), 0)
    back_full(1)
    back_full(0, False)

    forward(3)
    loss_grad(3)
    reduce_stage1(0)
    lax.fori_loop(0, 3, layers(3, back_hook), 0)
    back_full(0, False)
    sync(1)
    finish(1)


def write_body(w1, w2, g1, g2, m1, m2, full, *refs):
    dsts, stages, sem = refs[:6], refs[6:12], refs[12]
    srcs = (w1, w2, g1, g2, m1, m2)
    cps = []

    def put(src, i, lay):
        dst = dsts[i].at[0, lay] if i < 2 else dsts[i].at[lay]
        half = src.shape[0] // 2
        for rows in (pl.ds(0, half), pl.ds(half, half)):
            pltpu.make_async_copy(src.at[rows], dst.at[rows], sem.at[i, lay]).start()
        cps.append(pltpu.make_async_copy(src, dst, sem.at[i, lay]))

    for lay in range(2):
        for i in range(6):
            put(srcs[i].at[0, lay] if i < 2 else srcs[i].at[lay], i, lay)
    for p, (part, mat) in enumerate(PIECES):
        lay = 2 + part
        k = mat - 1
        wr, gr, mr = srcs[k], srcs[2 + k], srcs[4 + k]
        ws, gs, ms = stages[k], stages[2 + k], stages[4 + k]
        for u in range(8):
            rows, cols = unit_slice(mat, u)
            mean = full[p, u] * (1.0 / N_ALL)
            mom = OUTER_MOM * mr[lay, rows, cols] + mean
            glob = gr[lay, rows, cols] - OUTER_LR * (OUTER_MOM * mom + mean)
            ms[part, rows, cols] = mom
            gs[part, rows, cols] = glob
            ws[part, rows, cols] = MERGE_MIX * wr[0, lay, rows, cols] + (1.0 - MERGE_MIX) * glob
        for idx, st in enumerate((ws, gs, ms)):
            put(st.at[part], 2 * idx + k, lay)
    for cp in cps:
        cp.wait()


def solution(mesh):
    def device_fn(w1_loc, w2_loc, w1_glb, w2_glb, mom1, mom2, x_loc, y_loc):
        arrays = (w1_loc, w2_loc, w1_glb, w2_glb, mom1, mom2)
        shapes = [jax.ShapeDtypeStruct(a.shape, F32) for a in arrays]
        dma = pltpu.SemaphoreType.DMA
        work = pl.pallas_call(
            main_body,
            out_shape=shapes + [jax.ShapeDtypeStruct((4, 8, 128, 256), F32)],
            in_specs=[HBM] * 8,
            out_specs=[VMEM] * 7,
            scratch_shapes=[
                pltpu.VMEM((H, B, D), BF16), pltpu.VMEM((H, B, D), BF16),
                pltpu.VMEM((L, D, FF), BF16), pltpu.VMEM((L, FF, D), BF16),
                pltpu.VMEM((L, B, D), BF16), pltpu.VMEM((L, B, FF), BF16), pltpu.VMEM((L, B, FF), F32),
                pltpu.VMEM((B, D), F32), pltpu.VMEM((B, D), F32),
                pltpu.VMEM((2, B, D), BF16), pltpu.VMEM((2, B, FF), BF16),
                pltpu.VMEM((4, 8, 128, 256), BF16), pltpu.VMEM((3, 4, 8, 32, 256), BF16),
                pltpu.VMEM((4, 8, 32, 256), F32), pltpu.VMEM((4, 8, 16, 256), F32),
                pltpu.VMEM((4, 8, 16, 256), F32), pltpu.VMEM((4, 8, 16, 256), F32),
                dma((26,)), dma((12, 3)), dma((12, 3)), dma((8, 12)), dma((8, 12)),
            ],
            compiler_params=pltpu.CompilerParams(
                collective_id=0, has_side_effects=True, vmem_limit_bytes=22 * 2**20),
            name='diloco_round',
        )(*[pltpu.with_memory_space_constraint(a, pltpu.HBM) for a in (*arrays, x_loc, y_loc)])
        outs = pl.pallas_call(
            write_body,
            out_shape=shapes,
            in_specs=[VMEM] * 7,
            out_specs=[HBM] * 6,
            scratch_shapes=[pltpu.VMEM((2, D, FF), F32), pltpu.VMEM((2, FF, D), F32)] * 3 + [dma((6, L))],
            compiler_params=pltpu.CompilerParams(vmem_limit_bytes=16 * 2**20),
            name='write_out',
        )(*work)
        return tuple(outs)

    local_spec = P(('shard', 'worker'))
    whole_spec = P()
    return jax.shard_map(device_fn, mesh=mesh, in_specs=(local_spec, local_spec, whole_spec, whole_spec, whole_spec, whole_spec, local_spec, local_spec), out_specs=(local_spec, local_spec, whole_spec, whole_spec, whole_spec, whole_spec), check_vma=False)
```

```python
import jax
import jax.numpy as jnp
from jax import lax
from jax.experimental import pallas as pl
from jax.experimental.pallas import tpu as pltpu
from jax.sharding import PartitionSpec as P

OUTER_LR = 0.7
OUTER_MOM = 0.9
MERGE_MIX = 0.5

L = 4
H = 4
D = 256
FF = 1024
B = 128
NB = FF // D
INNER_LR = 2.0 * D / (FF * L)
N_ALL = 16
F32 = jnp.float32
BF16 = jnp.bfloat16
MESH = pl.DeviceIdType.MESH
HBM = pl.BlockSpec(memory_space=pltpu.HBM)
VMEM = pl.BlockSpec(memory_space=pltpu.VMEM)

PIECES = ((1, 2), (1, 1), (0, 2), (0, 1))
COLOR_UNITS = ((3, 3, 2), (3, 2, 3), (2, 3, 3), (3, 3, 2))
GROUPS = []
for piece_idx in range(4):
    first_unit = 0
    for color in range(3):
        GROUPS.append((piece_idx, color, first_unit, COLOR_UNITS[piece_idx][color]))
        first_unit += COLOR_UNITS[piece_idx][color]
GATHER_ORDER = (0, 2, 3, 1)
RS1, X2, AG1, AG2, DDA, DDB = range(6)


def dot(a, b, ca, cb):
    return lax.dot_general(a, b, (((ca,), (cb,)), ((), ())), preferred_element_type=F32)


def gelu_pair(a):
    k0 = 0.7978845608028654
    k1 = k0 * 0.044715
    a2 = a * a
    t = jnp.tanh(a * (k0 + k1 * a2))
    h = 0.5 + 0.5 * t
    u = a * h
    du = h + (u * (1.0 - h)) * (2.0 * k0 + (6.0 * k1) * a2)
    return u, du


def unit_slice(mat, u):
    if mat == 2:
        return pl.ds(u * 128, 128), pl.ds(0, 256)
    return pl.ds((u % 2) * 128, 128), pl.ds((u // 2) * 256, 256)


def main_body(w1_in, w2_in, g1_in, g2_in, m1_in, m2_in, x_in, y_in,
              w1, w2, g1, g2, m1, m2, full,
              xb, yb, w1b, w2b, hb, ub, du, hid, dhid, eb, cb,
              delta, raw, s1, r1, s2, r2,
              ld_sem, s0_send, s0_recv, st_send, st_recv):
    zc = lax.axis_index('shard')
    wk = lax.axis_index('worker')
    core = lax.rem(wk, 2)
    xc = lax.rem(wk // 2, 2)
    yc = wk // 4
    coord = (xc, yc, zc)

    def chip_peer(dim, same_core=True):
        w = wk
        s = zc
        if dim == 0:
            w = wk + 2 - 4 * xc
        elif dim == 1:
            w = wk + 4 - 8 * yc
        elif dim == 2:
            s = 1 - zc
        if not same_core:
            w = w + 1 - 2 * core
        return (s, w)

    partner = chip_peer(3, False)

    bar = pltpu.get_barrier_semaphore()
    pl.semaphore_signal(bar, inc=1, device_id=partner, device_id_type=MESH)
    for dim in range(3):
        for same in (True, False):
            pl.semaphore_signal(bar, inc=1, device_id=chip_peer(dim, same), device_id_type=MESH)

    def w_load(lay):
        return (pltpu.make_async_copy(w1_in.at[0, lay], w1.at[0, lay], ld_sem.at[lay]),
                pltpu.make_async_copy(w2_in.at[0, lay], w2.at[0, lay], ld_sem.at[L + lay]))

    def w_start(lay):
        for i in range(4):
            for src, dst, n, idx in ((w1_in, w1, D // 4, lay), (w2_in, w2, FF // 4, L + lay)):
                rows = pl.ds(i * n, n)
                pltpu.make_async_copy(src.at[0, lay, rows], dst.at[0, lay, rows], ld_sem.at[idx]).start()

    def g_load(mat, lay):
        if mat == 1:
            return pltpu.make_async_copy(g1_in.at[lay], g1.at[lay], ld_sem.at[2 * L + lay])
        return pltpu.make_async_copy(g2_in.at[lay], g2.at[lay], ld_sem.at[3 * L + lay])

    def m_load(mat, lay):
        if mat == 1:
            return pltpu.make_async_copy(m1_in.at[lay], m1.at[lay], ld_sem.at[4 * L + lay])
        return pltpu.make_async_copy(m2_in.at[lay], m2.at[lay], ld_sem.at[5 * L + lay])

    x_load = pltpu.make_async_copy(x_in.at[0], xb, ld_sem.at[6 * L])
    y_load = pltpu.make_async_copy(y_in.at[0], yb, ld_sem.at[6 * L + 1])
    x_load.start()
    w_start(0)
    y_load.start()
    for lay in range(1, L):
        w_start(lay)
    for lay in range(L):
        for mat in (1, 2):
            g_load(mat, lay).start()
    for lay in range(L):
        for mat in (1, 2):
            m_load(mat, lay).start()
    x_load.wait()
    y_load.wait()

    def dims_of(color_idx):
        return color_idx % 3, (color_idx + 1) % 3, (color_idx + 2) % 3

    def rs0_copies(gi):
        p, c, u0, nu = GROUPS[gi]
        d0 = dims_of(c)[0]
        k0 = coord[d0]
        us = pl.ds(u0, nu)
        other = 1 - core

        def rows(tc, blk):
            return pl.ds(pl.multiple_of(tc * 64 + blk * 32, 32), 32)

        out = []
        for idx, (tc, blk, dev) in enumerate(((other, k0, partner),
                                               (core, 1 - k0, chip_peer(d0, True)),
                                               (other, 1 - k0, chip_peer(d0, False)))):
            out.append(pltpu.make_async_remote_copy(
                src_ref=delta.at[p, us, rows(tc, blk)], dst_ref=raw.at[idx, p, us],
                send_sem=s0_send.at[gi, idx], recv_sem=s0_recv.at[gi, idx],
                device_id=dev, device_id_type=MESH))
        return out

    def stage_copy(stage, gi):
        p, c, u0, nu = GROUPS[gi]
        d0, d1, d2 = dims_of(c)
        k0, k1, k2 = coord[d0], coord[d1], coord[d2]
        us = pl.ds(u0, nu)
        if stage == RS1:
            src, dst, dev = s1.at[p, us, pl.ds(pl.multiple_of((1 - k1) * 16, 16), 16)], r1.at[p, us], chip_peer(d1)
        elif stage == X2:
            src, dst, dev = s2.at[p, us], r2.at[p, us], chip_peer(d2)
        else:
            base = core * 64
            if stage == AG1:
                off, n, dev = base + k0 * 32 + k1 * 16, 16, chip_peer(d1)
            elif stage == AG2:
                off, n, dev = base + k0 * 32, 32, chip_peer(d0)
            elif stage == DDA:
                off, n, dev = base + k0 * 32, 32, partner
            else:
                off, n, dev = base + (1 - k0) * 32, 32, partner
            src = full.at[p, us, pl.ds(pl.multiple_of(off, 16), n)]
            dst = src
        return pltpu.make_async_remote_copy(
            src_ref=src, dst_ref=dst, send_sem=st_send.at[stage, gi], recv_sem=st_recv.at[stage, gi],
            device_id=dev, device_id_type=MESH)

    def forward(k, before_layer_1=None):
        hid[...] = xb[k].astype(F32)

        def layer(lay, _):
            if k == 0:
                for cp in w_load(lay):
                    cp.wait()
            if before_layer_1 is not None and lay == 1:
                before_layer_1()
            h_bf = hid[...].astype(BF16)
            hb[lay] = h_bf
            acc = hid[...]
            for j in range(NB):
                cols = slice(j * D, (j + 1) * D)
                if k == 0:
                    w1b[lay, :, cols] = w1[0, lay, :, cols].astype(BF16)
                    w2b[lay, cols, :] = w2[0, lay, cols, :].astype(BF16)
                a = dot(h_bf, w1b[lay, :, cols], 1, 0)
                u, dg = gelu_pair(a)
                u_bf = u.astype(BF16)
                ub[lay, :, cols] = u_bf
                du[lay, :, cols] = dg
                acc = acc + dot(u_bf, w2b[lay, cols, :], 1, 0)
            hid[...] = acc
            return 0

        for lay in range(L):
            layer(lay, 0)

    def loss_grad(k):
        dhid[...] = (2.0 / (B * D)) * (hid[...] - yb[k].astype(F32))

    def update2(lay, cols, u_j, e):
        new2 = w2[0, lay, cols, :] - INNER_LR * dot(u_j, e, 0, 0)
        w2[0, lay, cols, :] = new2
        w2b[lay, cols, :] = new2.astype(BF16)

    def update1(lay, cols, h_bf, c):
        new1 = w1[0, lay, :, cols] - INNER_LR * dot(h_bf, c, 0, 0)
        w1[0, lay, :, cols] = new1
        w1b[lay, :, cols] = new1.astype(BF16)

    def send_piece(i, which):
        for p in (which, 2 + which):
            @pl.when(i == p // 2)
            def _(p=p):
                for gi in range(3 * p, 3 * p + 3):
                    for cp in rs0_copies(gi):
                        cp.start()

    def back_send(i, lay, after_first=None):
        p = 2 * i
        e = dhid[...].astype(BF16)
        h_bf = hb[lay]
        g_load(2, lay).wait()
        for j in range(NB):
            cols = slice(j * D, (j + 1) * D)
            new2 = w2[0, lay, cols, :] - INNER_LR * dot(ub[lay, :, cols], e, 0, 0)
            w2[0, lay, cols, :] = new2
            dl = (g2[lay, cols, :] - new2).astype(BF16)
            delta[p, 2 * j] = dl[:128]
            delta[p, 2 * j + 1] = dl[128:]
        send_piece(i, 0)
        if after_first is not None:
            pl.when(i == 0)(after_first)
        g_load(1, lay).wait()
        acc = dhid[...]
        for j in range(NB):
            cols = slice(j * D, (j + 1) * D)
            d_u = dot(e, w2b[lay, cols, :], 1, 1)
            c = (du[lay, :, cols] * d_u).astype(BF16)
            acc = acc + dot(c, w1b[lay, :, cols], 1, 1)
            new1 = w1[0, lay, :, cols] - INNER_LR * dot(h_bf, c, 0, 0)
            w1[0, lay, :, cols] = new1
            w1b[lay, :, cols] = new1.astype(BF16)
            dl = (g1[lay, :, cols] - new1).astype(BF16)
            delta[p + 1, 2 * j] = dl[:128]
            delta[p + 1, 2 * j + 1] = dl[128:]
        dhid[...] = acc
        send_piece(i, 1)
        w2b[lay] = w2[0, lay].astype(BF16)

    def back_full(lay, need_input_grad=True):
        e = dhid[...].astype(BF16)
        h_bf = hb[lay]
        acc = dhid[...]
        for j in range(NB):
            cols = slice(j * D, (j + 1) * D)
            d_u = dot(e, w2b[lay, cols, :], 1, 1)
            c = (du[lay, :, cols] * d_u).astype(BF16)
            update2(lay, cols, ub[lay, :, cols], e)
            if need_input_grad:
                acc = acc + dot(c, w1b[lay, :, cols], 1, 1)
            update1(lay, cols, h_bf, c)
        if need_input_grad:
            dhid[...] = acc

    def back_chain(lay):
        e = dhid[...].astype(BF16)
        eb[lay - 2] = e
        acc = dhid[...]
        for j in range(NB):
            cols = slice(j * D, (j + 1) * D)
            d_u = dot(e, w2b[lay, cols, :], 1, 1)
            c = (du[lay, :, cols] * d_u).astype(BF16)
            cb[lay - 2, :, cols] = c
            acc = acc + dot(c, w1b[lay, :, cols], 1, 1)
        dhid[...] = acc

    def back_weights(lay):
        e = eb[lay - 2]
        h_bf = hb[lay]
        for j in range(NB):
            cols = slice(j * D, (j + 1) * D)
            update2(lay, cols, ub[lay, :, cols], e)
            update1(lay, cols, h_bf, cb[lay - 2, :, cols])

    def reduce_stage1(p):
        for gi in range(3 * p, 3 * p + 3):
            _, c, u0, nu = GROUPS[gi]
            rows = pl.ds(pl.multiple_of(core * 64 + coord[dims_of(c)[0]] * 32, 32), 32)
            for cp in rs0_copies(gi):
                cp.wait_recv()
            for u in range(u0, u0 + nu):
                s1[p, u] = ((delta[p, u, rows, :].astype(F32) + raw[0, p, u].astype(F32))
                            + (raw[1, p, u].astype(F32) + raw[2, p, u].astype(F32)))
            stage_copy(RS1, gi).start()

    def reduce_stage2(p):
        for gi in range(3 * p, 3 * p + 3):
            _, c, u0, nu = GROUPS[gi]
            rows = pl.ds(pl.multiple_of(coord[dims_of(c)[1]] * 16, 16), 16)
            stage_copy(RS1, gi).wait_recv()
            for u in range(u0, u0 + nu):
                s2[p, u] = s1[p, u, rows, :] + r1[p, u]
            stage_copy(X2, gi).start()

    def reduce_stage3(p):
        for gi in range(3 * p, 3 * p + 3):
            _, c, u0, nu = GROUPS[gi]
            d0, d1, d2 = dims_of(c)
            rows = pl.ds(pl.multiple_of(core * 64 + coord[d0] * 32 + coord[d1] * 16, 16), 16)
            stage_copy(X2, gi).wait_recv()
            for u in range(u0, u0 + nu):
                full[p, u, rows, :] = s2[p, u] + r2[p, u]
            stage_copy(AG1, gi).start()

    def gather_stage2(p):
        for gi in range(3 * p, 3 * p + 3):
            stage_copy(AG1, gi).wait_recv()
            stage_copy(AG2, gi).start()
            stage_copy(DDA, gi).start()

    def gather_stage3(p):
        for gi in range(3 * p, 3 * p + 3):
            stage_copy(AG2, gi).wait_recv()
            stage_copy(DDB, gi).start()

    def outer_update(p, merge=True, outer=True):
        lay, mat = PIECES[p]
        wr, wbr, gr, mr = (w1, w1b, g1, m1) if mat == 1 else (w2, w2b, g2, m2)
        if merge:
            m_load(mat, lay).wait()
            wait_gathered(p)
        for u in range(8):
            rows, cols = unit_slice(mat, u)
            mean = full[p, u] * (1.0 / N_ALL)
            mom = OUTER_MOM * mr[lay, rows, cols] + mean
            glob = gr[lay, rows, cols] - OUTER_LR * (OUTER_MOM * mom + mean)
            if outer:
                mr[lay, rows, cols] = mom
                gr[lay, rows, cols] = glob
            if merge:
                merged = MERGE_MIX * wr[0, lay, rows, cols] + (1.0 - MERGE_MIX) * glob
                wr[0, lay, rows, cols] = merged
                wbr[lay, rows, cols] = merged.astype(BF16)

    last_piece = GATHER_ORDER[-1]

    def wait_gathered(p):
        for gi in range(3 * p, 3 * p + 3):
            stage_copy(DDA, gi).wait_recv()
            stage_copy(DDB, gi).wait_recv()

    def finish(frag):
        if frag == 0:
            outer_update(last_piece, outer=False)
        else:
            for p, (part, mat) in enumerate(PIECES):
                m_load(mat, 2 + part).wait()
                wait_gathered(p)
        for gi in range(12):
            for cp in rs0_copies(gi):
                cp.wait_send()
            for stage in range(6):
                stage_copy(stage, gi).wait_send()

    def sync(frag):
        reduce_stage1(3)
        for p in range(4):
            reduce_stage2(p)
        for p in range(4):
            reduce_stage3(p)
        for p in GATHER_ORDER:
            gather_stage2(p)
        back_full(1)
        back_full(0, False)
        prev = None
        for p in GATHER_ORDER:
            gather_stage3(p)
            if prev is not None and frag == 0:
                outer_update(prev)
            prev = p

    def layers(lo, body):
        def run(i, _):
            body(i, lo - i)
            return 0
        return run

    forward(0)
    pl.semaphore_wait(bar, 7)
    loss_grad(0)
    back_chain(3)
    back_chain(2)

    lax.fori_loop(0, 2, layers(1, back_send), 0)
    lax.fori_loop(0, 2, layers(3, lambda i, lay: back_weights(lay)), 0)

    def back_hook(i, lay):
        back_full(lay)
        for p in (1, 2):
            @pl.when(i == p - 1)
            def _(p=p):
                reduce_stage1(p)

    forward(1)
    loss_grad(1)
    reduce_stage1(0)
    lax.fori_loop(0, 2, layers(3, back_hook), 0)
    sync(0)

    forward(2, lambda: finish(0))
    loss_grad(2)

    lax.fori_loop(0, 2, layers(3, lambda i, lay: back_send(
        i, lay, lambda: outer_update(last_piece, merge=False))), 0)
    back_full(1)
    back_full(0, False)

    forward(3)
    loss_grad(3)
    reduce_stage1(0)
    lax.fori_loop(0, 2, layers(3, back_hook), 0)
    sync(1)
    finish(1)


def write_body(w1, w2, g1, g2, m1, m2, full, *refs):
    dsts, stages, sem = refs[:6], refs[6:12], refs[12]
    srcs = (w1, w2, g1, g2, m1, m2)
    cps = []

    def put(src, i, lay):
        dst = dsts[i].at[0, lay] if i < 2 else dsts[i].at[lay]
        half = src.shape[0] // 2
        for rows in (pl.ds(0, half), pl.ds(half, half)):
            pltpu.make_async_copy(src.at[rows], dst.at[rows], sem.at[i, lay]).start()
        cps.append(pltpu.make_async_copy(src, dst, sem.at[i, lay]))

    for lay in range(2):
        for i in range(6):
            put(srcs[i].at[0, lay] if i < 2 else srcs[i].at[lay], i, lay)
    for p, (part, mat) in enumerate(PIECES):
        lay = 2 + part
        k = mat - 1
        wr, gr, mr = srcs[k], srcs[2 + k], srcs[4 + k]
        ws, gs, ms = stages[k], stages[2 + k], stages[4 + k]
        for u in range(8):
            rows, cols = unit_slice(mat, u)
            mean = full[p, u] * (1.0 / N_ALL)
            mom = OUTER_MOM * mr[lay, rows, cols] + mean
            glob = gr[lay, rows, cols] - OUTER_LR * (OUTER_MOM * mom + mean)
            ms[part, rows, cols] = mom
            gs[part, rows, cols] = glob
            ws[part, rows, cols] = MERGE_MIX * wr[0, lay, rows, cols] + (1.0 - MERGE_MIX) * glob
        for idx, st in enumerate((ws, gs, ms)):
            put(st.at[part], 2 * idx + k, lay)
    for cp in cps:
        cp.wait()


def solution(mesh):
    def device_fn(w1_loc, w2_loc, w1_glb, w2_glb, mom1, mom2, x_loc, y_loc):
        arrays = (w1_loc, w2_loc, w1_glb, w2_glb, mom1, mom2)
        shapes = [jax.ShapeDtypeStruct(a.shape, F32) for a in arrays]
        dma = pltpu.SemaphoreType.DMA
        work = pl.pallas_call(
            main_body,
            out_shape=shapes + [jax.ShapeDtypeStruct((4, 8, 128, 256), F32)],
            in_specs=[HBM] * 8,
            out_specs=[VMEM] * 7,
            scratch_shapes=[
                pltpu.VMEM((H, B, D), BF16), pltpu.VMEM((H, B, D), BF16),
                pltpu.VMEM((L, D, FF), BF16), pltpu.VMEM((L, FF, D), BF16),
                pltpu.VMEM((L, B, D), BF16), pltpu.VMEM((L, B, FF), BF16), pltpu.VMEM((L, B, FF), F32),
                pltpu.VMEM((B, D), F32), pltpu.VMEM((B, D), F32),
                pltpu.VMEM((2, B, D), BF16), pltpu.VMEM((2, B, FF), BF16),
                pltpu.VMEM((4, 8, 128, 256), BF16), pltpu.VMEM((3, 4, 8, 32, 256), BF16),
                pltpu.VMEM((4, 8, 32, 256), F32), pltpu.VMEM((4, 8, 16, 256), F32),
                pltpu.VMEM((4, 8, 16, 256), F32), pltpu.VMEM((4, 8, 16, 256), F32),
                dma((26,)), dma((12, 3)), dma((12, 3)), dma((6, 12)), dma((6, 12)),
            ],
            compiler_params=pltpu.CompilerParams(
                collective_id=0, has_side_effects=True, vmem_limit_bytes=22 * 2**20),
            name='diloco_round',
        )(*[pltpu.with_memory_space_constraint(a, pltpu.HBM) for a in (*arrays, x_loc, y_loc)])
        outs = pl.pallas_call(
            write_body,
            out_shape=shapes,
            in_specs=[VMEM] * 7,
            out_specs=[HBM] * 6,
            scratch_shapes=[pltpu.VMEM((2, D, FF), F32), pltpu.VMEM((2, FF, D), F32)] * 3 + [dma((6, L))],
            compiler_params=pltpu.CompilerParams(vmem_limit_bytes=16 * 2**20),
            name='write_out',
        )(*work)
        return tuple(outs)

    local_spec = P(('shard', 'worker'))
    whole_spec = P()
    return jax.shard_map(device_fn, mesh=mesh, in_specs=(local_spec, local_spec, whole_spec, whole_spec, whole_spec, whole_spec, local_spec, local_spec), out_specs=(local_spec, local_spec, whole_spec, whole_spec, whole_spec, whole_spec), check_vma=False)
```

```python
import jax
import jax.numpy as jnp
from jax import lax
from jax.experimental import pallas as pl
from jax.experimental.pallas import tpu as pltpu
from jax.sharding import PartitionSpec as P

OUTER_LR = 0.7
OUTER_MOM = 0.9
MERGE_MIX = 0.5

L = 4
H = 4
D = 256
FF = 1024
B = 128
NB = FF // D
INNER_LR = 2.0 * D / (FF * L)
N_ALL = 16
GELU_K0 = 0.7978845608028654
GELU_K1 = GELU_K0 * 0.044715
F32 = jnp.float32
BF16 = jnp.bfloat16
MESH = pl.DeviceIdType.MESH
HBM = pl.BlockSpec(memory_space=pltpu.HBM)
VMEM = pl.BlockSpec(memory_space=pltpu.VMEM)

PIECES = ((1, 2), (1, 1), (0, 2), (0, 1))
COLOR_UNITS = ((3, 3, 2), (3, 2, 3), (2, 3, 3), (3, 3, 2))
GROUPS = []
for piece_idx in range(4):
    first_unit = 0
    for color in range(3):
        GROUPS.append((piece_idx, color, first_unit, COLOR_UNITS[piece_idx][color]))
        first_unit += COLOR_UNITS[piece_idx][color]
GATHER_ORDER = (0, 2, 3, 1)
RS1, X2, AG1, AG2, DDA, DDB = range(6)


def dot(a, b, ca, cb):
    return lax.dot_general(a, b, (((ca,), (cb,)), ((), ())), preferred_element_type=F32)


def gelu_parts(a):
    a2 = a * a
    t = jnp.tanh(a * (GELU_K0 + GELU_K1 * a2))
    return 0.5 + 0.5 * t, a2


def gelu_grad(u, h, a2):
    return h + (u * (1.0 - h)) * (2.0 * GELU_K0 + (6.0 * GELU_K1) * a2)


def unit_slice(mat, u):
    if mat == 2:
        return pl.ds(u * 128, 128), pl.ds(0, 256)
    return pl.ds((u % 2) * 128, 128), pl.ds((u // 2) * 256, 256)


def main_body(w1_in, w2_in, g1_in, g2_in, m1_in, m2_in, x_in, y_in,
              w1, w2, g1, g2, m1, m2, full,
              xb, yb, w1b, w2b, hb, ub, du, hid, dhid, eb, cb,
              delta, raw, s1, r1, s2, r2,
              ld_sem, s0_send, s0_recv, st_send, st_recv):
    zc = lax.axis_index('shard')
    wk = lax.axis_index('worker')
    core = lax.rem(wk, 2)
    xc = lax.rem(wk // 2, 2)
    yc = wk // 4
    coord = (xc, yc, zc)

    def chip_peer(dim, same_core=True):
        w = wk
        s = zc
        if dim == 0:
            w = wk + 2 - 4 * xc
        elif dim == 1:
            w = wk + 4 - 8 * yc
        elif dim == 2:
            s = 1 - zc
        if not same_core:
            w = w + 1 - 2 * core
        return (s, w)

    partner = chip_peer(3, False)

    bar = pltpu.get_barrier_semaphore()
    pl.semaphore_signal(bar, inc=1, device_id=partner, device_id_type=MESH)
    for dim in range(3):
        for same in (True, False):
            pl.semaphore_signal(bar, inc=1, device_id=chip_peer(dim, same), device_id_type=MESH)

    def w_load(lay):
        return (pltpu.make_async_copy(w1_in.at[0, lay], w1.at[0, lay], ld_sem.at[lay]),
                pltpu.make_async_copy(w2_in.at[0, lay], w2.at[0, lay], ld_sem.at[L + lay]))

    def w_start(lay):
        for i in range(4):
            for src, dst, n, idx in ((w1_in, w1, D // 4, lay), (w2_in, w2, FF // 4, L + lay)):
                rows = pl.ds(i * n, n)
                pltpu.make_async_copy(src.at[0, lay, rows], dst.at[0, lay, rows], ld_sem.at[idx]).start()

    def g_load(mat, lay):
        if mat == 1:
            return pltpu.make_async_copy(g1_in.at[lay], g1.at[lay], ld_sem.at[2 * L + lay])
        return pltpu.make_async_copy(g2_in.at[lay], g2.at[lay], ld_sem.at[3 * L + lay])

    def m_load(mat, lay):
        if mat == 1:
            return pltpu.make_async_copy(m1_in.at[lay], m1.at[lay], ld_sem.at[4 * L + lay])
        return pltpu.make_async_copy(m2_in.at[lay], m2.at[lay], ld_sem.at[5 * L + lay])

    x_load = pltpu.make_async_copy(x_in.at[0], xb, ld_sem.at[6 * L])
    y_load = pltpu.make_async_copy(y_in.at[0], yb, ld_sem.at[6 * L + 1])
    x_load.start()
    w_start(0)
    y_load.start()
    for lay in range(1, L):
        w_start(lay)
    for lay in range(L):
        for mat in (1, 2):
            g_load(mat, lay).start()
    for lay in range(L):
        for mat in (1, 2):
            m_load(mat, lay).start()
    x_load.wait()
    y_load.wait()

    def dims_of(color_idx):
        return color_idx % 3, (color_idx + 1) % 3, (color_idx + 2) % 3

    def rs0_copies(gi):
        p, c, u0, nu = GROUPS[gi]
        d0 = dims_of(c)[0]
        k0 = coord[d0]
        us = pl.ds(u0, nu)
        other = 1 - core

        def rows(tc, blk):
            return pl.ds(pl.multiple_of(tc * 64 + blk * 32, 32), 32)

        out = []
        for idx, (tc, blk, dev) in enumerate(((other, k0, partner),
                                               (core, 1 - k0, chip_peer(d0, True)),
                                               (other, 1 - k0, chip_peer(d0, False)))):
            out.append(pltpu.make_async_remote_copy(
                src_ref=delta.at[p, us, rows(tc, blk)], dst_ref=raw.at[idx, p, us],
                send_sem=s0_send.at[gi, idx], recv_sem=s0_recv.at[gi, idx],
                device_id=dev, device_id_type=MESH))
        return out

    def stage_copy(stage, gi):
        p, c, u0, nu = GROUPS[gi]
        d0, d1, d2 = dims_of(c)
        k0, k1, k2 = coord[d0], coord[d1], coord[d2]
        us = pl.ds(u0, nu)
        if stage == RS1:
            src, dst, dev = s1.at[p, us, pl.ds(pl.multiple_of((1 - k1) * 16, 16), 16)], r1.at[p, us], chip_peer(d1)
        elif stage == X2:
            src, dst, dev = s2.at[p, us], r2.at[p, us], chip_peer(d2)
        else:
            base = core * 64
            if stage == AG1:
                off, n, dev = base + k0 * 32 + k1 * 16, 16, chip_peer(d1)
            elif stage == AG2:
                off, n, dev = base + k0 * 32, 32, chip_peer(d0)
            elif stage == DDA:
                off, n, dev = base + k0 * 32, 32, partner
            else:
                off, n, dev = base + (1 - k0) * 32, 32, partner
            src = full.at[p, us, pl.ds(pl.multiple_of(off, 16), n)]
            dst = src
        return pltpu.make_async_remote_copy(
            src_ref=src, dst_ref=dst, send_sem=st_send.at[stage, gi], recv_sem=st_recv.at[stage, gi],
            device_id=dev, device_id_type=MESH)

    def keeps_pre_act(k, lay):
        return k == 2 or (k == 0 and lay < 2)

    def grad_from_pre_act(lay, cols):
        a = du[lay, :, cols]
        h, a2 = gelu_parts(a)
        return gelu_grad(a * h, h, a2)

    def forward(k, before_layer_1=None):
        hid[...] = xb[k].astype(F32)

        def layer(lay, _):
            if k == 0:
                for cp in w_load(lay):
                    cp.wait()
            if before_layer_1 is not None and lay == 1:
                before_layer_1()
            h_bf = hid[...].astype(BF16)
            hb[lay] = h_bf
            acc = hid[...]
            for j in range(NB):
                cols = slice(j * D, (j + 1) * D)
                if k == 0:
                    w1b[lay, :, cols] = w1[0, lay, :, cols].astype(BF16)
                    w2b[lay, cols, :] = w2[0, lay, cols, :].astype(BF16)
                a = dot(h_bf, w1b[lay, :, cols], 1, 0)
                h, a2 = gelu_parts(a)
                u = a * h
                u_bf = u.astype(BF16)
                ub[lay, :, cols] = u_bf
                du[lay, :, cols] = a if keeps_pre_act(k, lay) else gelu_grad(u, h, a2)
                acc = acc + dot(u_bf, w2b[lay, cols, :], 1, 0)
            hid[...] = acc
            return 0

        for lay in range(L):
            layer(lay, 0)

    def loss_grad(k):
        dhid[...] = (2.0 / (B * D)) * (hid[...] - yb[k].astype(F32))

    def update2(lay, cols, u_j, e):
        new2 = w2[0, lay, cols, :] - INNER_LR * dot(u_j, e, 0, 0)
        w2[0, lay, cols, :] = new2
        w2b[lay, cols, :] = new2.astype(BF16)

    def update1(lay, cols, h_bf, c):
        new1 = w1[0, lay, :, cols] - INNER_LR * dot(h_bf, c, 0, 0)
        w1[0, lay, :, cols] = new1
        w1b[lay, :, cols] = new1.astype(BF16)

    def send_piece(i, which):
        for p in (which, 2 + which):
            @pl.when(i == p // 2)
            def _(p=p):
                for gi in range(3 * p, 3 * p + 3):
                    for cp in rs0_copies(gi):
                        cp.start()

    def back_send(i, lay, after_first=None):
        p = 2 * i
        e = dhid[...].astype(BF16)
        h_bf = hb[lay]
        g_load(2, lay).wait()
        for j in range(NB):
            cols = slice(j * D, (j + 1) * D)
            new2 = w2[0, lay, cols, :] - INNER_LR * dot(ub[lay, :, cols], e, 0, 0)
            w2[0, lay, cols, :] = new2
            dl = (g2[lay, cols, :] - new2).astype(BF16)
            delta[p, 2 * j] = dl[:128]
            delta[p, 2 * j + 1] = dl[128:]
        send_piece(i, 0)
        if after_first is not None:
            pl.when(i == 0)(after_first)
        g_load(1, lay).wait()
        acc = dhid[...]
        for j in range(NB):
            cols = slice(j * D, (j + 1) * D)
            d_u = dot(e, w2b[lay, cols, :], 1, 1)
            c = (grad_from_pre_act(lay, cols) * d_u).astype(BF16)
            acc = acc + dot(c, w1b[lay, :, cols], 1, 1)
            new1 = w1[0, lay, :, cols] - INNER_LR * dot(h_bf, c, 0, 0)
            w1[0, lay, :, cols] = new1
            w1b[lay, :, cols] = new1.astype(BF16)
            dl = (g1[lay, :, cols] - new1).astype(BF16)
            delta[p + 1, 2 * j] = dl[:128]
            delta[p + 1, 2 * j + 1] = dl[128:]
        dhid[...] = acc
        send_piece(i, 1)
        w2b[lay] = w2[0, lay].astype(BF16)

    def back_full(lay, need_input_grad=True, pre_act=False):
        e = dhid[...].astype(BF16)
        h_bf = hb[lay]
        acc = dhid[...]
        for j in range(NB):
            cols = slice(j * D, (j + 1) * D)
            d_u = dot(e, w2b[lay, cols, :], 1, 1)
            grad = grad_from_pre_act(lay, cols) if pre_act else du[lay, :, cols]
            c = (grad * d_u).astype(BF16)
            update2(lay, cols, ub[lay, :, cols], e)
            if need_input_grad:
                acc = acc + dot(c, w1b[lay, :, cols], 1, 1)
            update1(lay, cols, h_bf, c)
        if need_input_grad:
            dhid[...] = acc

    def back_chain(lay):
        e = dhid[...].astype(BF16)
        eb[lay - 2] = e
        acc = dhid[...]
        for j in range(NB):
            cols = slice(j * D, (j + 1) * D)
            d_u = dot(e, w2b[lay, cols, :], 1, 1)
            c = (du[lay, :, cols] * d_u).astype(BF16)
            cb[lay - 2, :, cols] = c
            acc = acc + dot(c, w1b[lay, :, cols], 1, 1)
        dhid[...] = acc

    def back_weights(lay):
        e = eb[lay - 2]
        h_bf = hb[lay]
        for j in range(NB):
            cols = slice(j * D, (j + 1) * D)
            update2(lay, cols, ub[lay, :, cols], e)
            update1(lay, cols, h_bf, cb[lay - 2, :, cols])

    def reduce_stage1(p):
        for gi in range(3 * p, 3 * p + 3):
            _, c, u0, nu = GROUPS[gi]
            rows = pl.ds(pl.multiple_of(core * 64 + coord[dims_of(c)[0]] * 32, 32), 32)
            for cp in rs0_copies(gi):
                cp.wait_recv()
            for u in range(u0, u0 + nu):
                s1[p, u] = ((delta[p, u, rows, :].astype(F32) + raw[0, p, u].astype(F32))
                            + (raw[1, p, u].astype(F32) + raw[2, p, u].astype(F32)))
            stage_copy(RS1, gi).start()

    def reduce_stage2(p):
        for gi in range(3 * p, 3 * p + 3):
            _, c, u0, nu = GROUPS[gi]
            rows = pl.ds(pl.multiple_of(coord[dims_of(c)[1]] * 16, 16), 16)
            stage_copy(RS1, gi).wait_recv()
            for u in range(u0, u0 + nu):
                s2[p, u] = s1[p, u, rows, :] + r1[p, u]
            stage_copy(X2, gi).start()

    def reduce_stage3(p):
        for gi in range(3 * p, 3 * p + 3):
            _, c, u0, nu = GROUPS[gi]
            d0, d1, d2 = dims_of(c)
            rows = pl.ds(pl.multiple_of(core * 64 + coord[d0] * 32 + coord[d1] * 16, 16), 16)
            stage_copy(X2, gi).wait_recv()
            for u in range(u0, u0 + nu):
                full[p, u, rows, :] = s2[p, u] + r2[p, u]
            stage_copy(AG1, gi).start()

    def gather_stage2(p):
        for gi in range(3 * p, 3 * p + 3):
            stage_copy(AG1, gi).wait_recv()
            stage_copy(AG2, gi).start()
            stage_copy(DDA, gi).start()

    def gather_stage3(p):
        for gi in range(3 * p, 3 * p + 3):
            stage_copy(AG2, gi).wait_recv()
            stage_copy(DDB, gi).start()

    def outer_update(p, merge=True, outer=True):
        lay, mat = PIECES[p]
        wr, wbr, gr, mr = (w1, w1b, g1, m1) if mat == 1 else (w2, w2b, g2, m2)
        if merge:
            m_load(mat, lay).wait()
            wait_gathered(p)
        for u in range(8):
            rows, cols = unit_slice(mat, u)
            mean = full[p, u] * (1.0 / N_ALL)
            mom = OUTER_MOM * mr[lay, rows, cols] + mean
            glob = gr[lay, rows, cols] - OUTER_LR * (OUTER_MOM * mom + mean)
            if outer:
                mr[lay, rows, cols] = mom
                gr[lay, rows, cols] = glob
            if merge:
                merged = MERGE_MIX * wr[0, lay, rows, cols] + (1.0 - MERGE_MIX) * glob
                wr[0, lay, rows, cols] = merged
                wbr[lay, rows, cols] = merged.astype(BF16)

    last_piece = GATHER_ORDER[-1]

    def wait_gathered(p):
        for gi in range(3 * p, 3 * p + 3):
            stage_copy(DDA, gi).wait_recv()
            stage_copy(DDB, gi).wait_recv()

    def finish(frag):
        if frag == 0:
            outer_update(last_piece, outer=False)
        else:
            for p, (part, mat) in enumerate(PIECES):
                m_load(mat, 2 + part).wait()
                wait_gathered(p)
        for gi in range(12):
            for cp in rs0_copies(gi):
                cp.wait_send()
            for stage in range(6):
                stage_copy(stage, gi).wait_send()

    def sync(frag):
        reduce_stage1(3)
        for p in range(4):
            reduce_stage2(p)
        for p in range(4):
            reduce_stage3(p)
        for p in GATHER_ORDER:
            gather_stage2(p)
        back_full(1)
        back_full(0, False)
        prev = None
        for p in GATHER_ORDER:
            gather_stage3(p)
            if prev is not None and frag == 0:
                outer_update(prev)
            prev = p

    def layers(lo, body):
        def run(i, _):
            body(i, lo - i)
            return 0
        return run

    forward(0)
    pl.semaphore_wait(bar, 7)
    loss_grad(0)
    back_chain(3)
    back_chain(2)

    lax.fori_loop(0, 2, layers(1, back_send), 0)
    lax.fori_loop(0, 2, layers(3, lambda i, lay: back_weights(lay)), 0)

    def back_hook(i, lay):
        back_full(lay)
        for p in (1, 2):
            @pl.when(i == p - 1)
            def _(p=p):
                reduce_stage1(p)

    forward(1)
    loss_grad(1)
    reduce_stage1(0)
    lax.fori_loop(0, 2, layers(3, back_hook), 0)
    sync(0)

    forward(2, lambda: finish(0))
    loss_grad(2)

    lax.fori_loop(0, 2, layers(3, lambda i, lay: back_send(
        i, lay, lambda: outer_update(last_piece, merge=False))), 0)
    back_full(1, True, True)
    back_full(0, False, True)

    forward(3)
    loss_grad(3)
    reduce_stage1(0)
    lax.fori_loop(0, 2, layers(3, back_hook), 0)
    sync(1)
    finish(1)


def write_body(w1, w2, g1, g2, m1, m2, full, *refs):
    dsts, stages, sem = refs[:6], refs[6:12], refs[12]
    srcs = (w1, w2, g1, g2, m1, m2)
    cps = []

    def put(src, i, lay):
        dst = dsts[i].at[0, lay] if i < 2 else dsts[i].at[lay]
        half = src.shape[0] // 2
        for rows in (pl.ds(0, half), pl.ds(half, half)):
            pltpu.make_async_copy(src.at[rows], dst.at[rows], sem.at[i, lay]).start()
        cps.append(pltpu.make_async_copy(src, dst, sem.at[i, lay]))

    for lay in range(2):
        for i in range(6):
            put(srcs[i].at[0, lay] if i < 2 else srcs[i].at[lay], i, lay)
    for p, (part, mat) in enumerate(PIECES):
        lay = 2 + part
        k = mat - 1
        wr, gr, mr = srcs[k], srcs[2 + k], srcs[4 + k]
        ws, gs, ms = stages[k], stages[2 + k], stages[4 + k]
        for u in range(8):
            rows, cols = unit_slice(mat, u)
            mean = full[p, u] * (1.0 / N_ALL)
            mom = OUTER_MOM * mr[lay, rows, cols] + mean
            glob = gr[lay, rows, cols] - OUTER_LR * (OUTER_MOM * mom + mean)
            ms[part, rows, cols] = mom
            gs[part, rows, cols] = glob
            ws[part, rows, cols] = MERGE_MIX * wr[0, lay, rows, cols] + (1.0 - MERGE_MIX) * glob
        for idx, st in enumerate((ws, gs, ms)):
            put(st.at[part], 2 * idx + k, lay)
    for cp in cps:
        cp.wait()


def solution(mesh):
    def device_fn(w1_loc, w2_loc, w1_glb, w2_glb, mom1, mom2, x_loc, y_loc):
        arrays = (w1_loc, w2_loc, w1_glb, w2_glb, mom1, mom2)
        shapes = [jax.ShapeDtypeStruct(a.shape, F32) for a in arrays]
        dma = pltpu.SemaphoreType.DMA
        work = pl.pallas_call(
            main_body,
            out_shape=shapes + [jax.ShapeDtypeStruct((4, 8, 128, 256), F32)],
            in_specs=[HBM] * 8,
            out_specs=[VMEM] * 7,
            scratch_shapes=[
                pltpu.VMEM((H, B, D), BF16), pltpu.VMEM((H, B, D), BF16),
                pltpu.VMEM((L, D, FF), BF16), pltpu.VMEM((L, FF, D), BF16),
                pltpu.VMEM((L, B, D), BF16), pltpu.VMEM((L, B, FF), BF16), pltpu.VMEM((L, B, FF), F32),
                pltpu.VMEM((B, D), F32), pltpu.VMEM((B, D), F32),
                pltpu.VMEM((2, B, D), BF16), pltpu.VMEM((2, B, FF), BF16),
                pltpu.VMEM((4, 8, 128, 256), BF16), pltpu.VMEM((3, 4, 8, 32, 256), BF16),
                pltpu.VMEM((4, 8, 32, 256), F32), pltpu.VMEM((4, 8, 16, 256), F32),
                pltpu.VMEM((4, 8, 16, 256), F32), pltpu.VMEM((4, 8, 16, 256), F32),
                dma((26,)), dma((12, 3)), dma((12, 3)), dma((6, 12)), dma((6, 12)),
            ],
            compiler_params=pltpu.CompilerParams(
                collective_id=0, has_side_effects=True, vmem_limit_bytes=22 * 2**20),
            name='diloco_round',
        )(*[pltpu.with_memory_space_constraint(a, pltpu.HBM) for a in (*arrays, x_loc, y_loc)])
        outs = pl.pallas_call(
            write_body,
            out_shape=shapes,
            in_specs=[VMEM] * 7,
            out_specs=[HBM] * 6,
            scratch_shapes=[pltpu.VMEM((2, D, FF), F32), pltpu.VMEM((2, FF, D), F32)] * 3 + [dma((6, L))],
            compiler_params=pltpu.CompilerParams(vmem_limit_bytes=16 * 2**20),
            name='write_out',
        )(*work)
        return tuple(outs)

    local_spec = P(('shard', 'worker'))
    whole_spec = P()
    return jax.shard_map(device_fn, mesh=mesh, in_specs=(local_spec, local_spec, whole_spec, whole_spec, whole_spec, whole_spec, local_spec, local_spec), out_specs=(local_spec, local_spec, whole_spec, whole_spec, whole_spec, whole_spec), check_vma=False)
```

```python
import jax
import jax.numpy as jnp
from jax import lax
from jax.experimental import pallas as pl
from jax.experimental.pallas import tpu as pltpu
from jax.sharding import PartitionSpec as P

OUTER_LR = 0.7
OUTER_MOM = 0.9
MERGE_MIX = 0.5

L = 4
H = 4
D = 256
FF = 1024
B = 128
NB = FF // D
INNER_LR = 2.0 * D / (FF * L)
N_ALL = 16
GELU_K0 = 0.7978845608028654
GELU_K1 = GELU_K0 * 0.044715
F32 = jnp.float32
BF16 = jnp.bfloat16
MESH = pl.DeviceIdType.MESH
HBM = pl.BlockSpec(memory_space=pltpu.HBM)
VMEM = pl.BlockSpec(memory_space=pltpu.VMEM)

PIECES = ((1, 2), (1, 1), (0, 2), (0, 1))
COLOR_UNITS = ((3, 3, 2), (3, 2, 3), (2, 3, 3), (3, 3, 2))
GROUPS = []
for piece_idx in range(4):
    first_unit = 0
    for color in range(3):
        GROUPS.append((piece_idx, color, first_unit, COLOR_UNITS[piece_idx][color]))
        first_unit += COLOR_UNITS[piece_idx][color]
GATHER_ORDER = (0, 2, 3, 1)
RS1, X2, AG1, AG2, DDA, DDB = range(6)


def dot(a, b, ca, cb):
    return lax.dot_general(a, b, (((ca,), (cb,)), ((), ())), preferred_element_type=F32)


def gelu_parts(a):
    a2 = a * a
    t = jnp.tanh(a * (GELU_K0 + GELU_K1 * a2))
    return 0.5 + 0.5 * t, a2


def gelu_grad(u, h, a2):
    return h + (u * (1.0 - h)) * (2.0 * GELU_K0 + (6.0 * GELU_K1) * a2)


def unit_slice(mat, u):
    if mat == 2:
        return pl.ds(u * 128, 128), pl.ds(0, 256)
    return pl.ds((u % 2) * 128, 128), pl.ds((u // 2) * 256, 256)


def main_body(w1_in, w2_in, g1_in, g2_in, m1_in, m2_in, x_in, y_in,
              w1, w2, g1, g2, m1, m2, full,
              xb, yb, w1b, w2b, hb, ub, du, hid, dhid, eb, cb,
              delta, raw, s1, r1, s2, r2,
              ld_sem, s0_send, s0_recv, st_send, st_recv):
    zc = lax.axis_index('shard')
    wk = lax.axis_index('worker')
    core = lax.rem(wk, 2)
    xc = lax.rem(wk // 2, 2)
    yc = wk // 4
    coord = (xc, yc, zc)

    def chip_peer(dim, same_core=True):
        w = wk
        s = zc
        if dim == 0:
            w = wk + 2 - 4 * xc
        elif dim == 1:
            w = wk + 4 - 8 * yc
        elif dim == 2:
            s = 1 - zc
        if not same_core:
            w = w + 1 - 2 * core
        return (s, w)

    partner = chip_peer(3, False)

    bar = pltpu.get_barrier_semaphore()
    pl.semaphore_signal(bar, inc=1, device_id=partner, device_id_type=MESH)
    for dim in range(3):
        for same in (True, False):
            pl.semaphore_signal(bar, inc=1, device_id=chip_peer(dim, same), device_id_type=MESH)

    def w_load(lay):
        return (pltpu.make_async_copy(w1_in.at[0, lay], w1.at[0, lay], ld_sem.at[lay]),
                pltpu.make_async_copy(w2_in.at[0, lay], w2.at[0, lay], ld_sem.at[L + lay]))

    def w_start(lay):
        for src, dst, n, idx in ((w1_in, w1, D // 4, lay), (w2_in, w2, FF // 4, L + lay)):
            for i in range(4):
                rows = pl.ds(i * n, n)
                pltpu.make_async_copy(src.at[0, lay, rows], dst.at[0, lay, rows], ld_sem.at[idx]).start()

    def g_load(mat, lay):
        if mat == 1:
            return pltpu.make_async_copy(g1_in.at[lay], g1.at[lay], ld_sem.at[2 * L + lay])
        return pltpu.make_async_copy(g2_in.at[lay], g2.at[lay], ld_sem.at[3 * L + lay])

    def m_load(mat, lay):
        if mat == 1:
            return pltpu.make_async_copy(m1_in.at[lay], m1.at[lay], ld_sem.at[4 * L + lay])
        return pltpu.make_async_copy(m2_in.at[lay], m2.at[lay], ld_sem.at[5 * L + lay])

    x_load = pltpu.make_async_copy(x_in.at[0], xb, ld_sem.at[6 * L])
    y_load = pltpu.make_async_copy(y_in.at[0], yb, ld_sem.at[6 * L + 1])
    x_load.start()
    w_start(0)
    y_load.start()
    for lay in range(1, L):
        w_start(lay)
    for lay in range(L):
        for mat in (1, 2):
            g_load(mat, lay).start()
    for lay in range(L):
        for mat in (1, 2):
            m_load(mat, lay).start()
    x_load.wait()
    y_load.wait()

    def dims_of(color_idx):
        return color_idx % 3, (color_idx + 1) % 3, (color_idx + 2) % 3

    def rs0_copies(gi):
        p, c, u0, nu = GROUPS[gi]
        d0 = dims_of(c)[0]
        k0 = coord[d0]
        us = pl.ds(u0, nu)
        other = 1 - core

        def rows(tc, blk):
            return pl.ds(pl.multiple_of(tc * 64 + blk * 32, 32), 32)

        out = []
        for idx, (tc, blk, dev) in enumerate(((other, k0, partner),
                                               (core, 1 - k0, chip_peer(d0, True)),
                                               (other, 1 - k0, chip_peer(d0, False)))):
            out.append(pltpu.make_async_remote_copy(
                src_ref=delta.at[p, us, rows(tc, blk)], dst_ref=raw.at[idx, p, us],
                send_sem=s0_send.at[gi, idx], recv_sem=s0_recv.at[gi, idx],
                device_id=dev, device_id_type=MESH))
        return out

    def stage_copy(stage, gi):
        p, c, u0, nu = GROUPS[gi]
        d0, d1, d2 = dims_of(c)
        k0, k1, k2 = coord[d0], coord[d1], coord[d2]
        us = pl.ds(u0, nu)
        if stage == RS1:
            src, dst, dev = s1.at[p, us, pl.ds(pl.multiple_of((1 - k1) * 16, 16), 16)], r1.at[p, us], chip_peer(d1)
        elif stage == X2:
            src, dst, dev = s2.at[p, us], r2.at[p, us], chip_peer(d2)
        else:
            base = core * 64
            if stage == AG1:
                off, n, dev = base + k0 * 32 + k1 * 16, 16, chip_peer(d1)
            elif stage == AG2:
                off, n, dev = base + k0 * 32, 32, chip_peer(d0)
            elif stage == DDA:
                off, n, dev = base + k0 * 32, 32, partner
            else:
                off, n, dev = base + (1 - k0) * 32, 32, partner
            src = full.at[p, us, pl.ds(pl.multiple_of(off, 16), n)]
            dst = src
        return pltpu.make_async_remote_copy(
            src_ref=src, dst_ref=dst, send_sem=st_send.at[stage, gi], recv_sem=st_recv.at[stage, gi],
            device_id=dev, device_id_type=MESH)

    def keeps_pre_act(k, lay):
        return k == 2 or (k == 0 and lay < 2)

    def grad_from_pre_act(lay, cols):
        a = du[lay, :, cols]
        h, a2 = gelu_parts(a)
        return gelu_grad(a * h, h, a2)

    def forward(k, before_layer_1=None):
        hid[...] = xb[k].astype(F32)

        def layer(lay, _):
            if k == 0:
                load_1, load_2 = w_load(lay)
                load_1.wait()
                if lay > 0:
                    load_2.wait()
            if before_layer_1 is not None and lay == 1:
                before_layer_1()
            h_bf = hid[...].astype(BF16)
            hb[lay] = h_bf
            acc = hid[...]
            for j in range(NB):
                cols = slice(j * D, (j + 1) * D)
                if k == 0:
                    w1b[lay, :, cols] = w1[0, lay, :, cols].astype(BF16)
                a = dot(h_bf, w1b[lay, :, cols], 1, 0)
                h, a2 = gelu_parts(a)
                u = a * h
                u_bf = u.astype(BF16)
                ub[lay, :, cols] = u_bf
                du[lay, :, cols] = a if keeps_pre_act(k, lay) else gelu_grad(u, h, a2)
                if k == 0:
                    if lay == 0 and j == 0:
                        load_2.wait()
                    w2b[lay, cols, :] = w2[0, lay, cols, :].astype(BF16)
                acc = acc + dot(u_bf, w2b[lay, cols, :], 1, 0)
            hid[...] = acc
            return 0

        for lay in range(L):
            layer(lay, 0)

    def loss_grad(k):
        dhid[...] = (2.0 / (B * D)) * (hid[...] - yb[k].astype(F32))

    def update2(lay, cols, u_j, e):
        new2 = w2[0, lay, cols, :] - INNER_LR * dot(u_j, e, 0, 0)
        w2[0, lay, cols, :] = new2
        w2b[lay, cols, :] = new2.astype(BF16)

    def update1(lay, cols, h_bf, c):
        new1 = w1[0, lay, :, cols] - INNER_LR * dot(h_bf, c, 0, 0)
        w1[0, lay, :, cols] = new1
        w1b[lay, :, cols] = new1.astype(BF16)

    def send_piece(i, which):
        for p in (which, 2 + which):
            @pl.when(i == p // 2)
            def _(p=p):
                for gi in range(3 * p, 3 * p + 3):
                    for cp in rs0_copies(gi):
                        cp.start()

    def back_send(i, lay, after_first=None):
        p = 2 * i
        e = dhid[...].astype(BF16)
        h_bf = hb[lay]
        g_load(2, lay).wait()
        for j in range(NB):
            cols = slice(j * D, (j + 1) * D)
            new2 = w2[0, lay, cols, :] - INNER_LR * dot(ub[lay, :, cols], e, 0, 0)
            w2[0, lay, cols, :] = new2
            dl = (g2[lay, cols, :] - new2).astype(BF16)
            delta[p, 2 * j] = dl[:128]
            delta[p, 2 * j + 1] = dl[128:]
        send_piece(i, 0)
        if after_first is not None:
            pl.when(i == 0)(after_first)
        g_load(1, lay).wait()
        acc = dhid[...]
        for j in range(NB):
            cols = slice(j * D, (j + 1) * D)
            d_u = dot(e, w2b[lay, cols, :], 1, 1)
            c = (grad_from_pre_act(lay, cols) * d_u).astype(BF16)
            acc = acc + dot(c, w1b[lay, :, cols], 1, 1)
            new1 = w1[0, lay, :, cols] - INNER_LR * dot(h_bf, c, 0, 0)
            w1[0, lay, :, cols] = new1
            w1b[lay, :, cols] = new1.astype(BF16)
            dl = (g1[lay, :, cols] - new1).astype(BF16)
            delta[p + 1, 2 * j] = dl[:128]
            delta[p + 1, 2 * j + 1] = dl[128:]
        dhid[...] = acc
        send_piece(i, 1)
        w2b[lay] = w2[0, lay].astype(BF16)

    def back_full(lay, need_input_grad=True, pre_act=False):
        e = dhid[...].astype(BF16)
        h_bf = hb[lay]
        acc = dhid[...]
        for j in range(NB):
            cols = slice(j * D, (j + 1) * D)
            d_u = dot(e, w2b[lay, cols, :], 1, 1)
            grad = grad_from_pre_act(lay, cols) if pre_act else du[lay, :, cols]
            c = (grad * d_u).astype(BF16)
            update2(lay, cols, ub[lay, :, cols], e)
            if need_input_grad:
                acc = acc + dot(c, w1b[lay, :, cols], 1, 1)
            update1(lay, cols, h_bf, c)
        if need_input_grad:
            dhid[...] = acc

    def back_chain(lay):
        e = dhid[...].astype(BF16)
        eb[lay - 2] = e
        acc = dhid[...]
        for j in range(NB):
            cols = slice(j * D, (j + 1) * D)
            d_u = dot(e, w2b[lay, cols, :], 1, 1)
            c = (du[lay, :, cols] * d_u).astype(BF16)
            cb[lay - 2, :, cols] = c
            acc = acc + dot(c, w1b[lay, :, cols], 1, 1)
        dhid[...] = acc

    def back_weights(lay):
        e = eb[lay - 2]
        h_bf = hb[lay]
        for j in range(NB):
            cols = slice(j * D, (j + 1) * D)
            update2(lay, cols, ub[lay, :, cols], e)
            update1(lay, cols, h_bf, cb[lay - 2, :, cols])

    def reduce_stage1(p):
        for gi in range(3 * p, 3 * p + 3):
            _, c, u0, nu = GROUPS[gi]
            rows = pl.ds(pl.multiple_of(core * 64 + coord[dims_of(c)[0]] * 32, 32), 32)
            for cp in rs0_copies(gi):
                cp.wait_recv()
            for u in range(u0, u0 + nu):
                s1[p, u] = ((delta[p, u, rows, :].astype(F32) + raw[0, p, u].astype(F32))
                            + (raw[1, p, u].astype(F32) + raw[2, p, u].astype(F32)))
            stage_copy(RS1, gi).start()

    def reduce_stage2(p):
        for gi in range(3 * p, 3 * p + 3):
            _, c, u0, nu = GROUPS[gi]
            rows = pl.ds(pl.multiple_of(coord[dims_of(c)[1]] * 16, 16), 16)
            stage_copy(RS1, gi).wait_recv()
            for u in range(u0, u0 + nu):
                s2[p, u] = s1[p, u, rows, :] + r1[p, u]
            stage_copy(X2, gi).start()

    def reduce_stage3(p):
        for gi in range(3 * p, 3 * p + 3):
            _, c, u0, nu = GROUPS[gi]
            d0, d1, d2 = dims_of(c)
            rows = pl.ds(pl.multiple_of(core * 64 + coord[d0] * 32 + coord[d1] * 16, 16), 16)
            stage_copy(X2, gi).wait_recv()
            for u in range(u0, u0 + nu):
                full[p, u, rows, :] = s2[p, u] + r2[p, u]
            stage_copy(AG1, gi).start()

    def gather_stage2(p):
        for gi in range(3 * p, 3 * p + 3):
            stage_copy(AG1, gi).wait_recv()
            stage_copy(AG2, gi).start()
            stage_copy(DDA, gi).start()

    def gather_stage3(p):
        for gi in range(3 * p, 3 * p + 3):
            stage_copy(AG2, gi).wait_recv()
            stage_copy(DDB, gi).start()

    def outer_update(p, merge=True, outer=True):
        lay, mat = PIECES[p]
        wr, wbr, gr, mr = (w1, w1b, g1, m1) if mat == 1 else (w2, w2b, g2, m2)
        if merge:
            m_load(mat, lay).wait()
            wait_gathered(p)
        for u in range(8):
            rows, cols = unit_slice(mat, u)
            mean = full[p, u] * (1.0 / N_ALL)
            mom = OUTER_MOM * mr[lay, rows, cols] + mean
            glob = gr[lay, rows, cols] - OUTER_LR * (OUTER_MOM * mom + mean)
            if outer:
                mr[lay, rows, cols] = mom
                gr[lay, rows, cols] = glob
            if merge:
                merged = MERGE_MIX * wr[0, lay, rows, cols] + (1.0 - MERGE_MIX) * glob
                wr[0, lay, rows, cols] = merged
                wbr[lay, rows, cols] = merged.astype(BF16)

    last_piece = GATHER_ORDER[-1]

    def wait_gathered(p):
        for gi in range(3 * p, 3 * p + 3):
            stage_copy(DDA, gi).wait_recv()
            stage_copy(DDB, gi).wait_recv()

    def finish(frag):
        if frag == 0:
            outer_update(last_piece, outer=False)
        else:
            for p, (part, mat) in enumerate(PIECES):
                m_load(mat, 2 + part).wait()
                wait_gathered(p)
        for gi in range(12):
            for cp in rs0_copies(gi):
                cp.wait_send()
            for stage in range(6):
                stage_copy(stage, gi).wait_send()

    def sync(frag):
        reduce_stage1(3)
        for p in range(4):
            reduce_stage2(p)
        for p in range(4):
            reduce_stage3(p)
        for p in GATHER_ORDER:
            gather_stage2(p)
        back_full(1)
        back_full(0, False)
        prev = None
        for p in GATHER_ORDER:
            gather_stage3(p)
            if prev is not None and frag == 0:
                outer_update(prev)
            prev = p

    def layers(lo, body):
        def run(i, _):
            body(i, lo - i)
            return 0
        return run

    forward(0)
    pl.semaphore_wait(bar, 7)
    loss_grad(0)
    back_chain(3)
    back_chain(2)

    lax.fori_loop(0, 2, layers(1, back_send), 0)
    lax.fori_loop(0, 2, layers(3, lambda i, lay: back_weights(lay)), 0)

    def back_hook(i, lay):
        back_full(lay)
        for p in (1, 2):
            @pl.when(i == p - 1)
            def _(p=p):
                reduce_stage1(p)

    forward(1)
    loss_grad(1)
    reduce_stage1(0)
    lax.fori_loop(0, 2, layers(3, back_hook), 0)
    sync(0)

    forward(2, lambda: finish(0))
    loss_grad(2)

    lax.fori_loop(0, 2, layers(3, lambda i, lay: back_send(
        i, lay, lambda: outer_update(last_piece, merge=False))), 0)
    back_full(1, True, True)
    back_full(0, False, True)

    forward(3)
    loss_grad(3)
    reduce_stage1(0)
    lax.fori_loop(0, 2, layers(3, back_hook), 0)
    sync(1)
    finish(1)


def write_body(w1, w2, g1, g2, m1, m2, full, *refs):
    dsts, stages, sem = refs[:6], refs[6:12], refs[12]
    srcs = (w1, w2, g1, g2, m1, m2)
    cps = []

    def put(src, i, lay):
        dst = dsts[i].at[0, lay] if i < 2 else dsts[i].at[lay]
        half = src.shape[0] // 2
        for rows in (pl.ds(0, half), pl.ds(half, half)):
            pltpu.make_async_copy(src.at[rows], dst.at[rows], sem.at[i, lay]).start()
        cps.append(pltpu.make_async_copy(src, dst, sem.at[i, lay]))

    for lay in range(2):
        for i in range(6):
            put(srcs[i].at[0, lay] if i < 2 else srcs[i].at[lay], i, lay)
    for p, (part, mat) in enumerate(PIECES):
        lay = 2 + part
        k = mat - 1
        wr, gr, mr = srcs[k], srcs[2 + k], srcs[4 + k]
        ws, gs, ms = stages[k], stages[2 + k], stages[4 + k]
        for u in range(8):
            rows, cols = unit_slice(mat, u)
            mean = full[p, u] * (1.0 / N_ALL)
            mom = OUTER_MOM * mr[lay, rows, cols] + mean
            glob = gr[lay, rows, cols] - OUTER_LR * (OUTER_MOM * mom + mean)
            ms[part, rows, cols] = mom
            gs[part, rows, cols] = glob
            ws[part, rows, cols] = MERGE_MIX * wr[0, lay, rows, cols] + (1.0 - MERGE_MIX) * glob
        for idx, st in enumerate((ws, gs, ms)):
            put(st.at[part], 2 * idx + k, lay)
    for cp in cps:
        cp.wait()


def solution(mesh):
    def device_fn(w1_loc, w2_loc, w1_glb, w2_glb, mom1, mom2, x_loc, y_loc):
        arrays = (w1_loc, w2_loc, w1_glb, w2_glb, mom1, mom2)
        shapes = [jax.ShapeDtypeStruct(a.shape, F32) for a in arrays]
        dma = pltpu.SemaphoreType.DMA
        work = pl.pallas_call(
            main_body,
            out_shape=shapes + [jax.ShapeDtypeStruct((4, 8, 128, 256), F32)],
            in_specs=[HBM] * 8,
            out_specs=[VMEM] * 7,
            scratch_shapes=[
                pltpu.VMEM((H, B, D), BF16), pltpu.VMEM((H, B, D), BF16),
                pltpu.VMEM((L, D, FF), BF16), pltpu.VMEM((L, FF, D), BF16),
                pltpu.VMEM((L, B, D), BF16), pltpu.VMEM((L, B, FF), BF16), pltpu.VMEM((L, B, FF), F32),
                pltpu.VMEM((B, D), F32), pltpu.VMEM((B, D), F32),
                pltpu.VMEM((2, B, D), BF16), pltpu.VMEM((2, B, FF), BF16),
                pltpu.VMEM((4, 8, 128, 256), BF16), pltpu.VMEM((3, 4, 8, 32, 256), BF16),
                pltpu.VMEM((4, 8, 32, 256), F32), pltpu.VMEM((4, 8, 16, 256), F32),
                pltpu.VMEM((4, 8, 16, 256), F32), pltpu.VMEM((4, 8, 16, 256), F32),
                dma((26,)), dma((12, 3)), dma((12, 3)), dma((6, 12)), dma((6, 12)),
            ],
            compiler_params=pltpu.CompilerParams(
                collective_id=0, has_side_effects=True, vmem_limit_bytes=22 * 2**20),
            name='diloco_round',
        )(*[pltpu.with_memory_space_constraint(a, pltpu.HBM) for a in (*arrays, x_loc, y_loc)])
        outs = pl.pallas_call(
            write_body,
            out_shape=shapes,
            in_specs=[VMEM] * 7,
            out_specs=[HBM] * 6,
            scratch_shapes=[pltpu.VMEM((2, D, FF), F32), pltpu.VMEM((2, FF, D), F32)] * 3 + [dma((6, L))],
            compiler_params=pltpu.CompilerParams(vmem_limit_bytes=16 * 2**20),
            name='write_out',
        )(*work)
        return tuple(outs)

    local_spec = P(('shard', 'worker'))
    whole_spec = P()
    return jax.shard_map(device_fn, mesh=mesh, in_specs=(local_spec, local_spec, whole_spec, whole_spec, whole_spec, whole_spec, local_spec, local_spec), out_specs=(local_spec, local_spec, whole_spec, whole_spec, whole_spec, whole_spec), check_vma=False)
```
